32 devices in a mesh: fsdp: 16 (over z, x, core), rep: 2 (over y).
Axes of the slice: x: 2, y: 2, z: 4, core: 2. Of those that a mesh axis runs over, the one named last changes fastest.
Arguments:
- tokens: bfloat16 [37632, 256], P(('fsdp', 'rep')), may hold values from -6 to 6
- heights: int32 [32], P(('fsdp', 'rep')), may hold values from 7 to 28, as said below
- widths: int32 [32], P(('fsdp', 'rep')), may hold values from 7 to 42, as said below
- w_qkv: bfloat16 [2, 256, 768], P(None, 'fsdp'), may hold values from -0.375 to 0.375
- w_proj: bfloat16 [2, 256, 256], P(None, 'fsdp'), may hold values from -0.75 to 0.75
- w_fc1: bfloat16 [2, 256, 1024], P(None, 'fsdp'), may hold values from -0.375 to 0.375
- w_fc2: bfloat16 [2, 1024, 256], P(None, 'fsdp'), may hold values from -0.1875 to 0.1875
- vectors: bfloat16 [2, 22, 256], P(None, None, 'fsdp'), may hold values from -0.9 to 1.3
- cotangent: bfloat16 [37632, 256], P(('fsdp', 'rep')), may hold values from -6 to 6, as said below
Outputs:
- outputs: float32 [37632, 256], P(('fsdp', 'rep'))
- grad_tokens: float32 [37632, 256], P(('fsdp', 'rep'))
- grad_w_qkv: float32 [2, 256, 768], P(None, 'fsdp')
- grad_w_proj: float32 [2, 256, 256], P(None, 'fsdp')
- grad_w_fc1: float32 [2, 256, 1024], P(None, 'fsdp')
- grad_w_fc2: float32 [2, 1024, 256], P(None, 'fsdp')
- grad_vectors: float32 [2, 22, 256], P(None, None, 'fsdp')
The draws below stay inside these ranges and needn't reach their ends.
Inputs may be any that keep to these rules, and one draw needn't show every extreme that they name: `heights`: multiples of 7; the first image's height is 28. `widths`: multiples of 7; the first image's width is 42. `cotangent`: zero on cells that are not live.
All inputs are finite; a program needn't handle non-finite values.
Results may differ from the reference program's by a relative error of at most 0.018.
Values may be sent and summed in bfloat16 or wider, within the bound.
A program may use at most 192 MiB of HBM per device.

```python
import jax
import jax.numpy as jnp
from jax import lax

D = 256
FF = 1024
HEAD = 32
STRIPE = 7
LAYERS = 2
HP = 28
WP = 42
IMG_DEV = 1
IMAGES = 32
TOKENS = 37632
VROWS = 22


def image_sizes(key):
    levels_rows = jax.random.randint(jax.random.fold_in(key, 11), (IMAGES,), 1, HP // STRIPE + 1)
    levels_cols = jax.random.randint(jax.random.fold_in(key, 23), (IMAGES,), 1, WP // STRIPE + 1)
    heights_drawn = (STRIPE * levels_rows).at[0].set(HP).astype(jnp.int32)
    widths_drawn = (STRIPE * levels_cols).at[0].set(WP).astype(jnp.int32)
    return (heights_drawn, widths_drawn)


def draw_heights(key, part):
    return image_sizes(key)[0]


def draw_widths(key, part):
    return image_sizes(key)[1]


def draw_cotangent(key, part):
    heights_drawn, widths_drawn = image_sizes(key)
    row_index = lax.broadcasted_iota(jnp.int32, (IMAGES, HP, WP), 1)
    col_index = lax.broadcasted_iota(jnp.int32, (IMAGES, HP, WP), 2)
    live = (row_index < heights_drawn[:, None, None]) & (col_index < widths_drawn[:, None, None])
    live_rows = live.reshape(IMAGES * HP * WP, 1).astype(jnp.float32)
    noise_key = jax.random.fold_in(key, 37)
    raw_values = jnp.clip(jax.random.normal(noise_key, (IMAGES * HP * WP, D), jnp.float32), -6.0, 6.0)
    return (raw_values * live_rows).astype(jnp.bfloat16)


def draw_vectors(key, part):
    full_shape = (LAYERS, VROWS, D)
    raw_values = jnp.clip(jax.random.normal(key, full_shape, jnp.float32), -3.0, 3.0)
    row_id = lax.broadcasted_iota(jnp.int32, full_shape, 1)
    is_gain = (row_id == 0) | (row_id == 5)
    is_tap = (row_id >= 9) & (row_id < 18)
    spread = jnp.where(is_gain, 0.1, jnp.where(is_tap, 0.15, 0.3))
    return (jnp.where(is_gain, 1.0, 0.0) + spread * raw_values).astype(jnp.bfloat16)


def block_scale(rng, dims, cuts, low, largest):
    def one(dim, shards_of):
        draws = jax.random.uniform(jax.random.fold_in(jax.random.fold_in(rng, 6), dim), (shards_of,), jnp.float32, low / len(cuts), largest / len(cuts))
        return jnp.repeat(jnp.exp(draws), dims[dim] // shards_of).reshape((-1,) + (1,) * (len(dims) - dim - 1))

    level = one(*cuts[0])
    for cut in cuts[1:]:
        level = level * one(*cut)
    return level


def gaussian(own_key, dims, deviation, reach, cuts=(), dtype=jnp.bfloat16):
    factor_of = block_scale(own_key, dims, cuts, -0.22, 0.18) if cuts else 1.0
    drawn = jax.random.normal(own_key, dims, jnp.float32) * deviation * factor_of
    return jnp.minimum(jnp.maximum(drawn, -reach), reach).astype(dtype)


def setup_inputs(seed: int = 0) -> dict:
    key_list = jax.random.split(jax.random.key(seed), 10)
    tokens = gaussian(key_list[0], (TOKENS, D), 1.0, 6.0, ((0, 32),))
    heights = draw_heights(jax.random.fold_in(key_list[9], 71), 0)
    widths = draw_widths(jax.random.fold_in(key_list[9], 71), 0)
    w_qkv = gaussian(key_list[3], (LAYERS, D, 3 * D), D ** -0.5, 0.375, ((1, 16),))
    w_proj = gaussian(key_list[4], (LAYERS, D, D), (D // 4) ** -0.5, 0.75, ((1, 16),))
    w_fc1 = gaussian(key_list[5], (LAYERS, D, FF), D ** -0.5, 0.375, ((1, 16),))
    w_fc2 = gaussian(key_list[6], (LAYERS, FF, D), FF ** -0.5, 0.1875, ((1, 16),))
    vectors = draw_vectors(jax.random.fold_in(key_list[9], 71), 0)
    cotangent = draw_cotangent(jax.random.fold_in(key_list[9], 71), 0)
    return dict(tokens=tokens, heights=heights, widths=widths, w_qkv=w_qkv, w_proj=w_proj, w_fc1=w_fc1, w_fc2=w_fc2, vectors=vectors, cotangent=cotangent)


@jax.custom_vjp
def low(v):
    return lax.optimization_barrier(v.astype(jnp.bfloat16)).astype(jnp.float32)

@jax.custom_vjp
def low_back(v):
    return v

def low_keep(v):
    return (low(v), None)

def low_pass(kept, grad):
    return (grad,)

def back_keep(v):
    return (v, None)

def back_low(kept, grad):
    return (low(grad),)
low.defvjp(low_keep, low_pass)
low_back.defvjp(back_keep, back_low)
eps_norm = 1e-05
masked_score = -1000000000.0

def layer_norm(values, gain, shift):
    centre = lax.optimization_barrier(jnp.mean(values, axis=-1, keepdims=True))
    centred = values - centre
    spread = lax.optimization_barrier(jnp.mean(centred * centred, axis=-1, keepdims=True))
    return centred * lax.rsqrt(spread + eps_norm) * gain + shift

def position_term(values, taps, shift):
    image_count, height, breadth, channels = values.shape
    half_dim = channels // 2
    rows_part = values[..., :half_dim].reshape(image_count, height // STRIPE, STRIPE, breadth, half_dim)
    padded = jnp.pad(rows_part, ((0, 0), (0, 0), (1, 1), (1, 1), (0, 0)))
    total_rows = jnp.zeros_like(rows_part)
    for tap_index in range(9):
        offset_row, offset_col = (tap_index // 3, tap_index % 3)
        total_rows = total_rows + padded[:, :, offset_row:offset_row + STRIPE, offset_col:offset_col + breadth, :] * taps[tap_index, :half_dim]
    cols_part = values[..., half_dim:].reshape(image_count, height, breadth // STRIPE, STRIPE, half_dim)
    padded = jnp.pad(cols_part, ((0, 0), (1, 1), (0, 0), (1, 1), (0, 0)))
    total_cols = jnp.zeros_like(cols_part)
    for tap_index in range(9):
        offset_row, offset_col = (tap_index // 3, tap_index % 3)
        total_cols = total_cols + padded[:, offset_row:offset_row + height, :, offset_col:offset_col + STRIPE, :] * taps[tap_index, half_dim:]
    joined = jnp.concatenate([total_rows.reshape(image_count, height, breadth, half_dim), total_cols.reshape(image_count, height, breadth, half_dim)], axis=-1)
    return joined + shift

def to_rows(tensor):
    image_count, height, breadth, channels = tensor.shape
    return tensor.reshape(image_count, height // STRIPE, STRIPE * breadth, channels)

def from_rows(tensor, height, breadth):
    return tensor.reshape(tensor.shape[0], height, breadth, tensor.shape[-1])

def to_columns(tensor):
    image_count, height, breadth, channels = tensor.shape
    split = tensor.reshape(image_count, height, breadth // STRIPE, STRIPE, channels)
    return split.transpose(0, 2, 1, 3, 4).reshape(image_count, breadth // STRIPE, height * STRIPE, channels)

def from_columns(tensor, height, breadth):
    image_count, stripes, length, channels = tensor.shape
    split = tensor.reshape(image_count, stripes, height, STRIPE, channels)
    return split.transpose(0, 2, 1, 3, 4).reshape(image_count, height, breadth, channels)

def ref_attend(queries, keys_in, values, live):
    image_count, stripes, length, channels = queries.shape
    shape_five = (image_count, stripes, length, channels // HEAD, HEAD)
    score_scale = HEAD ** (-0.5)
    scores = jnp.einsum('gsqhd,gskhd->gshqk', queries.reshape(shape_five), keys_in.reshape(shape_five), precision=lax.Precision.HIGHEST) * score_scale
    scores = scores + jnp.where(live[:, :, None, None, :], 0.0, masked_score)
    scores = low_back(scores)
    row_max = lax.optimization_barrier(jnp.max(scores, axis=-1, keepdims=True))
    expo = jnp.exp(scores - row_max)
    probs = low(expo / lax.optimization_barrier(jnp.sum(expo, axis=-1, keepdims=True)))
    mixed = jnp.einsum('gshqk,gskhd->gsqhd', probs, values.reshape(shape_five), precision=lax.Precision.HIGHEST)
    return mixed.reshape(image_count, stripes, length, channels)

def ref_layer(hidden_in, live, params):
    w_mix, w_out, w_up, w_down, vec = params
    width_d = vec.shape[1]
    half_dim = width_d // 2
    height, breadth = (hidden_in.shape[1], hidden_in.shape[2])
    normed = layer_norm(hidden_in, vec[0], vec[1])
    bias_mix = jnp.concatenate([vec[2], jnp.zeros_like(vec[2]), vec[3]])
    mixed = low(low_back(jnp.einsum('gijc,cm->gijm', low(normed), w_mix, precision=lax.Precision.HIGHEST)) + bias_mix)
    queries = mixed[..., :width_d]
    keys_all = mixed[..., width_d:2 * width_d]
    values_all = mixed[..., 2 * width_d:] * live[..., None].astype(jnp.float32)
    live_rows = to_rows(live[..., None])[..., 0]
    live_cols = to_columns(live[..., None])[..., 0]
    out_rows = ref_attend(to_rows(queries[..., :half_dim]), to_rows(keys_all[..., :half_dim]), to_rows(values_all[..., :half_dim]), live_rows)
    out_cols = ref_attend(to_columns(queries[..., half_dim:]), to_columns(keys_all[..., half_dim:]), to_columns(values_all[..., half_dim:]), live_cols)
    attended = jnp.concatenate([from_rows(out_rows, height, breadth), from_columns(out_cols, height, breadth)], axis=-1)
    attn = low(low_back(attended + position_term(values_all, vec[9:18], vec[8])))
    after = hidden_in + low_back(jnp.einsum('gijc,cd->gijd', attn, w_out, precision=lax.Precision.HIGHEST)) + vec[4]
    normed_two = layer_norm(after, vec[5], vec[6])
    hidden = low_back(jnp.einsum('gijc,cf->gijf', low(normed_two), w_up, precision=lax.Precision.HIGHEST)) + vec[18:].reshape(-1)
    act = low(jax.nn.gelu(hidden, approximate=False))
    return after + low_back(jnp.einsum('gijf,fd->gijd', act, w_down, precision=lax.Precision.HIGHEST)) + vec[7]

def reference(tokens, heights, widths, w_qkv, w_proj, w_fc1, w_fc2, vectors, cotangent):
    params = (w_qkv.astype(jnp.float32), w_proj.astype(jnp.float32), w_fc1.astype(jnp.float32), w_fc2.astype(jnp.float32), vectors.astype(jnp.float32))
    group_count = IMAGES // IMG_DEV
    width_d = tokens.shape[1]
    inputs = tokens.astype(jnp.float32).reshape(group_count, IMG_DEV, HP, WP, width_d)
    cotangents = cotangent.astype(jnp.float32).reshape(group_count, IMG_DEV, HP, WP, width_d)
    heights_grouped = heights.reshape(group_count, IMG_DEV)
    widths_grouped = widths.reshape(group_count, IMG_DEV)
    row_index = lax.broadcasted_iota(jnp.int32, (IMG_DEV, HP, WP), 1)
    col_index = lax.broadcasted_iota(jnp.int32, (IMG_DEV, HP, WP), 2)

    def one_group(carry, group_item):
        inputs_here, heights_here, widths_here, cot_here = group_item
        live = (row_index < heights_here[:, None, None]) & (col_index < widths_here[:, None, None])

        def forward(hidden_in, weights):
            for layer_index in range(LAYERS):
                hidden_in = ref_layer(hidden_in, live, tuple((member[layer_index] for member in weights)))
            return hidden_in
        result, pullback = jax.vjp(forward, inputs_here, params)
        grad_in, grad_params = pullback(cot_here)
        carry = jax.tree.map(jnp.add, carry, grad_params)
        return (carry, (result, grad_in))
    zero_grads = jax.tree.map(jnp.zeros_like, params)
    totals, (results, grads_in) = lax.scan(one_group, zero_grads, (inputs, heights_grouped, widths_grouped, cotangents))
    return (results.reshape(-1, width_d), grads_in.reshape(-1, width_d), totals[0], totals[1], totals[2], totals[3], totals[4])
```

```python
import functools
import jax
import jax.numpy as jnp
from jax import lax
from jax.experimental import pallas as pl
from jax.experimental.pallas import tpu as pltpu

HEAD = 32
STRIPE = 7
HP = 28
WP = 42
HEADS = 4
GROUP = 8
WG = WP // STRIPE
ROWS = HP * WG * GROUP
CHUNK = STRIPE * WG * GROUP
TALL = HP * GROUP
WIDE_R = 384
WIDE_C = 256
BF = jnp.bfloat16
F32 = jnp.float32
eps_norm = 1e-05
masked_score = -1000000000.0
LOG2E = 1.4426950408889634
LN2 = 0.6931471805599453
SCALE = HEAD ** (-0.5)
NN = (((1,), (0,)), ((), ()))
NT = (((1,), (1,)), ((), ()))
TN = (((0,), (0,)), ((), ()))


def mm(a, b, dims=NN):
    return lax.dot_general(a, b, dims, preferred_element_type=F32)


def iota(shape, dim):
    return lax.broadcasted_iota(jnp.int32, shape, dim)


def span(index, size):
    return pl.ds(pl.multiple_of(index * size, size), size)


def pad_groups(src, dst, scale=None):
    def body(j, carry):
        block = src[pl.ds(pl.multiple_of(j * 56, 8), 56), :].astype(F32).reshape(7, 8, -1)
        place = iota((8, block.shape[-1]), 0)
        for u in range(8):
            if u == 0:
                group = block[0]
            elif u == 7:
                group = pltpu.roll(block[6], 7, 0)
            else:
                group = jnp.where(
                    place < u, pltpu.roll(block[u - 1], u, 0), pltpu.roll(block[u], u, 0)
                )
            group = jnp.where(place < 7, group, 0.0)
            dst[pl.ds(pl.multiple_of(j * 64 + u * 8, 8), 8), :] = group
        return carry

    lax.fori_loop(0, ROWS // 64, body, 0)


def drop_groups(src, dst):
    def body(j, carry):
        block = src[pl.ds(pl.multiple_of(j * 64, 8), 64), :].reshape(8, 8, -1)
        place = iota((8, block.shape[-1]), 0)
        for t in range(7):
            lower = block[t] if t == 0 else pltpu.roll(block[t], 8 - t, 0)
            upper = pltpu.roll(block[t + 1], 7 - t, 0)
            dst[pl.ds(pl.multiple_of(j * 56 + t * 8, 8), 8), :] = jnp.where(
                place <= 6 - t, lower, upper
            )
        return carry

    lax.fori_loop(0, ROWS // 64, body, 0)


def norm_parts(x):
    centre = jnp.mean(x, axis=-1, keepdims=True)
    centred = x - centre
    rate = lax.rsqrt(jnp.mean(centred * centred, axis=-1, keepdims=True) + eps_norm)
    return centred * rate, rate


def norm_back(d_n, xhat, rate, gain):
    e = d_n * gain
    return rate * (
        e
        - jnp.mean(e, axis=-1, keepdims=True)
        - xhat * jnp.mean(e * xhat, axis=-1, keepdims=True)
    )


def colsum(x):
    return jnp.sum(x, axis=0, keepdims=True)


def rows_live(stripe, h, w, lanes):
    shape = (STRIPE, WG * GROUP, lanes)
    row = iota(shape, 0) + stripe * STRIPE
    place = iota(shape, 1)
    within = place & 7
    col = (place >> 3) * STRIPE + within
    live = (row < h) & (col < w) & (within < STRIPE)
    return jnp.where(live, 1.0, 0.0).reshape(CHUNK, lanes)


def cols_live(stripe, h, w, lanes):
    shape = (HP, GROUP, lanes)
    row = iota(shape, 0)
    within = iota(shape, 1)
    live = (row < h) & (within + stripe * STRIPE < w) & (within < STRIPE)
    return jnp.where(live, 1.0, 0.0).reshape(TALL, lanes)


def with_mask(keys, live):
    lane = iota(live.shape, 1)
    extra = jnp.where(lane == 0, jnp.where(live > 0.0, 0.0, masked_score), 0.0)
    return jnp.concatenate([keys, extra.astype(BF)], axis=-1)


def stack_heads(ref, x, wide):
    length = x.shape[0]
    lane = iota(x.shape, 1)
    for h in range(HEADS):
        kept = jnp.where((lane >> 5) == h, x, jnp.zeros_like(x))
        ref[h * wide : h * wide + length, 0:128] = kept


def widen(x, wide):
    length = x.shape[0]
    return jnp.concatenate([x, jnp.zeros((wide - length, x.shape[1]), x.dtype)], axis=0)


def attend(q, k_mask, vm, qs, out_t, lse, stripe, wide):
    length = q.shape[0]
    stack_heads(qs, q, wide)
    scores = mm(k_mask, qs[0 : HEADS * wide, :], NT)
    v_t = widen(vm.astype(F32), wide).T.astype(BF)[:, 0:length]
    for h in range(HEADS):
        s = scores[:, h * wide : (h + 1) * wide]
        top = jnp.max(s, axis=0, keepdims=True)
        p = jnp.exp2(s - top)
        total = jnp.sum(p, axis=0, keepdims=True)
        o = mm(v_t[HEAD * h : HEAD * (h + 1), :], p.astype(BF))
        out_t[stripe, HEAD * h : HEAD * (h + 1), :] = o / total
        lse[stripe, h : h + 1, :] = top + jnp.log2(total)


def attend_back(q, k, k_mask, vm, da, qs, ds_stack, p_all, g_all, out_t, lse, stripe, wide):
    length = q.shape[0]
    stack_heads(qs, q, wide)
    stack_heads(ds_stack, da, wide)
    da_t = widen(da.astype(F32), wide).T
    k_t = widen(k.astype(F32), wide).T.astype(BF)[:, 0:length]
    weighted = da_t * out_t[stripe]
    dq_t = []
    scores = mm(k_mask, qs[0 : HEADS * wide, :], NT)
    d_probs = mm(vm, ds_stack[0 : HEADS * wide, :], NT)
    for h in range(HEADS):
        lanes = slice(h * wide, (h + 1) * wide)
        inner = jnp.sum(weighted[HEAD * h : HEAD * (h + 1), :], axis=0, keepdims=True)
        p = jnp.exp2(scores[:, lanes] - lse[stripe, h : h + 1, :])
        g = (p * (d_probs[:, lanes] - inner)).astype(BF)
        p_all[0:length, lanes] = p.astype(BF)
        g_all[0:length, lanes] = g
        dq_t.append(mm(k_t[HEAD * h : HEAD * (h + 1), :], g))
    dv = mm(p_all[0:length, 0 : HEADS * wide], ds_stack[0 : HEADS * wide, :])
    dk = mm(g_all[0:length, 0 : HEADS * wide], qs[0 : HEADS * wide, 0:128]) * LN2
    dq = jnp.concatenate(dq_t, axis=0).T[0:length, :] * SCALE
    return dq, dk, dv


def earlier(x):
    return jnp.concatenate([jnp.zeros_like(x[:1]), x[:-1]], axis=0)


def later(x):
    return jnp.concatenate([x[1:], jnp.zeros_like(x[:1])], axis=0)


def row_neighbours(x):
    groups = x.reshape(STRIPE * WG, GROUP, 128)
    place = iota(groups.shape, 1)
    edge = jnp.zeros((STRIPE, 1, GROUP, 128), x.dtype)
    far = pltpu.roll(groups, 2, 1).reshape(STRIPE, WG, GROUP, 128)
    far = jnp.concatenate([edge, far[:, :-1]], axis=1).reshape(groups.shape)
    left = jnp.where(place == 0, far, pltpu.roll(groups, 1, 1))
    far = pltpu.roll(groups, 6, 1).reshape(STRIPE, WG, GROUP, 128)
    far = jnp.concatenate([far[:, 1:], edge], axis=1).reshape(groups.shape)
    right = jnp.where(place == 6, far, pltpu.roll(groups, 7, 1))
    shape = (STRIPE, WG * GROUP, 128)
    return left.reshape(shape), x.reshape(shape), right.reshape(shape)


def col_neighbours(x):
    cells = x.reshape(HP, GROUP, 128)
    return pltpu.roll(cells, 1, 1), cells, pltpu.roll(cells, 7, 1)


def position(near, taps):
    rows = [sum(taps[3 * a + b] * near[b] for b in range(3)) for a in range(3)]
    return earlier(rows[0]) + rows[1] + later(rows[2])


def position_back(near, taps):
    rows = [sum(taps[3 * a + b] * near[2 - b] for b in range(3)) for a in range(3)]
    return later(rows[0]) + rows[1] + earlier(rows[2])


def tap_sums(da, near):
    sums = []
    for a in range(3):
        for b in range(3):
            x = near[b]
            x = earlier(x) if a == 0 else later(x) if a == 2 else x
            sums.append(colsum((da * x).reshape(-1, 128)))
    return sums


def forward_layer(l, h, w, wt, r):
    vec = wt.vec[l].astype(F32)

    def project(s, carry):
        rows = span(s, CHUNK)
        xhat, rate = norm_parts(r.x[l, rows, :])
        n1 = (xhat * vec[0:1] + vec[1:2]).astype(BF)
        r.n1[l, rows, :] = n1
        live = rows_live(s, h, w, 256)
        mixed = mm(n1, wt.qkv[l])
        q = (mixed[:, 0:256] + vec[2:3]) * (SCALE * LOG2E)
        k = mixed[:, 256:512]
        v = (mixed[:, 512:768] + vec[3:4]) * live
        for i, part in enumerate((q, k, v)):
            r.row[i, l, rows, :] = part[:, 0:128].astype(BF)
            cells = part[:, 128:256].reshape(STRIPE, WG, GROUP, 128)
            for c in range(STRIPE):
                r.turn[i, :, s * STRIPE + c] = cells[c]
        return carry

    lax.fori_loop(0, HP // STRIPE, project, 0)

    def horizontal(s, carry):
        rows = span(s, CHUNK)
        q, k, v = (r.row[i, l, rows, :] for i in range(3))
        attend(q, with_mask(k, rows_live(s, h, w, 128)), v, r.qs_r, r.o_r.at[l], r.lse_r.at[l], s, WIDE_R)
        near = row_neighbours(v.astype(F32))
        taps = vec[9:18, 0:128]
        pos = position(near, [taps[i : i + 1] for i in range(9)]) + vec[8:9, 0:128]
        o = r.o_r[l, s].T[0:CHUNK, :]
        r.a[l, rows, 0:128] = (o + pos.reshape(CHUNK, 128)).astype(BF)
        return carry

    lax.fori_loop(0, HP // STRIPE, horizontal, 0)

    def vertical(s, carry):
        q, k, v = (r.turn[i, s].reshape(TALL, 128).astype(BF) for i in range(3))
        for i, part in enumerate((q, k, v)):
            r.col[i, l, s] = part
        attend(q, with_mask(k, cols_live(s, h, w, 128)), v, r.qs_c, r.o_c.at[l], r.lse_c.at[l], s, WIDE_C)
        near = col_neighbours(v.astype(F32))
        taps = vec[9:18, 128:256]
        pos = position(near, [taps[i : i + 1] for i in range(9)]) + vec[8:9, 128:256]
        o = r.o_c[l, s].T[0:TALL, :]
        r.back[0, :, s] = o.reshape(HP, GROUP, 128) + pos
        return carry

    lax.fori_loop(0, WG, vertical, 0)

    def feed(s, carry):
        rows = span(s, CHUNK)
        turned = r.back[0, pl.ds(s * STRIPE, STRIPE)].reshape(CHUNK, 128).astype(BF)
        r.a[l, rows, 128:256] = turned
        x1 = r.x[l, rows, :] + mm(r.a[l, rows, :], wt.proj[l]) + vec[4:5]
        r.after[l, rows, :] = x1
        xhat, rate = norm_parts(x1)
        n2 = (xhat * vec[5:6] + vec[6:7]).astype(BF)
        r.n2[l, rows, :] = n2
        hidden_bias = jnp.concatenate([vec[18 + j : 19 + j] for j in range(4)], axis=1)
        hid = mm(n2, wt.fc1[l]) + hidden_bias
        phi = 0.5 * lax.erf(hid * 0.7071067811865476) + 0.5
        slope = phi + hid * (jnp.exp2(hid * hid * (-0.5 * LOG2E)) * 0.3989422804014327)
        act = (hid * phi).astype(BF)
        r.act[l, rows, :] = act
        r.slope[l, rows, :] = slope.astype(BF)
        r.x[l + 1, rows, :] = x1 + mm(act, wt.fc2[l]) + vec[7:8]
        return carry

    lax.fori_loop(0, HP // STRIPE, feed, 0)


def backward_layer(l, h, w, wt, r, out):
    vec = wt.vec[l].astype(F32)
    r.gv[...] = jnp.zeros_like(r.gv)

    def add(row, value):
        r.gv[row : row + 1, :] += value

    def feed(s, carry):
        rows = span(s, CHUNK)
        g = r.g[rows, :]
        add(7, colsum(g))
        gy = g.astype(BF)
        r.gy[rows, :] = gy
        d_hid = mm(gy, wt.fc2[l], NT) * r.slope[l, rows, :].astype(F32)
        for j in range(4):
            add(18 + j, colsum(d_hid[:, 256 * j : 256 * (j + 1)]))
        dh = d_hid.astype(BF)
        r.dh[rows, :] = dh
        d_n2 = mm(dh, wt.fc1[l], NT)
        xhat, rate = norm_parts(r.after[l, rows, :])
        add(5, colsum(d_n2 * xhat))
        add(6, colsum(d_n2))
        g1 = g + norm_back(d_n2, xhat, rate, vec[5:6])
        r.g[rows, :] = g1
        add(4, colsum(g1))
        g1_low = g1.astype(BF)
        r.g1[rows, :] = g1_low
        da = mm(g1_low, wt.proj[l], NT)
        r.da_r[rows, :] = da[:, 0:128].astype(BF)
        add(8, colsum(da.astype(BF).astype(F32)))
        cells = da[:, 128:256].reshape(STRIPE, WG, GROUP, 128)
        for c in range(STRIPE):
            r.turn[0, :, s * STRIPE + c] = cells[c]
        return carry

    lax.fori_loop(0, HP // STRIPE, feed, 0)
    out.fc2[l] = mm(r.act[l], r.gy[...], TN).astype(BF)
    out.fc1[l] = mm(r.n2[l], r.dh[...], TN).astype(BF)
    out.proj[l] = mm(r.a[l], r.g1[...], TN).astype(BF)

    def horizontal(s, carry):
        rows = span(s, CHUNK)
        q, k, v = (r.row[i, l, rows, :] for i in range(3))
        da = r.da_r[rows, :]
        live = rows_live(s, h, w, 128)
        dq, dk, dv = attend_back(
            q, k, with_mask(k, live), v, da, r.qs_r, r.ds_r, r.p_all, r.g_all,
            r.o_r.at[l], r.lse_r.at[l], s, WIDE_R,
        )
        taps = [vec[9 + i : 10 + i, 0:128] for i in range(9)]
        da_near = row_neighbours(da.astype(F32))
        dv = (dv + position_back(da_near, taps).reshape(CHUNK, 128)) * live
        sums = tap_sums(da_near[1], row_neighbours(v.astype(F32)))
        for i in range(9):
            r.gv[9 + i : 10 + i, 0:128] += sums[i]
        r.gv[2:3, 0:128] += colsum(dq)
        r.gv[3:4, 0:128] += colsum(dv)
        for i, part in enumerate((dq, dk, dv)):
            r.dqkv[rows, 256 * i : 256 * i + 128] = part.astype(BF)
        return carry

    lax.fori_loop(0, HP // STRIPE, horizontal, 0)

    def vertical(s, carry):
        q, k, v = (r.col[i, l, s] for i in range(3))
        da = r.turn[0, s].reshape(TALL, 128).astype(BF)
        live = cols_live(s, h, w, 128)
        dq, dk, dv = attend_back(
            q, k, with_mask(k, live), v, da, r.qs_c, r.ds_c, r.p_all, r.g_all,
            r.o_c.at[l], r.lse_c.at[l], s, WIDE_C,
        )
        taps = [vec[9 + i : 10 + i, 128:256] for i in range(9)]
        da_near = col_neighbours(da.astype(F32))
        dv = (dv + position_back(da_near, taps).reshape(TALL, 128)) * live
        sums = tap_sums(da_near[1], col_neighbours(v.astype(F32)))
        for i in range(9):
            r.gv[9 + i : 10 + i, 128:256] += sums[i]
        r.gv[2:3, 128:256] += colsum(dq)
        r.gv[3:4, 128:256] += colsum(dv)
        for i, part in enumerate((dq, dk, dv)):
            r.back[i, :, s] = part.reshape(HP, GROUP, 128)
        return carry

    lax.fori_loop(0, WG, vertical, 0)

    def mix(s, carry):
        rows = span(s, CHUNK)
        for i in range(3):
            turned = r.back[i, pl.ds(s * STRIPE, STRIPE)].reshape(CHUNK, 128)
            r.dqkv[rows, 256 * i + 128 : 256 * i + 256] = turned.astype(BF)
        d_n1 = mm(r.dqkv[rows, :], wt.qkv[l], NT)
        xhat, rate = norm_parts(r.x[l, rows, :])
        add(0, colsum(d_n1 * xhat))
        add(1, colsum(d_n1))
        r.g[rows, :] += norm_back(d_n1, xhat, rate, vec[0:1])
        return carry

    lax.fori_loop(0, HP // STRIPE, mix, 0)
    out.qkv[l] = mm(r.n1[l], r.dqkv[...], TN).astype(BF)
    out.vec[l] = r.gv[...].astype(BF)


SCRATCH = dict(
    x=((3, ROWS, 256), F32),
    after=((2, ROWS, 256), F32),
    n1=((2, ROWS, 256), BF),
    n2=((2, ROWS, 256), BF),
    a=((2, ROWS, 256), BF),
    act=((2, ROWS, 1024), BF),
    slope=((2, ROWS, 1024), BF),
    row=((3, 2, ROWS, 128), BF),
    col=((3, 2, WG, TALL, 128), BF),
    turn=((3, WG, HP, GROUP, 128), F32),
    back=((3, HP, WG, GROUP, 128), F32),
    o_r=((2, HP // STRIPE, 128, WIDE_R), F32),
    o_c=((2, WG, 128, WIDE_C), F32),
    lse_r=((2, HP // STRIPE, 8, WIDE_R), F32),
    lse_c=((2, WG, 8, WIDE_C), F32),
    qs_r=((HEADS * WIDE_R, 256), BF),
    qs_c=((HEADS * WIDE_C, 256), BF),
    ds_r=((HEADS * WIDE_R, 128), BF),
    ds_c=((HEADS * WIDE_C, 128), BF),
    p_all=((CHUNK, HEADS * WIDE_R), BF),
    g_all=((CHUNK, HEADS * WIDE_R), BF),
    g=((ROWS, 256), F32),
    gy=((ROWS, 256), BF),
    g1=((ROWS, 256), BF),
    dh=((ROWS, 1024), BF),
    da_r=((ROWS, 128), BF),
    dqkv=((ROWS, 768), BF),
    gv=((24, 256), F32),
)


class Refs:
    def __init__(self, names, refs):
        self.__dict__.update(zip(names, refs))


WEIGHTS = ("qkv", "proj", "fc1", "fc2", "vec")


def step_kernel(*refs):
    h_ref, w_ref, tok, cot = refs[:4]
    wt = Refs(WEIGHTS, refs[4:9])
    y_ref, gt_ref = refs[9:11]
    out = Refs(WEIGHTS, refs[11:16])
    r = Refs(SCRATCH, refs[16:])
    h, w = h_ref[0], w_ref[0]
    layers = wt.qkv.shape[0]
    for stack in (r.qs_r, r.qs_c):
        stack[...] = jnp.where(iota(stack.shape, 1) == 128, 1.0, 0.0).astype(BF)
    for stack in (r.ds_r, r.ds_c):
        stack[...] = jnp.zeros_like(stack)
    pad_groups(tok, r.x.at[0])
    pad_groups(cot, r.g)

    def forward(l, carry):
        forward_layer(l, h, w, wt, r)
        return carry

    lax.fori_loop(0, layers, forward, 0)
    drop_groups(r.x.at[layers], y_ref)

    def backward(i, carry):
        backward_layer(layers - 1 - i, h, w, wt, r, out)
        return carry

    lax.fori_loop(0, layers, backward, 0)
    drop_groups(r.g, gt_ref)


def local_step(heights, widths, tokens, cotangent, full):
    vmem = pl.BlockSpec(memory_space=pltpu.VMEM)
    smem = pl.BlockSpec(memory_space=pltpu.SMEM)
    count, width = tokens.shape
    layers = full[0].shape[0]
    shapes = [jax.ShapeDtypeStruct((count, width), F32)] * 2
    shapes += [jax.ShapeDtypeStruct(m.shape, BF) for m in full[:4]]
    shapes += [jax.ShapeDtypeStruct((layers, 24, width), BF)]
    return pl.pallas_call(
        step_kernel,
        out_shape=shapes,
        in_specs=[smem, smem, vmem, vmem] + [vmem] * 5,
        out_specs=[vmem] * 7,
        scratch_shapes=[pltpu.VMEM(s, d) for s, d in SCRATCH.values()],
        compiler_params=pltpu.CompilerParams(vmem_limit_bytes=67043328),
    )(heights, widths, tokens, cotangent, *full)


MESH = pl.DeviceIdType.MESH


class Grid:
    def __init__(self, shards, copies):
        self.cores = 2
        self.zs = 4
        self.xs = shards // 8
        self.copies = copies
        index = lax.axis_index("fsdp")
        self.rep = lax.axis_index("rep")
        self.core = lax.rem(index, 2)
        chip = lax.div(index, 2)
        self.x = lax.rem(chip, self.xs)
        self.z = lax.div(chip, self.xs)

    def at(self, z, x, core):
        return {"fsdp": (z * self.xs + x) * 2 + core, "rep": self.rep}

    def z_peers(self):
        return [(d, lax.rem(self.z + d, self.zs)) for d in range(1, self.zs)]

    def x_peers(self):
        return [(d, lax.rem(self.x + d, self.xs)) for d in range(1, self.xs)]

    def rep_peers(self):
        return [(d, lax.rem(self.rep + d, self.copies)) for d in range(1, self.copies)]

    def z_device(self, z):
        return self.at(z, self.x, self.core)

    def x_device(self, x):
        return self.at(self.z, x, self.core)

    def sibling(self):
        return self.at(self.z, self.x, 1 - self.core)

    def rep_device(self, rep):
        index = (self.z * self.xs + self.x) * 2 + self.core
        return {"fsdp": index, "rep": rep}

    def steps(self):
        return self.zs - 1 + self.xs - 1 + 1

    def greet(self, copies):
        devices = [self.z_device(z) for _, z in self.z_peers()]
        devices += [self.x_device(x) for _, x in self.x_peers()] + [self.sibling()]
        if copies:
            devices += [self.rep_device(rep) for _, rep in self.rep_peers()]
        barrier = pltpu.get_barrier_semaphore()
        for device in devices:
            pl.semaphore_signal(barrier, inc=1, device_id=device, device_id_type=MESH)
        pl.semaphore_wait(barrier, len(devices))


def remote(src, dst, send, recv, device):
    return pltpu.make_async_remote_copy(
        src_ref=src, dst_ref=dst, send_sem=send, recv_sem=recv,
        device_id=device, device_id_type=MESH,
    )


class Gather:
    def __init__(self, grid, own, full, sems, row):
        self.grid, self.own, self.full = grid, own, full
        send, recv, local = sems
        g = grid
        mine = full.at[g.z, g.x, g.core]
        self.keep = pltpu.make_async_copy(own, mine, local.at[row])
        self.along_z = [
            remote(own, mine, send.at[row, d - 1], recv.at[row, d - 1], g.z_device(z))
            for d, z in g.z_peers()
        ]
        base = g.zs - 2
        lane = full.at[:, g.x, g.core]
        self.along_x = [
            remote(lane, lane, send.at[row, base + d], recv.at[row, base + d], g.x_device(x))
            for d, x in g.x_peers()
        ]
        last = g.zs - 1 + g.xs - 1
        plane = full.at[:, :, g.core]
        self.across = remote(plane, plane, send.at[row, last], recv.at[row, last], g.sibling())

    def begin(self):
        self.keep.start()
        for copy in self.along_z:
            copy.start()

    def second(self):
        self.keep.wait()
        for copy in self.along_z:
            copy.wait_recv()
        for copy in self.along_x:
            copy.start()

    def third(self):
        for copy in self.along_x:
            copy.wait_recv()
        self.across.start()

    def finish(self):
        self.across.wait_recv()

    def drain(self):
        for copy in self.along_z + self.along_x + [self.across]:
            copy.wait_send()


class Reduce:
    def __init__(self, grid, part, bufs, out, sems, row):
        self.grid, self.part, self.out = grid, part, out
        send, recv = sems
        g = grid
        self.from_sibling, self.chip, self.from_x, self.line, self.from_z, self.own, self.from_rep = bufs
        self.across = remote(
            part.at[:, :, 1 - g.core], self.from_sibling, send.at[row, 0], recv.at[row, 0], g.sibling()
        )
        self.along_x = [
            remote(self.chip.at[:, x], self.from_x.at[d - 1], send.at[row, d], recv.at[row, d], g.x_device(x))
            for d, x in g.x_peers()
        ]
        base = g.xs - 1
        self.along_z = [
            remote(self.line.at[z], self.from_z.at[d - 1], send.at[row, base + d], recv.at[row, base + d], g.z_device(z))
            for d, z in g.z_peers()
        ]
        base += g.zs - 1
        self.along_rep = [
            remote(self.own, self.from_rep.at[d - 1], send.at[row, base + d], recv.at[row, base + d], g.rep_device(rep))
            for d, rep in g.rep_peers()
        ]

    def begin(self):
        self.across.start()

    def second(self):
        self.across.wait_recv()
        mine = self.part[:, :, self.grid.core].astype(F32)
        self.chip[...] = (mine + self.from_sibling[...].astype(F32)).astype(BF)
        for copy in self.along_x:
            copy.start()

    def third(self):
        for copy in self.along_x:
            copy.wait_recv()
        total = self.chip[:, self.grid.x].astype(F32)
        for d, _ in self.grid.x_peers():
            total = total + self.from_x[d - 1].astype(F32)
        self.line[...] = total.astype(BF)
        for copy in self.along_z:
            copy.start()

    def fourth(self):
        for copy in self.along_z:
            copy.wait_recv()
        total = self.line[self.grid.z].astype(F32)
        for d, _ in self.grid.z_peers():
            total = total + self.from_z[d - 1].astype(F32)
        self.own[...] = total.astype(BF)
        for copy in self.along_rep:
            copy.start()

    def finish(self):
        for copy in self.along_rep:
            copy.wait_recv()
        total = self.own[...].astype(F32)
        for d, _ in self.grid.rep_peers():
            total = total + self.from_rep[d - 1].astype(F32)
        self.out[...] = total

    def drain(self):
        for copy in [self.across] + self.along_x + self.along_z + self.along_rep:
            copy.wait_send()


def reduce_bufs(zs, xs, copies, shape):
    dims = [(zs, xs), (zs, xs), (max(xs - 1, 1), zs), (zs,), (zs - 1,), (), (max(copies - 1, 1),)]
    return [pltpu.VMEM(d + tuple(shape), BF) for d in dims]


def gather_kernel(shards, copies, count, *refs):
    own, full, sems = refs[:count], refs[count : 2 * count], refs[2 * count :]
    g = Grid(shards, copies)
    g.greet(False)
    parts = [Gather(g, own[i], full[i], sems, i) for i in range(count)]
    for move in ("begin", "second", "third", "finish", "drain"):
        for part in parts:
            getattr(part, move)()


def gather_all(own, shards, copies):
    count = len(own)
    vmem = pl.BlockSpec(memory_space=pltpu.VMEM)
    lead = (4, shards // 8, 2)
    steps = lead[0] - 1 + lead[1] - 1 + 1
    return pl.pallas_call(
        functools.partial(gather_kernel, shards, copies, count),
        out_shape=[jax.ShapeDtypeStruct(lead + o.shape, o.dtype) for o in own],
        in_specs=[vmem] * count,
        out_specs=[vmem] * count,
        scratch_shapes=[
            pltpu.SemaphoreType.DMA((count, steps)),
            pltpu.SemaphoreType.DMA((count, steps)),
            pltpu.SemaphoreType.DMA((count,)),
        ],
        compiler_params=pltpu.CompilerParams(
            collective_id=0, has_side_effects=True, vmem_limit_bytes=67043328
        ),
    )(*own)


def reduce_kernel(shards, copies, count, *refs):
    parts, outs = refs[:count], refs[count : 2 * count]
    bufs = refs[2 * count : 2 * count + 7 * count]
    sems = refs[9 * count :]
    g = Grid(shards, copies)
    g.greet(True)
    sums = [
        Reduce(g, parts[i], bufs[7 * i : 7 * i + 7], outs[i], sems, i) for i in range(count)
    ]
    for move in ("begin", "second", "third", "fourth", "finish", "drain"):
        for one in sums:
            getattr(one, move)()


def reduce_all(parts, shards, copies):
    count = len(parts)
    vmem = pl.BlockSpec(memory_space=pltpu.VMEM)
    zs, xs = 4, shards // 8
    steps = 1 + xs - 1 + zs - 1 + copies - 1
    scratch = []
    for p in parts:
        scratch += reduce_bufs(zs, xs, copies, p.shape[3:])
    return pl.pallas_call(
        functools.partial(reduce_kernel, shards, copies, count),
        out_shape=[jax.ShapeDtypeStruct(p.shape[3:], F32) for p in parts],
        in_specs=[vmem] * count,
        out_specs=[vmem] * count,
        scratch_shapes=scratch
        + [pltpu.SemaphoreType.DMA((count, steps)), pltpu.SemaphoreType.DMA((count, steps))],
        compiler_params=pltpu.CompilerParams(
            collective_id=1, has_side_effects=True, vmem_limit_bytes=67043328
        ),
    )(*parts)


def shards_step(shards, copies, tokens, heights, widths, w_qkv, w_proj, w_fc1, w_fc2, vectors, cotangent):
    layers = w_qkv.shape[0]
    vec_own = vectors.astype(F32).transpose(0, 2, 1)
    gathered = gather_all([w_qkv, w_proj, w_fc1, w_fc2, vec_own], shards, copies)
    full = []
    for i, m in enumerate(gathered):
        m = m.reshape((shards,) + m.shape[3:]).transpose(1, 0, 2, 3)
        full.append(m.reshape(layers, -1, m.shape[-1]))
    full[4] = full[4].transpose(0, 2, 1).astype(BF)
    y, gt, *grads = local_step(heights, widths, tokens, cotangent, full)
    lead = (4, shards // 8, 2)
    parts = []
    grads[4] = grads[4].transpose(0, 2, 1)
    for m in grads:
        m = m.reshape(layers, shards, -1, m.shape[-1]).transpose(1, 0, 2, 3)
        parts.append(m.reshape(lead + m.shape[1:]))
    sums = reduce_all(parts, shards, copies)
    vec = sums[4].transpose(0, 2, 1)[:, : vectors.shape[1]]
    return (y, gt, *sums[:4], vec)


def solution(mesh):
    from jax.sharding import PartitionSpec as P

    images = P(("fsdp", "rep"), None)
    weights = P(None, "fsdp", None)
    return jax.shard_map(
        functools.partial(shards_step, mesh.shape["fsdp"], mesh.shape["rep"]),
        mesh=mesh,
        in_specs=(images, P(("fsdp", "rep")), P(("fsdp", "rep")), weights, weights, weights, weights, P(None, None, "fsdp"), images),
        out_specs=(images, images, weights, weights, weights, weights, P(None, None, "fsdp")),
        check_vma=False,
    )
```

```python
import functools
import jax
import jax.numpy as jnp
from jax import lax
from jax.experimental import pallas as pl
from jax.experimental.pallas import tpu as pltpu
from jax.sharding import PartitionSpec as P

HEAD = 32
STRIPE = 7
HP = 28
WP = 42
HEADS = 4
GROUP = 8
WG = WP // STRIPE
ROWS = HP * WG * GROUP
CHUNK = STRIPE * WG * GROUP
TALL = HP * GROUP
WIDE_R = 384
WIDE_C = 256
BF = jnp.bfloat16
F32 = jnp.float32
eps_norm = 1e-05
masked_score = -1000000000.0
LOG2E = 1.4426950408889634
LN2 = 0.6931471805599453
SCALE = HEAD ** (-0.5)
NN = (((1,), (0,)), ((), ()))
NT = (((1,), (1,)), ((), ()))
TN = (((0,), (0,)), ((), ()))


def mm(a, b, dims=NN):
    return lax.dot_general(a, b, dims, preferred_element_type=F32)


def iota(shape, dim):
    return lax.broadcasted_iota(jnp.int32, shape, dim)


def span(index, size):
    return pl.ds(pl.multiple_of(index * size, size), size)


def pad_groups(src, dst, scale=None):
    def body(j, carry):
        block = src[pl.ds(pl.multiple_of(j * 56, 8), 56), :].astype(F32).reshape(7, 8, -1)
        place = iota((8, block.shape[-1]), 0)
        for u in range(8):
            if u == 0:
                group = block[0]
            elif u == 7:
                group = pltpu.roll(block[6], 7, 0)
            else:
                group = jnp.where(
                    place < u, pltpu.roll(block[u - 1], u, 0), pltpu.roll(block[u], u, 0)
                )
            group = jnp.where(place < 7, group, 0.0)
            dst[pl.ds(pl.multiple_of(j * 64 + u * 8, 8), 8), :] = group
        return carry

    lax.fori_loop(0, ROWS // 64, body, 0)


def drop_groups(src, dst):
    def body(j, carry):
        block = src[pl.ds(pl.multiple_of(j * 64, 8), 64), :].reshape(8, 8, -1)
        place = iota((8, block.shape[-1]), 0)
        for t in range(7):
            lower = block[t] if t == 0 else pltpu.roll(block[t], 8 - t, 0)
            upper = pltpu.roll(block[t + 1], 7 - t, 0)
            dst[pl.ds(pl.multiple_of(j * 56 + t * 8, 8), 8), :] = jnp.where(
                place <= 6 - t, lower, upper
            )
        return carry

    lax.fori_loop(0, ROWS // 64, body, 0)


def norm_parts(x):
    centre = jnp.mean(x, axis=-1, keepdims=True)
    centred = x - centre
    rate = lax.rsqrt(jnp.mean(centred * centred, axis=-1, keepdims=True) + eps_norm)
    return centred * rate, rate


def norm_back(d_n, xhat, rate, gain):
    e = d_n * gain
    return rate * (
        e
        - jnp.mean(e, axis=-1, keepdims=True)
        - xhat * jnp.mean(e * xhat, axis=-1, keepdims=True)
    )


def colsum(x):
    return jnp.sum(x, axis=0, keepdims=True)


def rows_live(stripe, h, w, lanes):
    shape = (STRIPE, WG * GROUP, lanes)
    row = iota(shape, 0) + stripe * STRIPE
    place = iota(shape, 1)
    within = place & 7
    col = (place >> 3) * STRIPE + within
    live = (row < h) & (col < w) & (within < STRIPE)
    return jnp.where(live, 1.0, 0.0).reshape(CHUNK, lanes)


def cols_live(stripe, h, w, lanes):
    shape = (HP, GROUP, lanes)
    row = iota(shape, 0)
    within = iota(shape, 1)
    live = (row < h) & (within + stripe * STRIPE < w) & (within < STRIPE)
    return jnp.where(live, 1.0, 0.0).reshape(TALL, lanes)


def with_mask(keys, live):
    lane = iota(live.shape, 1)
    extra = jnp.where(lane == 0, jnp.where(live > 0.0, 0.0, masked_score), 0.0)
    return jnp.concatenate([keys, extra.astype(BF)], axis=-1)


def stack_heads(ref, x, wide):
    length = x.shape[0]
    lane = iota(x.shape, 1)
    for h in range(HEADS):
        kept = jnp.where((lane >> 5) == h, x, jnp.zeros_like(x))
        ref[h * wide : h * wide + length, 0:128] = kept


def widen(x, wide):
    length = x.shape[0]
    return jnp.concatenate([x, jnp.zeros((wide - length, x.shape[1]), x.dtype)], axis=0)


def attend(q, k_mask, vm, qs, out_t, lse, stripe, wide):
    length = q.shape[0]
    stack_heads(qs, q, wide)
    scores = mm(k_mask, qs[0 : HEADS * wide, :], NT)
    v_t = widen(vm.astype(F32), wide).T.astype(BF)[:, 0:length]
    for h in range(HEADS):
        s = scores[:, h * wide : (h + 1) * wide]
        top = jnp.max(s, axis=0, keepdims=True)
        p = jnp.exp2(s - top)
        total = jnp.sum(p, axis=0, keepdims=True)
        o = mm(v_t[HEAD * h : HEAD * (h + 1), :], p.astype(BF))
        out_t[stripe, HEAD * h : HEAD * (h + 1), :] = o / total
        lse[stripe, h : h + 1, :] = top + jnp.log2(total)


def attend_back(q, k, k_mask, vm, da, qs, ds_stack, p_all, g_all, out_t, lse, stripe, wide):
    length = q.shape[0]
    stack_heads(qs, q, wide)
    stack_heads(ds_stack, da, wide)
    da_t = widen(da.astype(F32), wide).T
    k_t = widen(k.astype(F32), wide).T.astype(BF)[:, 0:length]
    weighted = da_t * out_t[stripe]
    dq_t = []
    scores = mm(k_mask, qs[0 : HEADS * wide, :], NT)
    d_probs = mm(vm, ds_stack[0 : HEADS * wide, :], NT)
    for h in range(HEADS):
        lanes = slice(h * wide, (h + 1) * wide)
        inner = jnp.sum(weighted[HEAD * h : HEAD * (h + 1), :], axis=0, keepdims=True)
        p = jnp.exp2(scores[:, lanes] - lse[stripe, h : h + 1, :])
        g = (p * (d_probs[:, lanes] - inner)).astype(BF)
        p_all[0:length, lanes] = p.astype(BF)
        g_all[0:length, lanes] = g
        dq_t.append(mm(k_t[HEAD * h : HEAD * (h + 1), :], g))
    dv = mm(p_all[0:length, 0 : HEADS * wide], ds_stack[0 : HEADS * wide, :])
    dk = mm(g_all[0:length, 0 : HEADS * wide], qs[0 : HEADS * wide, 0:128]) * LN2
    dq = jnp.concatenate(dq_t, axis=0).T[0:length, :] * SCALE
    return dq, dk, dv


def earlier(x):
    return jnp.concatenate([jnp.zeros_like(x[:1]), x[:-1]], axis=0)


def later(x):
    return jnp.concatenate([x[1:], jnp.zeros_like(x[:1])], axis=0)


def row_neighbours(x):
    groups = x.reshape(STRIPE * WG, GROUP, 128)
    place = iota(groups.shape, 1)
    edge = jnp.zeros((STRIPE, 1, GROUP, 128), x.dtype)
    far = pltpu.roll(groups, 2, 1).reshape(STRIPE, WG, GROUP, 128)
    far = jnp.concatenate([edge, far[:, :-1]], axis=1).reshape(groups.shape)
    left = jnp.where(place == 0, far, pltpu.roll(groups, 1, 1))
    far = pltpu.roll(groups, 6, 1).reshape(STRIPE, WG, GROUP, 128)
    far = jnp.concatenate([far[:, 1:], edge], axis=1).reshape(groups.shape)
    right = jnp.where(place == 6, far, pltpu.roll(groups, 7, 1))
    shape = (STRIPE, WG * GROUP, 128)
    return left.reshape(shape), x.reshape(shape), right.reshape(shape)


def col_neighbours(x):
    cells = x.reshape(HP, GROUP, 128)
    return pltpu.roll(cells, 1, 1), cells, pltpu.roll(cells, 7, 1)


def position(near, taps):
    rows = [sum(taps[3 * a + b] * near[b] for b in range(3)) for a in range(3)]
    return earlier(rows[0]) + rows[1] + later(rows[2])


def position_back(near, taps):
    rows = [sum(taps[3 * a + b] * near[2 - b] for b in range(3)) for a in range(3)]
    return later(rows[0]) + rows[1] + earlier(rows[2])


def tap_sums(da, near):
    sums = []
    for a in range(3):
        for b in range(3):
            x = near[b]
            x = earlier(x) if a == 0 else later(x) if a == 2 else x
            sums.append(colsum((da * x).reshape(-1, 128)))
    return sums


def forward_layer(l, h, w, wt, r, at):
    vec = r.vec[l]

    def project(s, carry):
        rows = span(s, CHUNK)
        xhat, rate = norm_parts(r.x[l, rows, :])
        n1 = (xhat * vec[0:1] + vec[1:2]).astype(BF)
        r.n1[l, rows, :] = n1
        live = rows_live(s, h, w, 256)
        mixed = mm(n1, wt.qkv(l))
        q = (mixed[:, 0:256] + vec[2:3]) * (SCALE * LOG2E)
        k = mixed[:, 256:512]
        v = (mixed[:, 512:768] + vec[3:4]) * live
        for i, part in enumerate((q, k, v)):
            r.row[i, l, rows, :] = part[:, 0:128].astype(BF)
            cells = part[:, 128:256].reshape(STRIPE, WG, GROUP, 128)
            for c in range(STRIPE):
                r.turn[i, :, s * STRIPE + c] = cells[c]
        return carry

    lax.fori_loop(0, HP // STRIPE, project, 0)
    at("projected", l)

    def horizontal(s, carry):
        rows = span(s, CHUNK)
        q, k, v = (r.row[i, l, rows, :] for i in range(3))
        attend(q, with_mask(k, rows_live(s, h, w, 128)), v, r.qs_r, r.o_r.at[l], r.lse_r.at[l], s, WIDE_R)
        near = row_neighbours(v.astype(F32))
        taps = vec[9:18, 0:128]
        pos = position(near, [taps[i : i + 1] for i in range(9)]) + vec[8:9, 0:128]
        o = r.o_r[l, s].T[0:CHUNK, :]
        r.a[l, rows, 0:128] = (o + pos.reshape(CHUNK, 128)).astype(BF)
        return carry

    lax.fori_loop(0, HP // STRIPE, horizontal, 0)
    at("horizontal", l)

    def vertical(s, carry):
        q, k, v = (r.turn[i, s].reshape(TALL, 128).astype(BF) for i in range(3))
        for i, part in enumerate((q, k, v)):
            r.col[i, l, s] = part
        attend(q, with_mask(k, cols_live(s, h, w, 128)), v, r.qs_c, r.o_c.at[l], r.lse_c.at[l], s, WIDE_C)
        near = col_neighbours(v.astype(F32))
        taps = vec[9:18, 128:256]
        pos = position(near, [taps[i : i + 1] for i in range(9)]) + vec[8:9, 128:256]
        o = r.o_c[l, s].T[0:TALL, :]
        r.back[0, :, s] = o.reshape(HP, GROUP, 128) + pos
        return carry

    lax.fori_loop(0, WG, vertical, 0)
    at("vertical", l)

    def feed(s, carry):
        rows = span(s, CHUNK)
        turned = r.back[0, pl.ds(s * STRIPE, STRIPE)].reshape(CHUNK, 128).astype(BF)
        r.a[l, rows, 128:256] = turned
        x1 = r.x[l, rows, :] + mm(r.a[l, rows, :], wt.proj(l)) + vec[4:5]
        r.after[l, rows, :] = x1
        xhat, rate = norm_parts(x1)
        n2 = (xhat * vec[5:6] + vec[6:7]).astype(BF)
        r.n2[l, rows, :] = n2
        hidden_bias = jnp.concatenate([vec[18 + j : 19 + j] for j in range(4)], axis=1)
        hid = mm(n2, wt.fc1(l)) + hidden_bias
        phi = 0.5 * lax.erf(hid * 0.7071067811865476) + 0.5
        slope = phi + hid * (jnp.exp2(hid * hid * (-0.5 * LOG2E)) * 0.3989422804014327)
        act = (hid * phi).astype(BF)
        r.act[l, rows, :] = act
        r.slope[l, rows, :] = slope.astype(BF)
        r.x[l + 1, rows, :] = x1 + mm(act, wt.fc2(l)) + vec[7:8]
        return carry

    lax.fori_loop(0, HP // STRIPE, feed, 0)
    at("fed", l)


def backward_layer(l, h, w, wt, r, out, at):
    vec = r.vec[l]
    r.gv[...] = jnp.zeros_like(r.gv)

    def add(row, value):
        r.gv[row : row + 1, :] += value

    def feed(s, carry):
        rows = span(s, CHUNK)
        g = r.g[rows, :]
        add(7, colsum(g))
        gy = g.astype(BF)
        r.gy[rows, :] = gy
        d_hid = mm(gy, wt.fc2(l), NT) * r.slope[l, rows, :].astype(F32)
        for j in range(4):
            add(18 + j, colsum(d_hid[:, 256 * j : 256 * (j + 1)]))
        dh = d_hid.astype(BF)
        r.slope[l, rows, :] = dh
        d_n2 = mm(dh, wt.fc1(l), NT)
        xhat, rate = norm_parts(r.after[l, rows, :])
        add(5, colsum(d_n2 * xhat))
        add(6, colsum(d_n2))
        g1 = g + norm_back(d_n2, xhat, rate, vec[5:6])
        r.g[rows, :] = g1
        add(4, colsum(g1))
        g1_low = g1.astype(BF)
        r.g1[rows, :] = g1_low
        da = mm(g1_low, wt.proj(l), NT)
        r.da_r[rows, :] = da[:, 0:128].astype(BF)
        add(8, colsum(da.astype(BF).astype(F32)))
        cells = da[:, 128:256].reshape(STRIPE, WG, GROUP, 128)
        for c in range(STRIPE):
            r.turn[0, :, s * STRIPE + c] = cells[c]
        return carry

    lax.fori_loop(0, HP // STRIPE, feed, 0)
    at("back fed", l)
    out.put("fc2", l, mm(r.act[l], r.gy[...], TN))
    out.put("fc1", l, mm(r.n2[l], r.slope[l], TN))
    out.put("proj", l, mm(r.a[l], r.g1[...], TN))
    at("back summed", l)

    def horizontal(s, carry):
        rows = span(s, CHUNK)
        q, k, v = (r.row[i, l, rows, :] for i in range(3))
        da = r.da_r[rows, :]
        live = rows_live(s, h, w, 128)
        dq, dk, dv = attend_back(
            q, k, with_mask(k, live), v, da, r.qs_r, r.ds_r, r.p_all, r.g_all,
            r.o_r.at[l], r.lse_r.at[l], s, WIDE_R,
        )
        taps = [vec[9 + i : 10 + i, 0:128] for i in range(9)]
        da_near = row_neighbours(da.astype(F32))
        dv = (dv + position_back(da_near, taps).reshape(CHUNK, 128)) * live
        sums = tap_sums(da_near[1], row_neighbours(v.astype(F32)))
        for i in range(9):
            r.gv[9 + i : 10 + i, 0:128] += sums[i]
        r.gv[2:3, 0:128] += colsum(dq)
        r.gv[3:4, 0:128] += colsum(dv)
        for i, part in enumerate((dq, dk, dv)):
            r.dqkv_r[rows, 128 * i : 128 * i + 128] = part.astype(BF)
        return carry

    lax.fori_loop(0, HP // STRIPE, horizontal, 0)
    out.put("qkv_r", l, mm(r.n1[l], r.dqkv_r[...], TN))
    at("back horizontal", l)

    def vertical(s, carry):
        q, k, v = (r.col[i, l, s] for i in range(3))
        da = r.turn[0, s].reshape(TALL, 128).astype(BF)
        live = cols_live(s, h, w, 128)
        dq, dk, dv = attend_back(
            q, k, with_mask(k, live), v, da, r.qs_c, r.ds_c, r.p_all, r.g_all,
            r.o_c.at[l], r.lse_c.at[l], s, WIDE_C,
        )
        taps = [vec[9 + i : 10 + i, 128:256] for i in range(9)]
        da_near = col_neighbours(da.astype(F32))
        dv = (dv + position_back(da_near, taps).reshape(TALL, 128)) * live
        sums = tap_sums(da_near[1], col_neighbours(v.astype(F32)))
        for i in range(9):
            r.gv[9 + i : 10 + i, 128:256] += sums[i]
        r.gv[2:3, 128:256] += colsum(dq)
        r.gv[3:4, 128:256] += colsum(dv)
        for i, part in enumerate((dq, dk, dv)):
            r.back[i, :, s] = part.reshape(HP, GROUP, 128)
        return carry

    lax.fori_loop(0, WG, vertical, 0)

    def turn(s, carry):
        rows = span(s, CHUNK)
        for i in range(3):
            cells = r.back[i, pl.ds(s * STRIPE, STRIPE)].reshape(CHUNK, 128)
            r.dqkv_c[rows, 128 * i : 128 * i + 128] = cells.astype(BF)
        return carry

    lax.fori_loop(0, HP // STRIPE, turn, 0)
    out.put("qkv_c", l, mm(r.n1[l], r.dqkv_c[...], TN))
    at("back vertical", l)

    def mix(s, carry):
        rows = span(s, CHUNK)
        parts = []
        for i in range(3):
            lanes = slice(128 * i, 128 * i + 128)
            parts += [r.dqkv_r[rows, lanes], r.dqkv_c[rows, lanes]]
        d_n1 = mm(jnp.concatenate(parts, axis=1), wt.qkv(l), NT)
        xhat, rate = norm_parts(r.x[l, rows, :])
        add(0, colsum(d_n1 * xhat))
        add(1, colsum(d_n1))
        r.g[rows, :] += norm_back(d_n1, xhat, rate, vec[0:1])
        return carry

    lax.fori_loop(0, HP // STRIPE, mix, 0)
    out.put("vec", l, r.gv[...].T)
    at("back mixed", l)


MESH = pl.DeviceIdType.MESH


class Grid:
    def __init__(self, shards, copies):
        self.cores = 2
        self.zs = 4
        self.xs = shards // 8
        self.copies = copies
        index = lax.axis_index("fsdp")
        self.rep = lax.axis_index("rep")
        self.core = lax.rem(index, 2)
        chip = lax.div(index, 2)
        self.x = lax.rem(chip, self.xs)
        self.z = lax.div(chip, self.xs)

    def at(self, z, x, core):
        return {"fsdp": (z * self.xs + x) * 2 + core, "rep": self.rep}

    def z_peers(self):
        return [(d, lax.rem(self.z + d, self.zs)) for d in range(1, self.zs)]

    def x_peers(self):
        return [(d, lax.rem(self.x + d, self.xs)) for d in range(1, self.xs)]

    def rep_peers(self):
        return [(d, lax.rem(self.rep + d, self.copies)) for d in range(1, self.copies)]

    def z_device(self, z):
        return self.at(z, self.x, self.core)

    def x_device(self, x):
        return self.at(self.z, x, self.core)

    def sibling(self):
        return self.at(self.z, self.x, 1 - self.core)

    def rep_device(self, rep):
        index = (self.z * self.xs + self.x) * 2 + self.core
        return {"fsdp": index, "rep": rep}

    def steps(self):
        return self.zs - 1 + self.xs - 1 + 1

    def peers(self):
        devices = [self.z_device(z) for _, z in self.z_peers()]
        devices += [self.x_device(x) for _, x in self.x_peers()] + [self.sibling()]
        return devices + [self.rep_device(rep) for _, rep in self.rep_peers()]

    def signal(self):
        for device in self.peers():
            pl.semaphore_signal(
                pltpu.get_barrier_semaphore(), inc=1, device_id=device, device_id_type=MESH
            )

    def wait(self):
        pl.semaphore_wait(pltpu.get_barrier_semaphore(), len(self.peers()))


def remote(src, dst, send, recv, device):
    return pltpu.make_async_remote_copy(
        src_ref=src, dst_ref=dst, send_sem=send, recv_sem=recv,
        device_id=device, device_id_type=MESH,
    )


class Gather:
    def __init__(self, grid, own, full, sems, row):
        self.grid, self.own, self.full = grid, own, full
        send, recv, local = sems
        g = grid
        mine = full.at[g.z, g.x, g.core]
        self.keep = pltpu.make_async_copy(own, mine, local.at[row])
        self.along_z = [
            remote(own, mine, send.at[row, d - 1], recv.at[row, d - 1], g.z_device(z))
            for d, z in g.z_peers()
        ]
        base = g.zs - 2
        lane = full.at[:, g.x, g.core]
        self.along_x = [
            remote(lane, lane, send.at[row, base + d], recv.at[row, base + d], g.x_device(x))
            for d, x in g.x_peers()
        ]
        last = g.zs - 1 + g.xs - 1
        plane = full.at[:, :, g.core]
        self.across = remote(plane, plane, send.at[row, last], recv.at[row, last], g.sibling())

    def begin(self):
        self.keep.start()
        for copy in self.along_z:
            copy.start()

    def second(self):
        self.keep.wait()
        for copy in self.along_z:
            copy.wait_recv()
        for copy in self.along_x:
            copy.start()

    def third(self):
        for copy in self.along_x:
            copy.wait_recv()
        self.across.start()

    def finish(self):
        self.across.wait_recv()

    def drain(self):
        for copy in self.along_z + self.along_x + [self.across]:
            copy.wait_send()


class Reduce:
    def __init__(self, grid, part, bufs, out, sems, row):
        self.grid, self.part, self.out = grid, part, out
        send, recv = sems
        g = grid
        self.from_sibling, self.chip, self.from_x, self.line, self.from_z, self.own, self.from_rep = bufs
        self.across = remote(
            part.at[:, :, 1 - g.core], self.from_sibling, send.at[row, 0], recv.at[row, 0], g.sibling()
        )
        self.along_x = [
            remote(self.chip.at[:, x], self.from_x.at[d - 1], send.at[row, d], recv.at[row, d], g.x_device(x))
            for d, x in g.x_peers()
        ]
        base = g.xs - 1
        self.along_z = [
            remote(self.line.at[z], self.from_z.at[d - 1], send.at[row, base + d], recv.at[row, base + d], g.z_device(z))
            for d, z in g.z_peers()
        ]
        base += g.zs - 1
        self.along_rep = [
            remote(self.own, self.from_rep.at[d - 1], send.at[row, base + d], recv.at[row, base + d], g.rep_device(rep))
            for d, rep in g.rep_peers()
        ]

    def begin(self):
        self.across.start()

    def second(self):
        self.across.wait_recv()
        mine = self.part[:, :, self.grid.core].astype(F32)
        self.chip[...] = (mine + self.from_sibling[...].astype(F32)).astype(BF)
        for copy in self.along_x:
            copy.start()

    def third(self):
        for copy in self.along_x:
            copy.wait_recv()
        total = self.chip[:, self.grid.x].astype(F32)
        for d, _ in self.grid.x_peers():
            total = total + self.from_x[d - 1].astype(F32)
        self.line[...] = total.astype(BF)
        for copy in self.along_z:
            copy.start()

    def fourth(self):
        for copy in self.along_z:
            copy.wait_recv()
        total = self.line[self.grid.z].astype(F32)
        for d, _ in self.grid.z_peers():
            total = total + self.from_z[d - 1].astype(F32)
        self.own[...] = total.astype(BF)
        for copy in self.along_rep:
            copy.start()

    def finish(self):
        for copy in self.along_rep:
            copy.wait_recv()
        total = self.own[...].astype(F32)
        for d, _ in self.grid.rep_peers():
            total = total + self.from_rep[d - 1].astype(F32)
        out, half = self.out
        if half is None:
            out[...] = total
            return
        for i in range(3):
            lanes = slice(256 * i + 128 * half, 256 * i + 128 * half + 128)
            out[:, lanes] = total[:, 128 * i : 128 * i + 128]

    def drain(self):
        for copy in [self.across] + self.along_x + self.along_z + self.along_rep:
            copy.wait_send()


def reduce_bufs(zs, xs, copies, shape):
    dims = [(zs, xs), (zs, xs), (max(xs - 1, 1), zs), (zs,), (zs - 1,), (), (max(copies - 1, 1),)]
    return [pltpu.VMEM(d + tuple(shape), BF) for d in dims]


SCRATCH = dict(
    x=((3, ROWS, 256), F32),
    after=((2, ROWS, 256), F32),
    n1=((2, ROWS, 256), BF),
    n2=((2, ROWS, 256), BF),
    a=((2, ROWS, 256), BF),
    act=((2, ROWS, 1024), BF),
    slope=((2, ROWS, 1024), BF),
    row=((3, 2, ROWS, 128), BF),
    col=((3, 2, WG, TALL, 128), BF),
    turn=((3, WG, HP, GROUP, 128), F32),
    back=((3, HP, WG, GROUP, 128), F32),
    o_r=((2, HP // STRIPE, 128, WIDE_R), F32),
    o_c=((2, WG, 128, WIDE_C), F32),
    lse_r=((2, HP // STRIPE, 8, WIDE_R), F32),
    lse_c=((2, WG, 8, WIDE_C), F32),
    qs_r=((HEADS * WIDE_R, 256), BF),
    qs_c=((HEADS * WIDE_C, 256), BF),
    ds_r=((HEADS * WIDE_R, 128), BF),
    ds_c=((HEADS * WIDE_C, 128), BF),
    p_all=((CHUNK, HEADS * WIDE_R), BF),
    g_all=((CHUNK, HEADS * WIDE_R), BF),
    g=((ROWS, 256), F32),
    gy=((ROWS, 256), BF),
    g1=((ROWS, 256), BF),
    da_r=((ROWS, 128), BF),
    dqkv_r=((ROWS, 384), BF),
    dqkv_c=((ROWS, 384), BF),
    gv=((128, 256), F32),
    vec=((2, 128, 256), F32),
)


class Refs:
    def __init__(self, names, refs):
        self.__dict__.update(zip(names, refs))


MATRICES = ("qkv", "proj", "fc1", "fc2")
SUMMED = ("fc2", "fc1", "proj", "qkv_r", "qkv_c", "vec")


class Weights:
    def __init__(self, full):
        self.full = full

    def whole(self, name, l):
        value = self.full[name][l]
        return value.reshape(-1, value.shape[-1])

    def qkv(self, l):
        return self.whole("qkv", l)

    def proj(self, l):
        return self.whole("proj", l)

    def fc1(self, l):
        return self.whole("fc1", l)

    def fc2(self, l):
        return self.whole("fc2", l)


class Queue:
    def __init__(self, moves):
        self.moves = moves
        self.under_way = []

    def begin(self, *parts):
        for part in parts:
            getattr(part, self.moves[0])()
        self.under_way += [[part, 1] for part in parts]

    def advance(self, parts=None):
        for entry in self.under_way:
            if (parts is None or entry[0] in parts) and entry[1] < len(self.moves):
                getattr(entry[0], self.moves[entry[1]])()
                entry[1] += 1

    def complete(self, parts=None):
        while any(
            e[1] < len(self.moves) for e in self.under_way if parts is None or e[0] in parts
        ):
            self.advance(parts)

    def drain(self):
        for part, _ in self.under_way:
            part.drain()


class Gradients:
    def __init__(self, parts):
        self.parts = parts

    def put(self, name, l, value):
        ref = self.parts[name, l]
        ref[...] = value.astype(BF).reshape(ref.shape)


def plan(shards, copies, layers, width, hidden):
    zs, xs = 4, shards // 8
    place = (zs, xs, 2)
    d, f = width // shards, hidden // shards
    shapes = {k: pltpu.VMEM(*v) for k, v in SCRATCH.items()}
    own = dict(qkv=(d, 3 * width), proj=(d, width), fc1=(d, hidden), fc2=(f, width))
    for name in MATRICES:
        shapes["full", name] = pltpu.VMEM((layers,) + place + own[name], BF)
    shapes["own", "vec"] = pltpu.VMEM((layers, d, 128), F32)
    shapes["full", "vec"] = pltpu.VMEM(place + (layers, d, 128), F32)
    gathers = len(MATRICES) * layers + 1
    hops = zs - 1 + xs - 1 + 1
    for name in ("gather send", "gather recv"):
        shapes[name] = pltpu.SemaphoreType.DMA((gathers, hops))
    shapes["gather local"] = pltpu.SemaphoreType.DMA((gathers,))
    own.update(qkv_r=(d, 3 * width // 2), qkv_c=(d, 3 * width // 2), vec=(d, 128))
    sums = len(SUMMED) * layers
    hops += copies - 1
    for l in range(layers):
        for name in SUMMED:
            shapes["part", name, l] = pltpu.VMEM(place + own[name], BF)
            for i, buf in enumerate(reduce_bufs(zs, xs, copies, own[name])):
                shapes["buf", name, l, i] = buf
    for name in ("sum send", "sum recv"):
        shapes[name] = pltpu.SemaphoreType.DMA((sums, hops))
    shapes["out"] = pltpu.SemaphoreType.DMA((2,))
    return shapes


def step_kernel(shards, copies, names, *refs):
    h_ref, w_ref, tok, cot = refs[:4]
    own = dict(zip(MATRICES, refs[4:8]))
    vec_own = refs[8]
    y_ref, gt_ref = refs[9:11]
    outs = dict(zip(MATRICES + ("vec",), refs[11:16]))
    s = dict(zip(names, refs[16:]))
    r = Refs(SCRATCH, [s[k] for k in SCRATCH])
    layers = own["qkv"].shape[0]
    grid = Grid(shards, copies)
    grid.signal()
    h, w = h_ref[0], w_ref[0]

    held = vec_own.shape[1]
    eye = (iota((held, 128), 0) == iota((held, 128), 1)).astype(F32).astype(BF)
    for l in range(layers):
        s["own", "vec"][l] = mm(vec_own[l], eye, TN)
    sems = [s["gather send"], s["gather recv"], s["gather local"]]
    order = [(name, l) for l in range(layers) for name in MATRICES]
    gathers = {
        (name, l): Gather(grid, own[name].at[l], s["full", name].at[l], sems, i)
        for i, (name, l) in enumerate(order)
    }
    gathers["vec"] = Gather(grid, s["own", "vec"], s["full", "vec"], sems, len(order))
    wt = Weights({name: s["full", name] for name in MATRICES})
    gather_queue = Queue(("begin", "second", "third", "finish"))
    first = [gathers["qkv", 0], gathers["vec"]]
    rest = [gathers[key] for key in order if key != ("qkv", 0)]
    early, late = rest[:3], rest[3:]

    grid.wait()
    gather_queue.begin(*first)
    for stack in (r.qs_r, r.qs_c):
        stack[...] = jnp.where(iota(stack.shape, 1) == 128, 1.0, 0.0).astype(BF)
    for stack in (r.ds_r, r.ds_c):
        stack[...] = jnp.zeros_like(stack)
    r.gv[...] = jnp.zeros_like(r.gv)
    pad_groups(tok, r.x.at[0])
    pad_groups(cot, r.g)
    gather_queue.advance(first)
    gather_queue.begin(*early)
    gather_queue.begin(*late)
    gather_queue.complete(first)
    for l in range(layers):
        value = s["full", "vec"][:, :, :, l]
        r.vec[l] = value.reshape(-1, 128).T

    def after_forward(point, l):
        if l == 0:
            if point == "horizontal":
                gather_queue.advance(early)
            if point == "vertical":
                gather_queue.complete(early)
                gather_queue.advance(late)
            if point == "fed":
                gather_queue.complete(late)

    for l in range(layers):
        forward_layer(l, h, w, wt, r, after_forward)
    y_copy = pltpu.make_async_copy(r.x.at[layers], y_ref, s["out"].at[0])
    y_copy.start()

    sum_queue = Queue(("begin", "second", "third", "fourth", "finish"))
    width = 128
    sums = {}
    for l in range(layers):
        for i, name in enumerate(SUMMED):
            if name in ("qkv_r", "qkv_c"):
                out = (outs["qkv"].at[l], 0 if name == "qkv_r" else 1)
            else:
                out = (outs[name].at[l], None)
            bufs = [s["buf", name, l, j] for j in range(7)]
            row = l * len(SUMMED) + i
            sums[name, l] = Reduce(
                grid, s["part", name, l], bufs, out, [s["sum send"], s["sum recv"]], row
            )
    gradients = Gradients({(name, l): s["part", name, l] for l in range(layers) for name in SUMMED})

    def after_backward(point, l):
        if point == "back summed":
            sum_queue.advance()
            sum_queue.begin(*(sums[name, l] for name in ("fc2", "fc1", "proj")))
        if point == "back horizontal":
            sum_queue.advance()
            sum_queue.begin(sums["qkv_r", l])
        if point == "back vertical":
            sum_queue.advance()
            sum_queue.begin(sums["qkv_c", l])
        if point == "back mixed":
            sum_queue.advance()
            sum_queue.begin(sums["vec", l])

    for l in reversed(range(layers)):
        backward_layer(l, h, w, wt, r, gradients, after_backward)
    g_copy = pltpu.make_async_copy(r.g, gt_ref, s["out"].at[1])
    g_copy.start()
    sum_queue.complete()
    gather_queue.drain()
    sum_queue.drain()
    y_copy.wait()
    g_copy.wait()


def finish_kernel(count, *refs):
    y, g = refs[:2]
    drop_groups(y, refs[count])
    drop_groups(g, refs[count + 1])
    for i in range(2, count - 1):
        refs[count + i][...] = refs[i][...]
    vec, out = refs[count - 1], refs[2 * count - 1]
    layers, held, places = out.shape
    for l in range(layers):
        turned = widen(vec[l], 128).T
        out[l] = turned[0:held, 0:places]


def shards_step(shards, copies, tokens, heights, widths, w_qkv, w_proj, w_fc1, w_fc2, vectors, cotangent):
    layers, _, hidden = w_fc1.shape
    count, width = tokens.shape
    vmem = pl.BlockSpec(memory_space=pltpu.VMEM)
    smem = pl.BlockSpec(memory_space=pltpu.SMEM)
    hbm = pl.BlockSpec(memory_space=pl.ANY)
    scratch = plan(shards, copies, layers, width, hidden)
    matrices = [w_qkv, w_proj, w_fc1, w_fc2]
    results = [jax.ShapeDtypeStruct((ROWS, width), F32)] * 2
    results += [jax.ShapeDtypeStruct(m.shape, F32) for m in matrices]
    results += [jax.ShapeDtypeStruct((layers, width // shards, 128), F32)]
    raw = pl.pallas_call(
        functools.partial(step_kernel, shards, copies, list(scratch)),
        out_shape=results,
        in_specs=[smem, smem, vmem, vmem] + [vmem] * 5,
        out_specs=[hbm, hbm] + [vmem] * 5,
        scratch_shapes=list(scratch.values()),
        compiler_params=pltpu.CompilerParams(
            collective_id=0, has_side_effects=True, vmem_limit_bytes=67043328
        ),
    )(heights, widths, tokens, cotangent, *matrices, vectors)
    final = [jax.ShapeDtypeStruct((count, width), F32)] * 2
    final += [jax.ShapeDtypeStruct(m.shape, F32) for m in matrices + [vectors]]
    return tuple(
        pl.pallas_call(
            functools.partial(finish_kernel, len(raw)),
            out_shape=final,
            in_specs=[vmem] * len(raw),
            out_specs=[vmem] * len(raw),
            compiler_params=pltpu.CompilerParams(vmem_limit_bytes=67043328),
        )(*raw)
    )


def solution(mesh):
    images = P(("fsdp", "rep"), None)
    weights = P(None, "fsdp", None)
    return jax.shard_map(
        functools.partial(shards_step, mesh.shape["fsdp"], mesh.shape["rep"]),
        mesh=mesh,
        in_specs=(images, P(("fsdp", "rep")), P(("fsdp", "rep")), weights, weights, weights, weights, P(None, None, "fsdp"), images),
        out_specs=(images, images, weights, weights, weights, weights, P(None, None, "fsdp")),
        check_vma=False,
    )
```

```python
import functools
import jax
import jax.numpy as jnp
from jax import lax
from jax.experimental import pallas as pl
from jax.experimental.pallas import tpu as pltpu
from jax.sharding import PartitionSpec as P

HEAD = 32
STRIPE = 7
HP = 28
WP = 42
HEADS = 4
GROUP = 8
WG = WP // STRIPE
ROWS = HP * WG * GROUP
CHUNK = STRIPE * WG * GROUP
TALL = HP * GROUP
WIDE_R = 384
WIDE_C = 256
BF = jnp.bfloat16
F32 = jnp.float32
eps_norm = 1e-05
masked_score = -1000000000.0
LOG2E = 1.4426950408889634
LN2 = 0.6931471805599453
SCALE = HEAD ** (-0.5)
NN = (((1,), (0,)), ((), ()))
NT = (((1,), (1,)), ((), ()))
TN = (((0,), (0,)), ((), ()))


def mm(a, b, dims=NN):
    return lax.dot_general(a, b, dims, preferred_element_type=F32)


def iota(shape, dim):
    return lax.broadcasted_iota(jnp.int32, shape, dim)


def span(index, size):
    return pl.ds(pl.multiple_of(index * size, size), size)


def pad_groups(src, dst, scale=None):
    def body(j, carry):
        block = src[pl.ds(pl.multiple_of(j * 56, 8), 56), :].astype(F32).reshape(7, 8, -1)
        place = iota((8, block.shape[-1]), 0)
        for u in range(8):
            if u == 0:
                group = block[0]
            elif u == 7:
                group = pltpu.roll(block[6], 7, 0)
            else:
                group = jnp.where(
                    place < u, pltpu.roll(block[u - 1], u, 0), pltpu.roll(block[u], u, 0)
                )
            group = jnp.where(place < 7, group, 0.0)
            dst[pl.ds(pl.multiple_of(j * 64 + u * 8, 8), 8), :] = group
        return carry

    lax.fori_loop(0, ROWS // 64, body, 0)


def drop_groups(src, dst):
    def body(j, carry):
        block = src[pl.ds(pl.multiple_of(j * 64, 8), 64), :].reshape(8, 8, -1)
        place = iota((8, block.shape[-1]), 0)
        for t in range(7):
            lower = block[t] if t == 0 else pltpu.roll(block[t], 8 - t, 0)
            upper = pltpu.roll(block[t + 1], 7 - t, 0)
            dst[pl.ds(pl.multiple_of(j * 56 + t * 8, 8), 8), :] = jnp.where(
                place <= 6 - t, lower, upper
            )
        return carry

    lax.fori_loop(0, ROWS // 64, body, 0)


def norm_parts(x):
    centre = jnp.mean(x, axis=-1, keepdims=True)
    centred = x - centre
    rate = lax.rsqrt(jnp.mean(centred * centred, axis=-1, keepdims=True) + eps_norm)
    return centred * rate, rate


def norm_back(d_n, xhat, rate, gain):
    e = d_n * gain
    return rate * (
        e
        - jnp.mean(e, axis=-1, keepdims=True)
        - xhat * jnp.mean(e * xhat, axis=-1, keepdims=True)
    )


def colsum(x):
    return jnp.sum(x, axis=0, keepdims=True)


def rows_live(stripe, h, w, lanes):
    shape = (STRIPE, WG * GROUP, lanes)
    row = iota(shape, 0) + stripe * STRIPE
    place = iota(shape, 1)
    within = place & 7
    col = (place >> 3) * STRIPE + within
    live = (row < h) & (col < w) & (within < STRIPE)
    return jnp.where(live, 1.0, 0.0).reshape(CHUNK, lanes)


def cols_live(stripe, h, w, lanes):
    shape = (HP, GROUP, lanes)
    row = iota(shape, 0)
    within = iota(shape, 1)
    live = (row < h) & (within + stripe * STRIPE < w) & (within < STRIPE)
    return jnp.where(live, 1.0, 0.0).reshape(TALL, lanes)


def with_mask(keys, live):
    lane = iota(live.shape, 1)
    extra = jnp.where(lane == 0, jnp.where(live > 0.0, 0.0, masked_score), 0.0)
    return jnp.concatenate([keys, extra.astype(BF)], axis=-1)


def stack_heads(ref, x, wide):
    length = x.shape[0]
    lane = iota(x.shape, 1)
    for h in range(HEADS):
        kept = jnp.where((lane >> 5) == h, x, jnp.zeros_like(x))
        ref[h * wide : h * wide + length, 0:128] = kept


def widen(x, wide):
    length = x.shape[0]
    return jnp.concatenate([x, jnp.zeros((wide - length, x.shape[1]), x.dtype)], axis=0)


def attend(q, k_mask, vm, qs, out_t, lse, stripe, wide):
    length = q.shape[0]
    stack_heads(qs, q, wide)
    scores = mm(k_mask, qs[0 : HEADS * wide, :], NT)
    v_t = widen(vm.astype(F32), wide).T.astype(BF)[:, 0:length]
    for h in range(HEADS):
        s = scores[:, h * wide : (h + 1) * wide]
        top = jnp.max(s, axis=0, keepdims=True)
        p = jnp.exp2(s - top)
        total = jnp.sum(p, axis=0, keepdims=True)
        o = mm(v_t[HEAD * h : HEAD * (h + 1), :], p.astype(BF))
        out_t[stripe, HEAD * h : HEAD * (h + 1), :] = o / total
        lse[stripe, h : h + 1, :] = top + jnp.log2(total)


def attend_back(q, k, k_mask, vm, da, qs, ds_stack, p_all, g_all, out_t, lse, stripe, wide):
    length = q.shape[0]
    stack_heads(qs, q, wide)
    stack_heads(ds_stack, da, wide)
    da_t = widen(da.astype(F32), wide).T
    k_t = widen(k.astype(F32), wide).T.astype(BF)[:, 0:length]
    weighted = da_t * out_t[stripe]
    dq_t = []
    scores = mm(k_mask, qs[0 : HEADS * wide, :], NT)
    d_probs = mm(vm, ds_stack[0 : HEADS * wide, :], NT)
    for h in range(HEADS):
        lanes = slice(h * wide, (h + 1) * wide)
        inner = jnp.sum(weighted[HEAD * h : HEAD * (h + 1), :], axis=0, keepdims=True)
        p = jnp.exp2(scores[:, lanes] - lse[stripe, h : h + 1, :])
        g = (p * (d_probs[:, lanes] - inner)).astype(BF)
        p_all[0:length, lanes] = p.astype(BF)
        g_all[0:length, lanes] = g
        dq_t.append(mm(k_t[HEAD * h : HEAD * (h + 1), :], g))
    dv = mm(p_all[0:length, 0 : HEADS * wide], ds_stack[0 : HEADS * wide, :])
    dk = mm(g_all[0:length, 0 : HEADS * wide], qs[0 : HEADS * wide, 0:128]) * LN2
    dq = jnp.concatenate(dq_t, axis=0).T[0:length, :] * SCALE
    return dq, dk, dv


def earlier(x):
    return jnp.concatenate([jnp.zeros_like(x[:1]), x[:-1]], axis=0)


def later(x):
    return jnp.concatenate([x[1:], jnp.zeros_like(x[:1])], axis=0)


def row_neighbours(x):
    groups = x.reshape(STRIPE * WG, GROUP, 128)
    place = iota(groups.shape, 1)
    edge = jnp.zeros((STRIPE, 1, GROUP, 128), x.dtype)
    far = pltpu.roll(groups, 2, 1).reshape(STRIPE, WG, GROUP, 128)
    far = jnp.concatenate([edge, far[:, :-1]], axis=1).reshape(groups.shape)
    left = jnp.where(place == 0, far, pltpu.roll(groups, 1, 1))
    far = pltpu.roll(groups, 6, 1).reshape(STRIPE, WG, GROUP, 128)
    far = jnp.concatenate([far[:, 1:], edge], axis=1).reshape(groups.shape)
    right = jnp.where(place == 6, far, pltpu.roll(groups, 7, 1))
    shape = (STRIPE, WG * GROUP, 128)
    return left.reshape(shape), x.reshape(shape), right.reshape(shape)


def col_neighbours(x):
    cells = x.reshape(HP, GROUP, 128)
    return pltpu.roll(cells, 1, 1), cells, pltpu.roll(cells, 7, 1)


def position(near, taps):
    rows = [sum(taps[3 * a + b] * near[b] for b in range(3)) for a in range(3)]
    return earlier(rows[0]) + rows[1] + later(rows[2])


def position_back(near, taps):
    rows = [sum(taps[3 * a + b] * near[2 - b] for b in range(3)) for a in range(3)]
    return later(rows[0]) + rows[1] + earlier(rows[2])


def tap_sums(da, near):
    sums = []
    for a in range(3):
        for b in range(3):
            x = near[b]
            x = earlier(x) if a == 0 else later(x) if a == 2 else x
            sums.append(colsum((da * x).reshape(-1, 128)))
    return sums


def forward_layer(l, h, w, wt, r, at):
    at("P", l)
    vec = r.vec[l]

    def project(s, carry):
        rows = span(s, CHUNK)
        xhat, rate = norm_parts(r.x[l, rows, :])
        n1 = (xhat * vec[0:1] + vec[1:2]).astype(BF)
        r.n1[l, rows, :] = n1
        live = rows_live(s, h, w, 256)
        mixed = mm(n1, wt.qkv(l))
        q = (mixed[:, 0:256] + vec[2:3]) * (SCALE * LOG2E)
        k = mixed[:, 256:512]
        v = (mixed[:, 512:768] + vec[3:4]) * live
        for i, part in enumerate((q, k, v)):
            r.row[i, l, rows, :] = part[:, 0:128].astype(BF)
            cells = part[:, 128:256].reshape(STRIPE, WG, GROUP, 128)
            for c in range(STRIPE):
                r.turn[i, :, s * STRIPE + c] = cells[c]
        at("P", l, s)
        return carry

    lax.fori_loop(0, HP // STRIPE, project, 0)

    at("H", l)

    def horizontal(s, carry):
        rows = span(s, CHUNK)
        q, k, v = (r.row[i, l, rows, :] for i in range(3))
        attend(q, with_mask(k, rows_live(s, h, w, 128)), v, r.qs_r, r.o_r.at[l], r.lse_r.at[l], s, WIDE_R)
        near = row_neighbours(v.astype(F32))
        taps = vec[9:18, 0:128]
        pos = position(near, [taps[i : i + 1] for i in range(9)]) + vec[8:9, 0:128]
        o = r.o_r[l, s].T[0:CHUNK, :]
        r.a[l, rows, 0:128] = (o + pos.reshape(CHUNK, 128)).astype(BF)
        at("H", l, s)
        return carry

    lax.fori_loop(0, HP // STRIPE, horizontal, 0)

    def vertical(s, carry):
        q, k, v = (r.turn[i, s].reshape(TALL, 128).astype(BF) for i in range(3))
        for i, part in enumerate((q, k, v)):
            r.col[i, l, s] = part
        attend(q, with_mask(k, cols_live(s, h, w, 128)), v, r.qs_c, r.o_c.at[l], r.lse_c.at[l], s, WIDE_C)
        near = col_neighbours(v.astype(F32))
        taps = vec[9:18, 128:256]
        pos = position(near, [taps[i : i + 1] for i in range(9)]) + vec[8:9, 128:256]
        o = r.o_c[l, s].T[0:TALL, :]
        r.back[0, :, s] = o.reshape(HP, GROUP, 128) + pos
        at("V", l, s)
        return carry

    lax.fori_loop(0, WG, vertical, 0)

    at("F", l)

    def feed(s, carry):
        rows = span(s, CHUNK)
        turned = r.back[0, pl.ds(s * STRIPE, STRIPE)].reshape(CHUNK, 128).astype(BF)
        r.a[l, rows, 128:256] = turned
        x1 = r.x[l, rows, :] + mm(r.a[l, rows, :], wt.proj(l)) + vec[4:5]
        r.after[l, rows, :] = x1
        xhat, rate = norm_parts(x1)
        n2 = (xhat * vec[5:6] + vec[6:7]).astype(BF)
        r.n2[l, rows, :] = n2
        hidden_bias = jnp.concatenate([vec[18 + j : 19 + j] for j in range(4)], axis=1)
        hid = mm(n2, wt.fc1(l)) + hidden_bias
        phi = 0.5 * lax.erf(hid * 0.7071067811865476) + 0.5
        slope = phi + hid * (jnp.exp2(hid * hid * (-0.5 * LOG2E)) * 0.3989422804014327)
        act = (hid * phi).astype(BF)
        r.act[l, rows, :] = act
        r.slope[l, rows, :] = slope.astype(BF)
        at("F", l, s)
        return carry

    lax.fori_loop(0, HP // STRIPE, feed, 0)
    at("G", l)

    def close(s, carry):
        rows = span(s, CHUNK)
        x1 = r.after[l, rows, :]
        r.x[l + 1, rows, :] = x1 + mm(r.act[l, rows, :], wt.fc2(l)) + vec[7:8]
        at("G", l, s)
        return carry

    lax.fori_loop(0, HP // STRIPE, close, 0)


def backward_layer(l, h, w, wt, r, out, at):
    vec = r.vec[l]
    r.gv[...] = jnp.zeros_like(r.gv)

    def add(row, value):
        r.gv[row : row + 1, :] += value

    def feed(s, carry):
        rows = span(s, CHUNK)
        g = r.g[rows, :]
        add(7, colsum(g))
        gy = g.astype(BF)
        r.gy[rows, :] = gy
        d_hid = mm(gy, wt.fc2(l), NT) * r.slope[l, rows, :].astype(F32)
        for j in range(4):
            add(18 + j, colsum(d_hid[:, 256 * j : 256 * (j + 1)]))
        dh = d_hid.astype(BF)
        r.slope[l, rows, :] = dh
        d_n2 = mm(dh, wt.fc1(l), NT)
        xhat, rate = norm_parts(r.after[l, rows, :])
        add(5, colsum(d_n2 * xhat))
        add(6, colsum(d_n2))
        g1 = g + norm_back(d_n2, xhat, rate, vec[5:6])
        r.g[rows, :] = g1
        add(4, colsum(g1))
        g1_low = g1.astype(BF)
        r.g1[rows, :] = g1_low
        da = mm(g1_low, wt.proj(l), NT)
        r.da_r[rows, :] = da[:, 0:128].astype(BF)
        add(8, colsum(da.astype(BF).astype(F32)))
        cells = da[:, 128:256].reshape(STRIPE, WG, GROUP, 128)
        for c in range(STRIPE):
            r.turn[0, :, s * STRIPE + c] = cells[c]
        at("BF", l, s)
        return carry

    lax.fori_loop(0, HP // STRIPE, feed, 0)
    out.put("fc2", l, mm(r.act[l], r.gy[...], TN))
    at("B2", l)
    out.put("fc1", l, mm(r.n2[l], r.slope[l], TN))
    out.put("proj", l, mm(r.a[l], r.g1[...], TN))
    at("BS", l)

    def horizontal(s, carry):
        rows = span(s, CHUNK)
        q, k, v = (r.row[i, l, rows, :] for i in range(3))
        da = r.da_r[rows, :]
        live = rows_live(s, h, w, 128)
        dq, dk, dv = attend_back(
            q, k, with_mask(k, live), v, da, r.qs_r, r.ds_r, r.p_all, r.g_all,
            r.o_r.at[l], r.lse_r.at[l], s, WIDE_R,
        )
        taps = [vec[9 + i : 10 + i, 0:128] for i in range(9)]
        da_near = row_neighbours(da.astype(F32))
        dv = (dv + position_back(da_near, taps).reshape(CHUNK, 128)) * live
        sums = tap_sums(da_near[1], row_neighbours(v.astype(F32)))
        for i in range(9):
            r.gv[9 + i : 10 + i, 0:128] += sums[i]
        r.gv[2:3, 0:128] += colsum(dq)
        r.gv[3:4, 0:128] += colsum(dv)
        for i, part in enumerate((dq, dk, dv)):
            r.dqkv_r[rows, 128 * i : 128 * i + 128] = part.astype(BF)
        at("BH", l, s)
        return carry

    lax.fori_loop(0, HP // STRIPE, horizontal, 0)
    out.put("qkv_r", l, mm(r.n1[l], r.dqkv_r[...], TN))
    at("BR", l)

    def vertical(s, carry):
        q, k, v = (r.col[i, l, s] for i in range(3))
        da = r.turn[0, s].reshape(TALL, 128).astype(BF)
        live = cols_live(s, h, w, 128)
        dq, dk, dv = attend_back(
            q, k, with_mask(k, live), v, da, r.qs_c, r.ds_c, r.p_all, r.g_all,
            r.o_c.at[l], r.lse_c.at[l], s, WIDE_C,
        )
        taps = [vec[9 + i : 10 + i, 128:256] for i in range(9)]
        da_near = col_neighbours(da.astype(F32))
        dv = (dv + position_back(da_near, taps).reshape(TALL, 128)) * live
        sums = tap_sums(da_near[1], col_neighbours(v.astype(F32)))
        for i in range(9):
            r.gv[9 + i : 10 + i, 128:256] += sums[i]
        r.gv[2:3, 128:256] += colsum(dq)
        r.gv[3:4, 128:256] += colsum(dv)
        for i, part in enumerate((dq, dk, dv)):
            r.back[i, :, s] = part.reshape(HP, GROUP, 128)
        at("BV", l, s)
        return carry

    lax.fori_loop(0, WG, vertical, 0)

    def turn(s, carry):
        rows = span(s, CHUNK)
        for i in range(3):
            cells = r.back[i, pl.ds(s * STRIPE, STRIPE)].reshape(CHUNK, 128)
            r.dqkv_c[rows, 128 * i : 128 * i + 128] = cells.astype(BF)
        at("BT", l, s)
        return carry

    lax.fori_loop(0, HP // STRIPE, turn, 0)
    out.put("qkv_c", l, mm(r.n1[l], r.dqkv_c[...], TN))
    at("BC", l)

    def mix(s, carry):
        rows = span(s, CHUNK)
        parts = []
        for i in range(3):
            lanes = slice(128 * i, 128 * i + 128)
            parts += [r.dqkv_r[rows, lanes], r.dqkv_c[rows, lanes]]
        d_n1 = mm(jnp.concatenate(parts, axis=1), wt.qkv(l), NT)
        xhat, rate = norm_parts(r.x[l, rows, :])
        add(0, colsum(d_n1 * xhat))
        add(1, colsum(d_n1))
        r.g[rows, :] += norm_back(d_n1, xhat, rate, vec[0:1])
        at("BM", l, s)
        return carry

    lax.fori_loop(0, HP // STRIPE, mix, 0)
    out.put("vec", l, r.gv[...].T)
    at("BX", l)


MESH = pl.DeviceIdType.MESH


class Grid:
    def __init__(self, shards, copies):
        self.cores = 2
        self.zs = 4
        self.xs = shards // 8
        self.copies = copies
        index = lax.axis_index("fsdp")
        self.rep = lax.axis_index("rep")
        self.core = lax.rem(index, 2)
        chip = lax.div(index, 2)
        self.x = lax.rem(chip, self.xs)
        self.z = lax.div(chip, self.xs)

    def at(self, z, x, core):
        return {"fsdp": (z * self.xs + x) * 2 + core, "rep": self.rep}

    def z_peers(self):
        return [(d, lax.rem(self.z + d, self.zs)) for d in range(1, self.zs)]

    def x_peers(self):
        return [(d, lax.rem(self.x + d, self.xs)) for d in range(1, self.xs)]

    def rep_peers(self):
        return [(d, lax.rem(self.rep + d, self.copies)) for d in range(1, self.copies)]

    def z_device(self, z):
        return self.at(z, self.x, self.core)

    def x_device(self, x):
        return self.at(self.z, x, self.core)

    def sibling(self):
        return self.at(self.z, self.x, 1 - self.core)

    def rep_device(self, rep):
        index = (self.z * self.xs + self.x) * 2 + self.core
        return {"fsdp": index, "rep": rep}

    def steps(self):
        return self.zs - 1 + self.xs - 1 + 1

    def peers(self):
        devices = [self.z_device(z) for _, z in self.z_peers()]
        devices += [self.x_device(x) for _, x in self.x_peers()] + [self.sibling()]
        return devices + [self.rep_device(rep) for _, rep in self.rep_peers()]

    def signal(self):
        for device in self.peers():
            pl.semaphore_signal(
                pltpu.get_barrier_semaphore(), inc=1, device_id=device, device_id_type=MESH
            )

    def wait(self):
        pl.semaphore_wait(pltpu.get_barrier_semaphore(), len(self.peers()))


def remote(src, dst, send, recv, device):
    return pltpu.make_async_remote_copy(
        src_ref=src, dst_ref=dst, send_sem=send, recv_sem=recv,
        device_id=device, device_id_type=MESH,
    )


class Gather:
    def __init__(self, grid, own, full, sems, row):
        self.grid, self.own, self.full = grid, own, full
        send, recv, local = sems
        g = grid
        mine = full.at[g.z, g.x, g.core]
        self.keep = pltpu.make_async_copy(own, mine, local.at[row])
        self.along_z = [
            remote(own, mine, send.at[row, d - 1], recv.at[row, d - 1], g.z_device(z))
            for d, z in g.z_peers()
        ]
        base = g.zs - 2
        lane = full.at[:, g.x, g.core]
        self.along_x = [
            remote(lane, lane, send.at[row, base + d], recv.at[row, base + d], g.x_device(x))
            for d, x in g.x_peers()
        ]
        last = g.zs - 1 + g.xs - 1
        plane = full.at[:, :, g.core]
        self.across = remote(plane, plane, send.at[row, last], recv.at[row, last], g.sibling())

    def begin(self):
        self.keep.start()
        for copy in self.along_z:
            copy.start()

    def second(self):
        self.keep.wait()
        for copy in self.along_z:
            copy.wait_recv()
        for copy in self.along_x:
            copy.start()

    def third(self):
        for copy in self.along_x:
            copy.wait_recv()
        self.across.start()

    def finish(self):
        self.across.wait_recv()

    def drain(self):
        for copy in self.along_z + self.along_x + [self.across]:
            copy.wait_send()


class Reduce:
    def __init__(self, grid, part, bufs, out, sems, row):
        self.grid, self.part, self.out = grid, part, out
        send, recv = sems
        g = grid
        self.from_sibling, self.chip, self.from_x, self.line, self.from_z, self.own, self.from_rep = bufs
        self.across = remote(
            part.at[:, :, 1 - g.core], self.from_sibling, send.at[row, 0], recv.at[row, 0], g.sibling()
        )
        self.along_x = [
            remote(self.chip.at[:, x], self.from_x.at[d - 1], send.at[row, d], recv.at[row, d], g.x_device(x))
            for d, x in g.x_peers()
        ]
        base = g.xs - 1
        self.along_z = [
            remote(self.line.at[z], self.from_z.at[d - 1], send.at[row, base + d], recv.at[row, base + d], g.z_device(z))
            for d, z in g.z_peers()
        ]
        base += g.zs - 1
        self.along_rep = [
            remote(self.own, self.from_rep.at[d - 1], send.at[row, base + d], recv.at[row, base + d], g.rep_device(rep))
            for d, rep in g.rep_peers()
        ]

    def begin(self):
        self.across.start()

    def second(self):
        self.across.wait_recv()
        mine = self.part[:, :, self.grid.core].astype(F32)
        self.chip[...] = (mine + self.from_sibling[...].astype(F32)).astype(BF)
        for copy in self.along_x:
            copy.start()

    def third(self):
        for copy in self.along_x:
            copy.wait_recv()
        total = self.chip[:, self.grid.x].astype(F32)
        for d, _ in self.grid.x_peers():
            total = total + self.from_x[d - 1].astype(F32)
        self.line[...] = total.astype(BF)
        for copy in self.along_z:
            copy.start()

    def fourth(self):
        for copy in self.along_z:
            copy.wait_recv()
        total = self.line[self.grid.z].astype(F32)
        for d, _ in self.grid.z_peers():
            total = total + self.from_z[d - 1].astype(F32)
        self.own[...] = total.astype(BF)
        for copy in self.along_rep:
            copy.start()

    def finish(self):
        for copy in self.along_rep:
            copy.wait_recv()
        total = self.own[...].astype(F32)
        for d, _ in self.grid.rep_peers():
            total = total + self.from_rep[d - 1].astype(F32)
        out, half = self.out
        if half is None:
            out[...] = total
            return
        for i in range(3):
            lanes = slice(256 * i + 128 * half, 256 * i + 128 * half + 128)
            out[:, lanes] = total[:, 128 * i : 128 * i + 128]

    def drain(self):
        for copy in [self.across] + self.along_x + self.along_z + self.along_rep:
            copy.wait_send()


def reduce_bufs(zs, xs, copies, shape):
    dims = [(zs, xs), (zs, xs), (max(xs - 1, 1), zs), (zs,), (zs - 1,), (), (max(copies - 1, 1),)]
    return [pltpu.VMEM(d + tuple(shape), BF) for d in dims]


SCRATCH = dict(
    x=((3, ROWS, 256), F32),
    after=((2, ROWS, 256), F32),
    n1=((2, ROWS, 256), BF),
    n2=((2, ROWS, 256), BF),
    a=((2, ROWS, 256), BF),
    act=((2, ROWS, 1024), BF),
    slope=((2, ROWS, 1024), BF),
    row=((3, 2, ROWS, 128), BF),
    col=((3, 2, WG, TALL, 128), BF),
    turn=((3, WG, HP, GROUP, 128), F32),
    back=((3, HP, WG, GROUP, 128), F32),
    o_r=((2, HP // STRIPE, 128, WIDE_R), F32),
    o_c=((2, WG, 128, WIDE_C), F32),
    lse_r=((2, HP // STRIPE, 8, WIDE_R), F32),
    lse_c=((2, WG, 8, WIDE_C), F32),
    qs_r=((HEADS * WIDE_R, 256), BF),
    qs_c=((HEADS * WIDE_C, 256), BF),
    ds_r=((HEADS * WIDE_R, 128), BF),
    ds_c=((HEADS * WIDE_C, 128), BF),
    p_all=((CHUNK, HEADS * WIDE_R), BF),
    g_all=((CHUNK, HEADS * WIDE_R), BF),
    g=((ROWS, 256), F32),
    gy=((ROWS, 256), BF),
    g1=((ROWS, 256), BF),
    da_r=((ROWS, 128), BF),
    dqkv_r=((ROWS, 384), BF),
    dqkv_c=((ROWS, 384), BF),
    gv=((128, 256), F32),
    vec=((2, 128, 256), F32),
)


class Refs:
    def __init__(self, names, refs):
        self.__dict__.update(zip(names, refs))


MATRICES = ("qkv", "proj", "fc1", "fc2")
SUMMED = ("fc2", "fc1", "proj", "qkv_r", "qkv_c", "vec")


class Weights:
    def __init__(self, full):
        self.full = full

    def whole(self, name, l):
        value = self.full[name][l]
        return value.reshape(-1, value.shape[-1])

    def qkv(self, l):
        return self.whole("qkv", l)

    def proj(self, l):
        return self.whole("proj", l)

    def fc1(self, l):
        return self.whole("fc1", l)

    def fc2(self, l):
        return self.whole("fc2", l)


GATHER_MOVES = {
    ("P", 0, 3): ["proj 0 second", "fc1 0 second"],
    ("H", 0, 1): ["fc2 0 second", "qkv 1 begin"],
    ("V", 0, 0): ["proj 1 begin"],
    ("V", 0, 3): ["proj 0 third", "fc1 0 third"],
    ("V", 0, 4): ["qkv 1 second", "fc1 1 begin"],
    ("F", 0, None): ["proj 0 finish", "fc1 0 finish"],
    ("F", 0, 1): ["fc2 0 third", "fc2 1 begin"],
    ("G", 0, None): ["fc2 0 finish"],
    ("G", 0, 0): ["qkv 1 third"],
    ("G", 0, 3): ["proj 1 second", "fc1 1 second"],
    ("P", 1, None): ["qkv 1 finish"],
    ("P", 1, 3): ["fc2 1 second"],
    ("H", 1, 3): ["proj 1 third", "fc1 1 third"],
    ("V", 1, 3): ["fc2 1 third"],
    ("F", 1, None): ["proj 1 finish", "fc1 1 finish"],
    ("G", 1, None): ["fc2 1 finish"],
}
SUM_MOVES = {
    ("B2", 1, None): ["fc2 1 begin"],
    ("BS", 1, None): ["fc1 1 begin", "proj 1 begin"],
    ("BH", 1, 0): ["fc2 1 second", "fc1 1 second", "proj 1 second"],
    ("BR", 1, None): ["qkv_r 1 begin", "fc2 1 third"],
    ("BV", 1, 0): ["qkv_r 1 second"],
    ("BV", 1, 2): ["fc1 1 third", "proj 1 third"],
    ("BV", 1, 4): ["qkv_r 1 third"],
    ("BC", 1, None): ["qkv_c 1 begin"],
    ("BM", 1, 0): ["fc2 1 fourth"],
    ("BM", 1, 2): ["qkv_c 1 second"],
    ("BX", 1, None): ["vec 1 begin"],
    ("BF", 0, 1): ["fc1 1 fourth", "proj 1 fourth", "vec 1 second"],
    ("BF", 0, 3): ["fc2 1 finish", "qkv_r 1 fourth", "qkv_c 1 third"],
    ("B2", 0, None): ["fc2 0 begin"],
    ("BS", 0, None): ["fc1 0 begin", "proj 0 begin"],
    ("BH", 0, 0): ["fc2 0 second", "fc1 0 second", "proj 0 second", "vec 1 third"],
    ("BH", 0, 1): ["fc1 1 finish", "proj 1 finish", "qkv_r 1 finish"],
    ("BH", 0, 2): ["qkv_c 1 fourth", "vec 1 fourth"],
    ("BR", 0, None): ["qkv_r 0 begin", "fc2 0 third"],
    ("BV", 0, 0): ["qkv_r 0 second"],
    ("BV", 0, 2): ["fc1 0 third", "proj 0 third"],
    ("BV", 0, 3): ["qkv_c 1 finish", "vec 1 finish"],
    ("BV", 0, 4): ["qkv_r 0 third"],
    ("BC", 0, None): ["qkv_c 0 begin"],
    ("BM", 0, 0): ["fc2 0 fourth"],
    ("BM", 0, 2): ["qkv_c 0 second"],
    ("BX", 0, None): ["vec 0 begin"],
}
LAST_MOVES = [
    ("vec", 0, "second"), ("fc1", 0, "fourth"), ("proj", 0, "fourth"), ("qkv_c", 0, "third"),
    ("vec", 0, "third"), ("qkv_r", 0, "fourth"), ("fc2", 0, "finish"), ("fc1", 0, "finish"),
    ("proj", 0, "finish"), ("qkv_r", 0, "finish"), ("qkv_c", 0, "fourth"), ("vec", 0, "fourth"),
    ("qkv_c", 0, "finish"), ("vec", 0, "finish"),
]


class Moves:
    def __init__(self, table, parts):
        self.table, self.parts = table, parts

    def take(self, moves):
        for move in moves:
            name, l, verb = move.split()
            getattr(self.parts[name, int(l)], verb)()

    def __call__(self, phase, l, step=None):
        if step is None:
            self.take(self.table.get((phase, l, None), []))
            return
        for (name, block, when), moves in self.table.items():
            if (name, block) == (phase, l) and when is not None:
                pl.when(step == when)(functools.partial(self.take, moves))


class Gradients:
    def __init__(self, parts):
        self.parts = parts

    def put(self, name, l, value):
        ref = self.parts[name, l]
        ref[...] = value.astype(BF).reshape(ref.shape)


def plan(shards, copies, layers, width, hidden, held):
    zs, xs = 4, shards // 8
    place = (zs, xs, 2)
    d, f = width // shards, hidden // shards
    shapes = {k: pltpu.VMEM(*v) for k, v in SCRATCH.items()}
    own = dict(qkv=(d, 3 * width), proj=(d, width), fc1=(d, hidden), fc2=(f, width))
    for name in MATRICES:
        shapes["full", name] = pltpu.VMEM((layers,) + place + own[name], BF)
    shapes["full", "vec"] = pltpu.VMEM(place + (layers, d, held), BF)
    gathers = len(MATRICES) * layers + 1
    hops = zs - 1 + xs - 1 + 1
    for name in ("gather send", "gather recv"):
        shapes[name] = pltpu.SemaphoreType.DMA((gathers, hops))
    shapes["gather local"] = pltpu.SemaphoreType.DMA((gathers,))
    own.update(qkv_r=(d, 3 * width // 2), qkv_c=(d, 3 * width // 2), vec=(d, 128))
    sums = len(SUMMED) * layers
    hops += copies - 1
    for l in range(layers):
        for name in SUMMED:
            shapes["part", name, l] = pltpu.VMEM(place + own[name], BF)
            for i, buf in enumerate(reduce_bufs(zs, xs, copies, own[name])):
                shapes["buf", name, l, i] = buf
    for name in ("sum send", "sum recv"):
        shapes[name] = pltpu.SemaphoreType.DMA((sums, hops))
    shapes["out"] = pltpu.SemaphoreType.DMA((2,))
    return shapes


def step_kernel(shards, copies, names, *refs):
    h_ref, w_ref, tok, cot = refs[:4]
    own = dict(zip(MATRICES, refs[4:8]))
    vec_own = refs[8]
    y_ref, gt_ref = refs[9:11]
    outs = dict(zip(MATRICES + ("vec",), refs[11:16]))
    s = dict(zip(names, refs[16:]))
    r = Refs(SCRATCH, [s[k] for k in SCRATCH])
    layers = own["qkv"].shape[0]
    grid = Grid(shards, copies)
    grid.signal()
    h, w = h_ref[0], w_ref[0]

    sems = [s["gather send"], s["gather recv"], s["gather local"]]
    order = [(name, l) for l in range(layers) for name in MATRICES]
    gathers = {
        (name, l): Gather(grid, own[name].at[l], s["full", name].at[l], sems, i)
        for i, (name, l) in enumerate(order)
    }
    gathers["vec", 0] = Gather(grid, vec_own, s["full", "vec"], sems, len(order))
    wt = Weights({name: s["full", name] for name in MATRICES})
    wt = Weights({name: s["full", name] for name in MATRICES})

    grid.wait()
    first = [gathers["qkv", 0], gathers["vec", 0]]
    for one in first:
        one.begin()
    for stack in (r.qs_r, r.qs_c):
        stack[...] = jnp.where(iota(stack.shape, 1) == 128, 1.0, 0.0).astype(BF)
    for stack in (r.ds_r, r.ds_c):
        stack[...] = jnp.zeros_like(stack)
    r.gv[...] = jnp.zeros_like(r.gv)
    pad_groups(tok, r.x.at[0])
    pad_groups(cot, r.g)
    for one in first:
        one.second()
    gathers["proj", 0].begin()
    gathers["fc1", 0].begin()
    for one in first:
        one.third()
    gathers["fc2", 0].begin()
    for one in first:
        one.finish()
    for l in range(layers):
        value = s["full", "vec"][:, :, :, l].astype(F32)
        value = value.reshape(-1, value.shape[-1])
        value = jnp.concatenate([value, jnp.zeros((value.shape[0], 128 - value.shape[1]), F32)], axis=1)
        r.vec[l] = value.T

    at = Moves(GATHER_MOVES, gathers)
    for l in range(layers):
        forward_layer(l, h, w, wt, r, at)
    y_copy = pltpu.make_async_copy(r.x.at[layers], y_ref, s["out"].at[0])
    y_copy.start()

    sums = {}
    for l in range(layers):
        for i, name in enumerate(SUMMED):
            if name in ("qkv_r", "qkv_c"):
                out = (outs["qkv"].at[l], 0 if name == "qkv_r" else 1)
            else:
                out = (outs[name].at[l], None)
            bufs = [s["buf", name, l, j] for j in range(7)]
            row = l * len(SUMMED) + i
            sums[name, l] = Reduce(
                grid, s["part", name, l], bufs, out, [s["sum send"], s["sum recv"]], row
            )
    gradients = Gradients({(name, l): s["part", name, l] for l in range(layers) for name in SUMMED})

    at = Moves(SUM_MOVES, sums)
    for l in reversed(range(layers)):
        backward_layer(l, h, w, wt, r, gradients, at)
    g_copy = pltpu.make_async_copy(r.g, gt_ref, s["out"].at[1])
    g_copy.start()
    for name, l, move in LAST_MOVES:
        getattr(sums[name, l], move)()
    for one in list(gathers.values()) + list(sums.values()):
        one.drain()
    y_copy.wait()
    g_copy.wait()


def finish_kernel(count, *refs):
    y, g = refs[:2]
    drop_groups(y, refs[count])
    drop_groups(g, refs[count + 1])
    for i in range(2, count - 1):
        refs[count + i][...] = refs[i][...]
    vec, out = refs[count - 1], refs[2 * count - 1]
    out[...] = vec[:, :, 0 : out.shape[2]]


def shards_step(shards, copies, tokens, heights, widths, w_qkv, w_proj, w_fc1, w_fc2, vectors, cotangent):
    layers, _, hidden = w_fc1.shape
    count, width = tokens.shape
    vmem = pl.BlockSpec(memory_space=pltpu.VMEM)
    smem = pl.BlockSpec(memory_space=pltpu.SMEM)
    hbm = pl.BlockSpec(memory_space=pl.ANY)
    turned = vectors.transpose(0, 2, 1)
    scratch = plan(shards, copies, layers, width, hidden, turned.shape[2])
    matrices = [w_qkv, w_proj, w_fc1, w_fc2]
    results = [jax.ShapeDtypeStruct((ROWS, width), F32)] * 2
    results += [jax.ShapeDtypeStruct(m.shape, F32) for m in matrices]
    results += [jax.ShapeDtypeStruct((layers, width // shards, 128), F32)]
    raw = pl.pallas_call(
        functools.partial(step_kernel, shards, copies, list(scratch)),
        out_shape=results,
        in_specs=[smem, smem, vmem, vmem] + [vmem] * 5,
        out_specs=[hbm, hbm] + [vmem] * 5,
        scratch_shapes=list(scratch.values()),
        compiler_params=pltpu.CompilerParams(
            collective_id=0, has_side_effects=True, vmem_limit_bytes=67043328
        ),
    )(heights, widths, tokens, cotangent, *matrices, turned)
    final = [jax.ShapeDtypeStruct((count, width), F32)] * 2
    final += [jax.ShapeDtypeStruct(m.shape, F32) for m in matrices + [turned]]
    *arrays, vec = pl.pallas_call(
        functools.partial(finish_kernel, len(raw)),
        out_shape=final,
        in_specs=[vmem] * len(raw),
        out_specs=[vmem] * len(raw),
        compiler_params=pltpu.CompilerParams(vmem_limit_bytes=67043328),
    )(*raw)
    return (*arrays, vec.transpose(0, 2, 1))


def solution(mesh):
    images = P(("fsdp", "rep"), None)
    weights = P(None, "fsdp", None)
    return jax.shard_map(
        functools.partial(shards_step, mesh.shape["fsdp"], mesh.shape["rep"]),
        mesh=mesh,
        in_specs=(images, P(("fsdp", "rep")), P(("fsdp", "rep")), weights, weights, weights, weights, P(None, None, "fsdp"), images),
        out_specs=(images, images, weights, weights, weights, weights, P(None, None, "fsdp")),
        check_vma=False,
    )
```

```python
import functools
import jax
import jax.numpy as jnp
from jax import lax
from jax.experimental import pallas as pl
from jax.experimental.pallas import tpu as pltpu
from jax.sharding import PartitionSpec as P

HEAD = 32
STRIPE = 7
HP = 28
WP = 42
HEADS = 4
GROUP = 8
WG = WP // STRIPE
ROWS = HP * WG * GROUP
CHUNK = STRIPE * WG * GROUP
TALL = HP * GROUP
WIDE_R = 384
WIDE_C = 256
BF = jnp.bfloat16
F32 = jnp.float32
eps_norm = 1e-05
masked_score = -1000000000.0
LOG2E = 1.4426950408889634
LN2 = 0.6931471805599453
SCALE = HEAD ** (-0.5)
NN = (((1,), (0,)), ((), ()))
NT = (((1,), (1,)), ((), ()))
TN = (((0,), (0,)), ((), ()))


def mm(a, b, dims=NN):
    return lax.dot_general(a, b, dims, preferred_element_type=F32)


def iota(shape, dim):
    return lax.broadcasted_iota(jnp.int32, shape, dim)


def span(index, size):
    return pl.ds(pl.multiple_of(index * size, size), size)


def map_rows(stripe):
    return pl.ds(stripe * STRIPE, STRIPE)


def pad_groups(src, dst, scale=None):
    def body(j, carry):
        block = src[pl.ds(pl.multiple_of(j * 56, 8), 56), :].astype(F32).reshape(7, 8, -1)
        place = iota((8, block.shape[-1]), 0)
        for u in range(8):
            if u == 0:
                group = block[0]
            elif u == 7:
                group = pltpu.roll(block[6], 7, 0)
            else:
                group = jnp.where(
                    place < u, pltpu.roll(block[u - 1], u, 0), pltpu.roll(block[u], u, 0)
                )
            group = jnp.where(place < 7, group, 0.0)
            dst[pl.ds(pl.multiple_of(j * 64 + u * 8, 8), 8), :] = group
        return carry

    lax.fori_loop(0, ROWS // 64, body, 0)


def drop_groups(src, dst):
    def body(j, carry):
        block = src[pl.ds(pl.multiple_of(j * 64, 8), 64), :].reshape(8, 8, -1)
        place = iota((8, block.shape[-1]), 0)
        for t in range(7):
            lower = block[t] if t == 0 else pltpu.roll(block[t], 8 - t, 0)
            upper = pltpu.roll(block[t + 1], 7 - t, 0)
            dst[pl.ds(pl.multiple_of(j * 56 + t * 8, 8), 8), :] = jnp.where(
                place <= 6 - t, lower, upper
            )
        return carry

    lax.fori_loop(0, ROWS // 64, body, 0)


def norm_parts(x):
    centre = jnp.mean(x, axis=-1, keepdims=True)
    centred = x - centre
    rate = lax.rsqrt(jnp.mean(centred * centred, axis=-1, keepdims=True) + eps_norm)
    return centred * rate, rate


def norm_back(d_n, xhat, rate, gain):
    e = d_n * gain
    return rate * (
        e
        - jnp.mean(e, axis=-1, keepdims=True)
        - xhat * jnp.mean(e * xhat, axis=-1, keepdims=True)
    )


def colsum(x):
    return jnp.sum(x, axis=0, keepdims=True)


def rows_live(stripe, h, w, lanes):
    shape = (STRIPE, WG * GROUP, lanes)
    row = iota(shape, 0) + stripe * STRIPE
    place = iota(shape, 1)
    within = place & 7
    col = (place >> 3) * STRIPE + within
    live = (row < h) & (col < w) & (within < STRIPE)
    return jnp.where(live, 1.0, 0.0).reshape(CHUNK, lanes)


def cols_live(stripe, h, w, lanes):
    shape = (HP, GROUP, lanes)
    row = iota(shape, 0)
    within = iota(shape, 1)
    live = (row < h) & (within + stripe * STRIPE < w) & (within < STRIPE)
    return jnp.where(live, 1.0, 0.0).reshape(TALL, lanes)


def with_mask(keys, live):
    lane = iota(live.shape, 1)
    extra = jnp.where(lane == 0, jnp.where(live > 0.0, 0.0, masked_score), 0.0)
    return jnp.concatenate([keys, extra.astype(BF)], axis=-1)


def stack_heads(ref, x, wide):
    length = x.shape[0]
    lane = iota(x.shape, 1)
    for h in range(HEADS):
        kept = jnp.where((lane >> 5) == h, x, jnp.zeros_like(x))
        ref[h * wide : h * wide + length, 0:128] = kept


def widen(x, wide):
    length = x.shape[0]
    return jnp.concatenate([x, jnp.zeros((wide - length, x.shape[1]), x.dtype)], axis=0)


def attend(q, k_mask, vm, qs, out_t, inv, probs, stripe, wide):
    length = q.shape[0]
    stack_heads(qs, q, wide)
    scores = mm(k_mask, qs[0 : HEADS * wide, :], NT)
    v_t = widen(vm.astype(F32), wide).T.astype(BF)[:, 0:length]
    for h in range(HEADS):
        s = scores[:, h * wide : (h + 1) * wide]
        top = jnp.max(s, axis=0, keepdims=True)
        p = jnp.exp2(s - top)
        total = jnp.sum(p, axis=0, keepdims=True)
        p_low = p.astype(BF)
        probs[stripe, :, h * wide : (h + 1) * wide] = p_low
        rate = 1.0 / total
        inv[stripe, h : h + 1, :] = rate
        o = mm(v_t[HEAD * h : HEAD * (h + 1), :], p_low)
        out_t[stripe, HEAD * h : HEAD * (h + 1), :] = o * rate


def attend_back(q, k, vm, da, qs, da_stack, g_all, out_t, inv, probs, stripe, wide):
    length = q.shape[0]
    stack_heads(qs, q, wide)
    da_t = widen(da.astype(F32), wide).T
    k_t = widen(k.astype(F32), wide).T.astype(BF)[:, 0:length]
    inner = []
    for h in range(HEADS):
        rows = slice(HEAD * h, HEAD * (h + 1))
        scaled = (da_t[rows, :] * inv[stripe, h : h + 1, :]).astype(BF)
        da_stack[rows, h * wide : (h + 1) * wide] = scaled
        inner.append(colsum(scaled.astype(F32) * out_t[stripe, rows, :]))
    d_probs = mm(vm, da_stack[...])
    dq_t = []
    for h in range(HEADS):
        lanes = slice(h * wide, (h + 1) * wide)
        p = probs[stripe, :, lanes].astype(F32)
        g = (p * (d_probs[:, lanes] - inner[h])).astype(BF)
        g_all[0:length, lanes] = g
        dq_t.append(mm(k_t[HEAD * h : HEAD * (h + 1), :], g))
    dv = mm(probs[stripe], da_stack[...], NT)
    dk = mm(g_all[0:length, 0 : HEADS * wide], qs[0 : HEADS * wide, 0:128]) * LN2
    dq = jnp.concatenate(dq_t, axis=0).T[0:length, :] * SCALE
    return dq, dk, dv


def earlier(x):
    return jnp.concatenate([jnp.zeros_like(x[:1]), x[:-1]], axis=0)


def later(x):
    return jnp.concatenate([x[1:], jnp.zeros_like(x[:1])], axis=0)


def row_neighbours(x):
    groups = x.reshape(STRIPE * WG, GROUP, 128)
    place = iota(groups.shape, 1)
    edge = jnp.zeros((STRIPE, 1, GROUP, 128), x.dtype)
    far = pltpu.roll(groups, 2, 1).reshape(STRIPE, WG, GROUP, 128)
    far = jnp.concatenate([edge, far[:, :-1]], axis=1).reshape(groups.shape)
    left = jnp.where(place == 0, far, pltpu.roll(groups, 1, 1))
    far = pltpu.roll(groups, 6, 1).reshape(STRIPE, WG, GROUP, 128)
    far = jnp.concatenate([far[:, 1:], edge], axis=1).reshape(groups.shape)
    right = jnp.where(place == 6, far, pltpu.roll(groups, 7, 1))
    shape = (STRIPE, WG * GROUP, 128)
    return left.reshape(shape), x.reshape(shape), right.reshape(shape)


def col_neighbours(x):
    cells = x.reshape(HP, GROUP, 128)
    return pltpu.roll(cells, 1, 1), cells, pltpu.roll(cells, 7, 1)


def position(near, taps):
    rows = [sum(taps[3 * a + b] * near[b] for b in range(3)) for a in range(3)]
    return earlier(rows[0]) + rows[1] + later(rows[2])


def position_back(near, taps):
    rows = [sum(taps[3 * a + b] * near[2 - b] for b in range(3)) for a in range(3)]
    return later(rows[0]) + rows[1] + earlier(rows[2])


def tap_sums(da, near):
    sums = []
    for a in range(3):
        for b in range(3):
            x = near[b]
            x = earlier(x) if a == 0 else later(x) if a == 2 else x
            sums.append(colsum((da * x).reshape(-1, 128)))
    return sums


def forward_layer(l, h, w, wt, r, at):
    at(P_, l)
    vec = r.vec[l]

    def keep_row(rows, parts):
        for i, part in enumerate(parts):
            r.row[i, l, rows, :] = part.astype(BF)

    def keep_col(s, parts):
        for i, part in enumerate(parts):
            r.cells[i, map_rows(s)] = part.reshape(STRIPE, WG, GROUP, 128)

    def split(mixed, s, half, lanes):
        here = slice(128 * half, 128 * half + 128)
        q = (mixed[:, lanes[0]] + vec[2:3, here]) * (SCALE * LOG2E)
        v = (mixed[:, lanes[2]] + vec[3:4, here]) * rows_live(s, h, w, 128)
        return q, mixed[:, lanes[1]], v

    def norm(s):
        rows = span(s, CHUNK)
        xhat, rate = norm_parts(r.x[l, rows, :])
        n1 = (xhat * vec[0:1] + vec[1:2]).astype(BF)
        r.n1[l, rows, :] = n1
        return rows, n1

    alone = [slice(128 * i, 128 * i + 128) for i in range(3)]

    def project(s):
        rows, n1 = norm(s)
        mixed = mm(n1, wt.qkv(l))
        for half in range(2):
            lanes = [slice(256 * i + 128 * half, 256 * i + 128 * half + 128) for i in range(3)]
            parts = split(mixed, s, half, lanes)
            keep_col(s, parts) if half else keep_row(rows, parts)

    def project_row(s):
        rows, n1 = norm(s)
        keep_row(rows, split(mm(n1, wt.qkv_half(l, 0)), s, 0, alone))

    def project_col(s):
        n1 = r.n1[l, span(s, CHUNK), :]
        keep_col(s, split(mm(n1, wt.qkv_half(l, 1)), s, 1, alone))

    sweep(P_, l, HP // STRIPE, project if l else project_row, at)

    at(H_, l)

    def horizontal(s):
        rows = span(s, CHUNK)
        q, k, v = (r.row[i, l, rows, :] for i in range(3))
        attend(q, with_mask(k, rows_live(s, h, w, 128)), v, r.qs_r, r.o_r.at[l], r.inv_r.at[l], r.p_r, s, WIDE_R)
        near = row_neighbours(v.astype(F32))
        taps = vec[9:18, 0:128]
        pos = position(near, [taps[i : i + 1] for i in range(9)]) + vec[8:9, 0:128]
        o = r.o_r[l, s].T[0:CHUNK, :]
        r.a[l, rows, 0:128] = (o + pos.reshape(CHUNK, 128)).astype(BF)

    sweep(H_, l, HP // STRIPE, horizontal, at)
    at(PC_, l)
    if l == 0:
        sweep(PC_, l, HP // STRIPE, project_col, at)

    def vertical(s):
        q, k, v = (r.cells[i, :, s].reshape(TALL, 128).astype(BF) for i in range(3))
        for i, part in enumerate((q, k, v)):
            r.col[i, l, s] = part
        attend(q, with_mask(k, cols_live(s, h, w, 128)), v, r.qs_c, r.o_c.at[l], r.inv_c.at[l], r.p_c, s, WIDE_C)
        near = col_neighbours(v.astype(F32))
        taps = vec[9:18, 128:256]
        pos = position(near, [taps[i : i + 1] for i in range(9)]) + vec[8:9, 128:256]
        o = r.o_c[l, s].T[0:TALL, :]
        r.cells[3, :, s] = o.reshape(HP, GROUP, 128) + pos

    sweep(V_, l, WG, vertical, at)

    at(F_, l)

    def feed(s):
        rows = span(s, CHUNK)
        turned = r.cells[3, map_rows(s)].reshape(CHUNK, 128).astype(BF)
        r.a[l, rows, 128:256] = turned
        x1 = r.x[l, rows, :] + mm(r.a[l, rows, :], wt.proj(l)) + vec[4:5]
        r.after[l, rows, :] = x1
        xhat, rate = norm_parts(x1)
        n2 = (xhat * vec[5:6] + vec[6:7]).astype(BF)
        r.n2[l, rows, :] = n2
        hidden_bias = jnp.concatenate([vec[18 + j : 19 + j] for j in range(4)], axis=1)
        hid = mm(n2, wt.fc1(l)) + hidden_bias
        phi = 0.5 * lax.erf(hid * 0.7071067811865476) + 0.5
        slope = phi + hid * (jnp.exp2(hid * hid * (-0.5 * LOG2E)) * 0.3989422804014327)
        act = (hid * phi).astype(BF)
        r.act[l, rows, :] = act
        r.slope[l, rows, :] = slope.astype(BF)

    sweep(F_, l, HP // STRIPE, feed, at)
    at(G_, l)

    def close(s):
        rows = span(s, CHUNK)
        x1 = r.after[l, rows, :]
        r.x[l + 1, rows, :] = x1 + mm(r.act[l, rows, :], wt.fc2(l)) + vec[7:8]

    sweep(G_, l, HP // STRIPE, close, at)


def backward_layer(l, h, w, wt, r, out, at):
    vec = r.vec[l]
    r.gv[...] = jnp.zeros_like(r.gv)

    def add(row, value):
        r.gv[row : row + 1, :] += value

    def feed(s):
        rows = span(s, CHUNK)
        g = r.g[rows, :]
        add(7, colsum(g))
        gy = g.astype(BF)
        r.gy[rows, :] = gy
        d_hid = mm(gy, wt.fc2(l), NT) * r.slope[l, rows, :].astype(F32)
        for j in range(4):
            add(18 + j, colsum(d_hid[:, 256 * j : 256 * (j + 1)]))
        dh = d_hid.astype(BF)
        r.slope[l, rows, :] = dh
        d_n2 = mm(dh, wt.fc1(l), NT)
        xhat, rate = norm_parts(r.after[l, rows, :])
        add(5, colsum(d_n2 * xhat))
        add(6, colsum(d_n2))
        g1 = g + norm_back(d_n2, xhat, rate, vec[5:6])
        r.g[rows, :] = g1
        add(4, colsum(g1))
        g1_low = g1.astype(BF)
        r.g1[rows, :] = g1_low
        da = mm(g1_low, wt.proj(l), NT)
        r.da_r[rows, :] = da[:, 0:128].astype(BF)
        add(8, colsum(da.astype(BF).astype(F32)))
        r.cells[3, map_rows(s)] = da[:, 128:256].reshape(STRIPE, WG, GROUP, 128)

    sweep(BF_, l, HP // STRIPE, feed, at)
    out.put(FC2, l, mm(r.gy[...], r.act[l], TN).astype(BF).T)
    at(B2_, l)
    out.put(FC1, l, mm(r.n2[l], r.slope[l], TN))
    out.put(PROJ, l, mm(r.a[l], r.g1[...], TN))
    at(BS_, l)

    def horizontal(s):
        rows = span(s, CHUNK)
        q, k, v = (r.row[i, l, rows, :] for i in range(3))
        da = r.da_r[rows, :]
        live = rows_live(s, h, w, 128)
        dq, dk, dv = attend_back(
            q, k, v, da, r.qs_r, r.dt_r, r.g_all, r.o_r.at[l], r.inv_r.at[l], r.p_r, s, WIDE_R
        )
        taps = [vec[9 + i : 10 + i, 0:128] for i in range(9)]
        da_near = row_neighbours(da.astype(F32))
        dv = (dv + position_back(da_near, taps).reshape(CHUNK, 128)) * live
        sums = tap_sums(da_near[1], row_neighbours(v.astype(F32)))
        for i in range(9):
            r.gv[9 + i : 10 + i, 0:128] += sums[i]
        r.gv[2:3, 0:128] += colsum(dq)
        r.gv[3:4, 0:128] += colsum(dv)
        for i, part in enumerate((dq, dk, dv)):
            r.dqkv_r[rows, 128 * i : 128 * i + 128] = part.astype(BF)

    sweep(BH_, l, HP // STRIPE, horizontal, at)
    out.put(QKV_R, l, mm(r.n1[l], r.dqkv_r[...], TN))
    at(BR_, l)

    def vertical(s):
        q, k, v = (r.col[i, l, s] for i in range(3))
        da = r.cells[3, :, s].reshape(TALL, 128).astype(BF)
        live = cols_live(s, h, w, 128)
        dq, dk, dv = attend_back(
            q, k, v, da, r.qs_c, r.dt_c, r.g_all, r.o_c.at[l], r.inv_c.at[l], r.p_c, s, WIDE_C
        )
        taps = [vec[9 + i : 10 + i, 128:256] for i in range(9)]
        da_near = col_neighbours(da.astype(F32))
        dv = (dv + position_back(da_near, taps).reshape(TALL, 128)) * live
        sums = tap_sums(da_near[1], col_neighbours(v.astype(F32)))
        for i in range(9):
            r.gv[9 + i : 10 + i, 128:256] += sums[i]
        r.gv[2:3, 128:256] += colsum(dq)
        r.gv[3:4, 128:256] += colsum(dv)
        for i, part in enumerate((dq, dk, dv)):
            r.cells[i, :, s] = part.reshape(HP, GROUP, 128)

    sweep(BV_, l, WG, vertical, at)

    def turn(s):
        rows = span(s, CHUNK)
        for i in range(3):
            cells = r.cells[i, map_rows(s)].reshape(CHUNK, 128)
            r.dqkv_c[rows, 128 * i : 128 * i + 128] = cells.astype(BF)

    sweep(BT_, l, HP // STRIPE, turn, at)
    out.put(QKV_C, l, mm(r.n1[l], r.dqkv_c[...], TN))
    at(BC_, l)

    def mix(s):
        rows = span(s, CHUNK)
        parts = []
        for i in range(3):
            lanes = slice(128 * i, 128 * i + 128)
            parts += [r.dqkv_r[rows, lanes], r.dqkv_c[rows, lanes]]
        d_n1 = mm(jnp.concatenate(parts, axis=1), wt.qkv(l), NT)
        xhat, rate = norm_parts(r.x[l, rows, :])
        add(0, colsum(d_n1 * xhat))
        add(1, colsum(d_n1))
        r.g[rows, :] += norm_back(d_n1, xhat, rate, vec[0:1])

    sweep(BM_, l, HP // STRIPE, mix, at)
    out.put(VEC, l, r.gv[...].T)
    at(BX_, l)


MESH = pl.DeviceIdType.MESH


class Grid:
    def __init__(self, shards, copies):
        self.cores = 2
        self.zs = 4
        self.xs = shards // 8
        self.copies = copies
        index = lax.axis_index("fsdp")
        self.rep = lax.axis_index("rep")
        self.core = lax.rem(index, 2)
        chip = lax.div(index, 2)
        self.x = lax.rem(chip, self.xs)
        self.z = lax.div(chip, self.xs)

    def at(self, z, x, core):
        return {"fsdp": (z * self.xs + x) * 2 + core, "rep": self.rep}

    def z_peers(self):
        return [(d, lax.rem(self.z + d, self.zs)) for d in range(1, self.zs)]

    def x_peers(self):
        return [(d, lax.rem(self.x + d, self.xs)) for d in range(1, self.xs)]

    def rep_peers(self):
        return [(d, lax.rem(self.rep + d, self.copies)) for d in range(1, self.copies)]

    def z_device(self, z):
        return self.at(z, self.x, self.core)

    def x_device(self, x):
        return self.at(self.z, x, self.core)

    def sibling(self):
        return self.at(self.z, self.x, 1 - self.core)

    def rep_device(self, rep):
        index = (self.z * self.xs + self.x) * 2 + self.core
        return {"fsdp": index, "rep": rep}

    def steps(self):
        return self.zs - 1 + self.xs - 1 + 1

    def peers(self):
        devices = [self.z_device(z) for _, z in self.z_peers()]
        devices += [self.x_device(x) for _, x in self.x_peers()] + [self.sibling()]
        return devices + [self.rep_device(rep) for _, rep in self.rep_peers()]

    def signal(self):
        for device in self.peers():
            pl.semaphore_signal(
                pltpu.get_barrier_semaphore(), inc=1, device_id=device, device_id_type=MESH
            )

    def wait(self):
        pl.semaphore_wait(pltpu.get_barrier_semaphore(), len(self.peers()))


def remote(src, dst, send, recv, device):
    return pltpu.make_async_remote_copy(
        src_ref=src, dst_ref=dst, send_sem=send, recv_sem=recv,
        device_id=device, device_id_type=MESH,
    )


class Gather:
    def __init__(self, grid, own, full, sems, row):
        self.grid, self.own, self.full = grid, own, full
        send, recv, local = sems
        g = grid
        mine = full.at[g.z, g.x, g.core]
        self.keep = pltpu.make_async_copy(own, mine, local.at[row])
        self.along_z = [
            remote(own, mine, send.at[row, d - 1], recv.at[row, d - 1], g.z_device(z))
            for d, z in g.z_peers()
        ]
        base = g.zs - 2
        lane = full.at[:, g.x, g.core]
        self.along_x = [
            remote(lane, lane, send.at[row, base + d], recv.at[row, base + d], g.x_device(x))
            for d, x in g.x_peers()
        ]
        last = g.zs - 1 + g.xs - 1
        plane = full.at[:, :, g.core]
        self.across = remote(plane, plane, send.at[row, last], recv.at[row, last], g.sibling())

    def begin(self):
        self.keep.start()
        for copy in self.along_z:
            copy.start()

    def second(self):
        self.keep.wait()
        for copy in self.along_z:
            copy.wait_recv()
        for copy in self.along_x:
            copy.start()

    def third(self):
        for copy in self.along_x:
            copy.wait_recv()
        self.across.start()

    def finish(self):
        self.across.wait_recv()

    def drain(self):
        for copy in self.along_z + self.along_x + [self.across]:
            copy.wait_send()


class Group:
    def __init__(self, parts):
        self.parts = parts

    def each(self, verb):
        for part in self.parts:
            getattr(part, verb)()

    def begin(self):
        self.each(VERBS[BEGIN])

    def second(self):
        self.each(VERBS[SECOND])

    def third(self):
        self.each(VERBS[THIRD])

    def finish(self):
        self.each(VERBS[FINISH])

    def drain(self):
        for part in self.parts:
            part.drain()


class Reduce:
    def __init__(self, grid, part, bufs, out, sems, row):
        self.grid, self.part, self.out = grid, part, out
        send, recv = sems
        g = grid
        self.from_sibling, self.from_x, self.from_z, self.from_rep = bufs
        self.chip, self.line, self.own = self.from_sibling, self.from_x.at[0], self.from_z.at[0]
        self.across = remote(
            part.at[:, :, 1 - g.core], self.from_sibling, send.at[row, 0], recv.at[row, 0], g.sibling()
        )
        self.along_x = [
            remote(self.chip.at[:, x], self.from_x.at[d - 1], send.at[row, d], recv.at[row, d], g.x_device(x))
            for d, x in g.x_peers()
        ]
        base = g.xs - 1
        self.along_z = [
            remote(self.line.at[z], self.from_z.at[d - 1], send.at[row, base + d], recv.at[row, base + d], g.z_device(z))
            for d, z in g.z_peers()
        ]
        base += g.zs - 1
        self.along_rep = [
            remote(self.own, self.from_rep.at[d - 1], send.at[row, base + d], recv.at[row, base + d], g.rep_device(rep))
            for d, rep in g.rep_peers()
        ]

    def begin(self):
        self.across.start()

    def second(self):
        self.across.wait_recv()
        mine = self.part[:, :, self.grid.core].astype(F32)
        self.chip[...] = (mine + self.chip[...].astype(F32)).astype(BF)
        for copy in self.along_x:
            copy.start()

    def third(self):
        for copy in self.along_x:
            copy.wait_recv()
        total = self.chip[:, self.grid.x].astype(F32)
        for d, _ in self.grid.x_peers():
            total = total + self.from_x[d - 1].astype(F32)
        self.line[...] = total.astype(BF)
        for copy in self.along_z:
            copy.start()

    def fourth(self):
        for copy in self.along_z:
            copy.wait_recv()
        total = self.line[self.grid.z].astype(F32)
        for d, _ in self.grid.z_peers():
            total = total + self.from_z[d - 1].astype(F32)
        self.own[...] = total.astype(BF)
        for copy in self.along_rep:
            copy.start()

    def finish(self):
        for copy in self.along_rep:
            copy.wait_recv()
        total = self.own[...].astype(F32)
        for d, _ in self.grid.rep_peers():
            total = total + self.from_rep[d - 1].astype(F32)
        held, half, self.leave = self.out
        if half is None:
            held[...] = total[:, 0 : held.shape[1]]
        else:
            for i in range(3):
                held[:, lanes_of(i, half)] = total[:, 128 * i : 128 * i + 128]
        if self.leave is not None:
            self.leave.start()

    def drain(self):
        for copy in [self.across] + self.along_x + self.along_z + self.along_rep:
            copy.wait_send()
        if self.leave is not None:
            self.leave.wait()


def reduce_bufs(zs, xs, copies, shape):
    dims = [(zs, xs), (xs - 1, zs), (zs - 1,), (copies - 1,)]
    return [pltpu.VMEM(d + tuple(shape), BF) for d in dims]


SCRATCH = dict(
    x=((3, ROWS, 256), F32),
    after=((2, ROWS, 256), F32),
    n1=((2, ROWS, 256), BF),
    n2=((2, ROWS, 256), BF),
    a=((2, ROWS, 256), BF),
    act=((2, ROWS, 1024), BF),
    slope=((2, ROWS, 1024), BF),
    row=((3, 2, ROWS, 128), BF),
    col=((3, 2, WG, TALL, 128), BF),
    cells=((4, HP, WG, GROUP, 128), F32),
    o_r=((2, HP // STRIPE, 128, WIDE_R), F32),
    o_c=((2, WG, 128, WIDE_C), F32),
    inv_r=((2, HP // STRIPE, 8, WIDE_R), F32),
    inv_c=((2, WG, 8, WIDE_C), F32),
    p_r=((HP // STRIPE, CHUNK, HEADS * WIDE_R), BF),
    p_c=((WG, TALL, HEADS * WIDE_C), BF),
    qs_r=((HEADS * WIDE_R, 256), BF),
    qs_c=((HEADS * WIDE_C, 256), BF),
    dt_r=((128, HEADS * WIDE_R), BF),
    dt_c=((128, HEADS * WIDE_C), BF),
    g_all=((CHUNK, HEADS * WIDE_R), BF),
    g=((ROWS, 256), F32),
    gy=((ROWS, 256), BF),
    g1=((ROWS, 256), BF),
    da_r=((ROWS, 128), BF),
    dqkv_r=((ROWS, 384), BF),
    dqkv_c=((ROWS, 384), BF),
    gv=((128, 256), F32),
    vec=((2, 128, 256), F32),
)


KEPT = ("p_r", "p_c")


class Refs:
    def __init__(self, names, refs):
        self.__dict__.update(zip(names, refs))


QKV, PROJ, FC1, FC2, QKV_R, QKV_C, VEC, SAVE, LOAD_R, LOAD_C = range(10)
MATRICES = (QKV, PROJ, FC1, FC2)
SUMMED = (FC2, FC1, PROJ, QKV_R, QKV_C, VEC)
BEGIN, SECOND, THIRD, FOURTH, FINISH = range(5)
VERBS = ("begin", "second", "third", "fourth", "finish")
P_, H_, V_, F_, G_, BF_, B2_, BS_, BH_, BR_, BV_, BT_, BC_, BM_, BX_, PC_ = range(16)
STRIDE = {P_: 4, F_: 4, BM_: 4, BT_: 4, G_: 4}


def lanes_of(block, half):
    return slice(256 * block + 128 * half, 256 * block + 128 * half + 128)


class Weights:
    def __init__(self, full):
        self.full = full

    def whole(self, name, l):
        value = self.full[name][l]
        return value.reshape(-1, value.shape[-1])

    def qkv_half(self, l, half):
        parts = []
        for i in range(3):
            value = self.full[QKV][l, :, :, :, :, lanes_of(i, half)]
            parts.append(value.reshape(-1, 128))
        return jnp.concatenate(parts, axis=1)

    def qkv(self, l):
        return self.whole(QKV, l)

    def proj(self, l):
        return self.whole(PROJ, l)

    def fc1(self, l):
        return self.whole(FC1, l)

    def fc2(self, l):
        return self.whole(FC2, l)


GATHER_MOVES = {
    (P_, 0, 3): [(QKV_C, 0, SECOND)],
    (H_, 0, 2): [(PROJ, 0, SECOND), (FC1, 0, SECOND), (QKV_C, 0, THIRD)],
    (H_, 0, 3): [(QKV, 1, BEGIN)],
    (PC_, 0, None): [(QKV_C, 0, FINISH)],
    (V_, 0, 0): [(FC2, 0, SECOND), (PROJ, 1, BEGIN)],
    (V_, 0, 3): [(FC1, 1, BEGIN)],
    (V_, 0, 4): [(PROJ, 0, THIRD), (FC1, 0, THIRD), (QKV, 1, SECOND)],
    (F_, 0, None): [(PROJ, 0, FINISH), (FC1, 0, FINISH), (SAVE, 0, BEGIN)],
    (F_, 0, 1): [(FC2, 0, THIRD), (FC2, 1, BEGIN)],
    (G_, 0, None): [(FC2, 0, FINISH)],
    (G_, 0, 1): [(QKV, 1, THIRD)],
    (P_, 1, None): [(QKV, 1, FINISH), (PROJ, 1, SECOND), (FC1, 1, SECOND)],
    (P_, 1, 3): [(SAVE, 0, FINISH)],
    (H_, 1, 1): [(FC2, 1, SECOND)],
    (V_, 1, 1): [(PROJ, 1, THIRD), (FC1, 1, THIRD)],
    (V_, 1, 4): [(FC2, 1, THIRD)],
    (F_, 1, None): [(PROJ, 1, FINISH), (FC1, 1, FINISH)],
    (G_, 1, None): [(FC2, 1, FINISH)],
}
SUM_MOVES = {
    (B2_, 1, None): [(FC2, 1, BEGIN)],
    (BS_, 1, None): [(FC1, 1, BEGIN), (PROJ, 1, BEGIN)],
    (BH_, 1, 0): [(FC2, 1, SECOND)],
    (BH_, 1, 1): [(FC1, 1, SECOND), (PROJ, 1, SECOND)],
    (BR_, 1, None): [(QKV_R, 1, BEGIN), (LOAD_R, 0, BEGIN)],
    (BV_, 1, 0): [(FC2, 1, THIRD)],
    (BV_, 1, 1): [(QKV_R, 1, SECOND)],
    (BV_, 1, 3): [(FC1, 1, THIRD), (PROJ, 1, THIRD)],
    (BV_, 1, 5): [(QKV_R, 1, THIRD)],
    (BC_, 1, None): [(QKV_C, 1, BEGIN), (LOAD_C, 0, BEGIN)],
    (BM_, 1, 1): [(FC2, 1, FOURTH)],
    (BM_, 1, 3): [(QKV_C, 1, SECOND)],
    (BX_, 1, None): [(VEC, 1, BEGIN)],
    (BF_, 0, 1): [(VEC, 1, SECOND)],
    (BF_, 0, 3): [(QKV_C, 1, THIRD), (FC1, 1, FOURTH), (PROJ, 1, FOURTH), (QKV_R, 1, FOURTH)],
    (B2_, 0, None): [(FC2, 0, BEGIN), (FC2, 1, FINISH)],
    (BS_, 0, None): [(FC1, 0, BEGIN), (PROJ, 0, BEGIN), (LOAD_R, 0, FINISH), (VEC, 1, THIRD)],
    (BH_, 0, 0): [(FC2, 0, SECOND)],
    (BH_, 0, 1): [
        (FC1, 0, SECOND), (PROJ, 0, SECOND), (FC1, 1, FINISH), (PROJ, 1, FINISH),
        (QKV_R, 1, FINISH),
    ],
    (BH_, 0, 3): [(QKV_C, 1, FOURTH), (VEC, 1, FOURTH)],
    (BR_, 0, None): [(QKV_R, 0, BEGIN), (LOAD_C, 0, FINISH)],
    (BV_, 0, 0): [(FC2, 0, THIRD)],
    (BV_, 0, 1): [(QKV_R, 0, SECOND)],
    (BV_, 0, 2): [(QKV_C, 1, FINISH), (VEC, 1, FINISH)],
    (BV_, 0, 3): [(FC1, 0, THIRD), (PROJ, 0, THIRD)],
    (BV_, 0, 5): [(QKV_R, 0, THIRD)],
    (BC_, 0, None): [(QKV_C, 0, BEGIN)],
    (BM_, 0, 1): [(FC2, 0, FOURTH), (QKV_C, 0, SECOND)],
    (BX_, 0, None): [(VEC, 0, BEGIN)],
}
LAST_MOVES = [
    (VEC, 0, SECOND), (FC1, 0, FOURTH), (PROJ, 0, FOURTH), (QKV_C, 0, THIRD),
    (VEC, 0, THIRD), (QKV_R, 0, FOURTH), (FC2, 0, FINISH), (FC1, 0, FINISH),
    (PROJ, 0, FINISH), (QKV_R, 0, FINISH), (QKV_C, 0, FOURTH), (VEC, 0, FOURTH),
    (QKV_C, 0, FINISH), (VEC, 0, FINISH),
]


class Local:
    def __init__(self, *copies):
        self.copies = copies

    def begin(self):
        for copy in self.copies:
            copy.start()

    def finish(self):
        for copy in self.copies:
            copy.wait()


class Moves:
    def __init__(self, table, parts):
        self.table, self.parts = table, parts

    def take(self, moves):
        for move in moves:
            name, l, verb = move
            getattr(self.parts[name, l], VERBS[verb])()

    def __call__(self, phase, l, step=None):
        if step is None:
            self.take(self.table.get((phase, l, None), []))
            return
        start, turn, stride = step
        for (name, block, when), moves in self.table.items():
            if (name, block) != (phase, l) or when is None or when % stride != turn:
                continue
            if start is None:
                self.take(moves)
            else:
                pl.when(start == when // stride)(functools.partial(self.take, moves))


def sweep(phase, l, count, body, at):
    stride = STRIDE.get(phase, 1)
    if stride == count:
        for s in range(count):
            body(s)
            at(phase, l, (None, s, stride))
        return

    def steps(i, carry):
        for turn in range(stride):
            body(i * stride + turn)
            at(phase, l, (i, turn, stride))
        return carry

    lax.fori_loop(0, count // stride, steps, 0)


class Gradients:
    def __init__(self, parts):
        self.parts = parts

    def put(self, name, l, value):
        ref = self.parts[name, l]
        ref[...] = value.astype(BF).reshape(ref.shape)


def plan(shards, copies, layers, width, hidden, held):
    zs, xs = 4, shards // 8
    place = (zs, xs, 2)
    d, f = width // shards, hidden // shards
    shapes = {k: pltpu.VMEM(*v) for k, v in SCRATCH.items()}
    own = {QKV: (d, 3 * width), PROJ: (d, width), FC1: (d, hidden), FC2: (f, width)}
    for name in MATRICES:
        shapes["full", name] = pltpu.VMEM((layers,) + place + own[name], BF)
    shapes["full", VEC] = pltpu.VMEM(place + (layers, d, held), BF)
    gathers = len(MATRICES) * layers + 1 + 6
    hops = zs - 1 + xs - 1 + 1
    for name in ("gather send", "gather recv"):
        shapes[name] = pltpu.SemaphoreType.DMA((gathers, hops))
    shapes["gather local"] = pltpu.SemaphoreType.DMA((gathers,))
    half = (d, 3 * width // 2)
    own.update({QKV_R: half, QKV_C: half, VEC: (d, 128)})
    sums = len(SUMMED) * layers
    hops += copies - 1
    for l in range(layers):
        for name in SUMMED:
            shapes["part", name, l] = pltpu.VMEM(place + own[name], BF)
            for i, buf in enumerate(reduce_bufs(zs, xs, copies, own[name])):
                shapes["buf", name, l, i] = buf
    for name in ("sum send", "sum recv"):
        shapes[name] = pltpu.SemaphoreType.DMA((sums, hops))
    shapes["out"] = pltpu.SemaphoreType.DMA((8 + 6 * layers,))
    for name in MATRICES:
        shapes["sum", name] = pltpu.VMEM((layers,) + own[name], F32)
    shapes["sum", VEC] = pltpu.VMEM((layers, d, held), F32)
    for name in ("tok", "cot"):
        shapes[name] = pltpu.VMEM((HP * WP, width), BF)
    return shapes


def step_kernel(shards, copies, names, *refs):
    h_ref, w_ref, tok, cot = refs[:4]
    own = dict(zip(MATRICES, refs[4:8]))
    vec_own = refs[8]
    y_ref, gt_ref = refs[9:11]
    outs = dict(zip(MATRICES + (VEC,), refs[11:16]))
    p_r_ref, p_c_ref = refs[16:18]
    s = dict(zip(names, refs[18:]))
    r = Refs(SCRATCH, [s[k] for k in SCRATCH])
    layers = own[QKV].shape[0]
    grid = Grid(shards, copies)
    grid.signal()
    h, w = h_ref[0], w_ref[0]

    sems = [s["gather send"], s["gather recv"], s["gather local"]]
    order = [(name, l) for l in range(layers) for name in MATRICES][1:]
    gathers = {
        (name, l): Gather(grid, own[name].at[l], s["full", name].at[l], sems, i)
        for i, (name, l) in enumerate(order)
    }
    gathers[VEC, 0] = Gather(grid, vec_own, s["full", VEC], sems, len(order))
    for half, name in enumerate((QKV_R, QKV_C)):
        parts = []
        for i in range(3):
            lanes = lanes_of(i, half)
            full = s["full", QKV].at[0, :, :, :, :, lanes]
            row = len(order) + 1 + 3 * half + i
            parts.append(Gather(grid, own[QKV].at[0, :, lanes], full, sems, row))
        gathers[name, 0] = Group(parts)
    wt = Weights({name: s["full", name] for name in MATRICES})

    def local(src, dst, i):
        return pltpu.make_async_copy(src, dst, s["out"].at[i])

    tok_copy, cot_copy = local(tok, s["tok"], 6), local(cot, s["cot"], 7)
    tok_copy.start()
    cot_copy.start()
    grid.wait()
    first = [gathers[QKV_R, 0], gathers[VEC, 0]]
    for one in first:
        one.begin()
    for stack in (r.qs_r, r.qs_c):
        stack[...] = jnp.where(iota(stack.shape, 1) == 128, 1.0, 0.0).astype(BF)
    for stack in (r.dt_r, r.dt_c):
        stack[...] = jnp.zeros_like(stack)
    r.gv[...] = jnp.zeros_like(r.gv)
    tok_copy.wait()
    pad_groups(s["tok"], r.x.at[0])
    cot_copy.wait()
    pad_groups(s["cot"], r.g)
    for one in first:
        one.second()
    gathers[QKV_C, 0].begin()
    for one in first:
        one.third()
    gathers[PROJ, 0].begin()
    gathers[FC1, 0].begin()
    for one in first:
        one.finish()
    gathers[FC2, 0].begin()
    for l in range(layers):
        value = s["full", VEC][:, :, :, l].astype(F32)
        value = value.reshape(-1, value.shape[-1])
        value = jnp.concatenate([value, jnp.zeros((value.shape[0], 128 - value.shape[1]), F32)], axis=1)
        r.vec[l] = value.T

    save = Local(local(r.p_r, p_r_ref, 2), local(r.p_c, p_c_ref, 3))
    at = Moves(GATHER_MOVES, {**gathers, (SAVE, 0): save})
    for l in range(layers):
        forward_layer(l, h, w, wt, r, at)

    sums = {}
    for l in range(layers):
        for i, name in enumerate(SUMMED):
            whole = QKV if name in (QKV_R, QKV_C) else name
            held = s["sum", whole].at[l]
            half = {QKV_R: 0, QKV_C: 1}.get(name)
            leave = None if half == 0 else local(held, outs[whole].at[l], 8 + l * 6 + i)
            out = (held, half, leave)
            bufs = [s["buf", name, l, j] for j in range(4)]
            row = l * len(SUMMED) + i
            sums[name, l] = Reduce(
                grid, s["part", name, l], bufs, out, [s["sum send"], s["sum recv"]], row
            )
    gradients = Gradients({(name, l): s["part", name, l] for l in range(layers) for name in SUMMED})

    load_r = Local(local(p_r_ref, r.p_r, 4))
    load_c = Local(local(p_c_ref, r.p_c, 5))
    at = Moves(SUM_MOVES, {**sums, (LOAD_R, 0): load_r, (LOAD_C, 0): load_c})
    for l in reversed(range(layers)):
        backward_layer(l, h, w, wt, r, gradients, at)
    flat = pl.ds(0, HP * WP)
    drop_groups(r.g, r.g)
    g_copy = local(r.g.at[flat], gt_ref, 1)
    g_copy.start()
    at.take(LAST_MOVES[:1])
    drop_groups(r.x.at[layers], r.x.at[layers])
    y_copy = local(r.x.at[layers, flat], y_ref, 0)
    y_copy.start()
    at.take(LAST_MOVES[1:])
    for one in list(gathers.values()) + list(sums.values()):
        one.drain()
    y_copy.wait()
    g_copy.wait()


PIECES = 3


def finish_kernel(count, *refs):
    src, dst, held = refs[:count], refs[count : 2 * count], refs[2 * count : 3 * count]
    sem_in, sem_out = refs[3 * count :]
    moves = []
    for i in range(count):
        pieces = PIECES if i < 2 else 1
        size = src[i].shape[0] // pieces
        for j in range(pieces):
            part = pl.ds(j * size, size)
            place = (i, j)
            first = pltpu.make_async_copy(src[i].at[part], held[i].at[part], sem_in.at[place])
            last = pltpu.make_async_copy(held[i].at[part], dst[i].at[part], sem_out.at[place])
            moves.append((first, last))
    for first, _ in moves:
        first.start()
    for first, last in moves:
        first.wait()
        last.start()
    for _, last in moves:
        last.wait()


def shards_step(shards, copies, tokens, heights, widths, w_qkv, w_proj, w_fc1, w_fc2, vectors, cotangent):
    layers, _, hidden = w_fc1.shape
    count, width = tokens.shape
    vmem = pl.BlockSpec(memory_space=pltpu.VMEM)
    smem = pl.BlockSpec(memory_space=pltpu.SMEM)
    hbm = pl.BlockSpec(memory_space=pl.ANY)
    turned = vectors.transpose(0, 2, 1)
    scratch = plan(shards, copies, layers, width, hidden, turned.shape[2])
    matrices = [w_qkv, w_proj, w_fc1, w_fc2]
    results = [jax.ShapeDtypeStruct((count, width), F32)] * 2
    results += [jax.ShapeDtypeStruct(m.shape, F32) for m in matrices]
    results += [jax.ShapeDtypeStruct(turned.shape, F32)]
    results += [jax.ShapeDtypeStruct(*SCRATCH[k]) for k in KEPT]
    *raw, _, _ = pl.pallas_call(
        functools.partial(step_kernel, shards, copies, list(scratch)),
        out_shape=results,
        in_specs=[smem, smem, hbm, hbm] + [hbm] * 5,
        out_specs=[hbm] * 9,
        scratch_shapes=list(scratch.values()),
        compiler_params=pltpu.CompilerParams(
            collective_id=0, has_side_effects=True, vmem_limit_bytes=67043328
        ),
    )(heights, widths, tokens, cotangent, *matrices, turned)
    final = [jax.ShapeDtypeStruct((count, width), F32)] * 2
    final += [jax.ShapeDtypeStruct(m.shape, F32) for m in matrices + [turned]]
    sems = pltpu.SemaphoreType.DMA((len(raw), PIECES))
    *arrays, vec = pl.pallas_call(
        functools.partial(finish_kernel, len(raw)),
        out_shape=final,
        in_specs=[hbm] * len(raw),
        out_specs=[hbm] * len(raw),
        scratch_shapes=[pltpu.VMEM(f.shape, F32) for f in final] + [sems, sems],
        compiler_params=pltpu.CompilerParams(vmem_limit_bytes=67043328),
    )(*raw)
    return (*arrays, vec.transpose(0, 2, 1))


def solution(mesh):
    images = P(("fsdp", "rep"), None)
    weights = P(None, "fsdp", None)
    return jax.shard_map(
        functools.partial(shards_step, mesh.shape["fsdp"], mesh.shape["rep"]),
        mesh=mesh,
        in_specs=(images, P(("fsdp", "rep")), P(("fsdp", "rep")), weights, weights, weights, weights, P(None, None, "fsdp"), images),
        out_specs=(images, images, weights, weights, weights, weights, P(None, None, "fsdp")),
        check_vma=False,
    )
```

```python
import functools
import jax
import jax.numpy as jnp
from jax import lax
from jax.experimental import pallas as pl
from jax.experimental.pallas import tpu as pltpu
from jax.sharding import PartitionSpec as P

HEAD = 32
STRIPE = 7
HP = 28
WP = 42
HEADS = 4
GROUP = 8
WG = WP // STRIPE
ROWS = HP * WG * GROUP
CHUNK = STRIPE * WG * GROUP
TALL = HP * GROUP
WIDE_R = 384
WIDE_C = 256
BF = jnp.bfloat16
F32 = jnp.float32
eps_norm = 1e-05
masked_score = -1000000000.0
LOG2E = 1.4426950408889634
LN2 = 0.6931471805599453
SCALE = HEAD ** (-0.5)
NN = (((1,), (0,)), ((), ()))
NT = (((1,), (1,)), ((), ()))
TN = (((0,), (0,)), ((), ()))


def mm(a, b, dims=NN):
    return lax.dot_general(a, b, dims, preferred_element_type=F32)


def iota(shape, dim):
    return lax.broadcasted_iota(jnp.int32, shape, dim)


def span(index, size):
    return pl.ds(pl.multiple_of(index * size, size), size)


def map_rows(stripe):
    return pl.ds(stripe * STRIPE, STRIPE)


def pad_groups(src, dst, scale=None):
    def body(j, carry):
        block = src[pl.ds(pl.multiple_of(j * 56, 8), 56), :].astype(F32).reshape(7, 8, -1)
        place = iota((8, block.shape[-1]), 0)
        for u in range(8):
            if u == 0:
                group = block[0]
            elif u == 7:
                group = pltpu.roll(block[6], 7, 0)
            else:
                group = jnp.where(
                    place < u, pltpu.roll(block[u - 1], u, 0), pltpu.roll(block[u], u, 0)
                )
            group = jnp.where(place < 7, group, 0.0)
            dst[pl.ds(pl.multiple_of(j * 64 + u * 8, 8), 8), :] = group
        return carry

    lax.fori_loop(0, ROWS // 64, body, 0)


def drop_groups(src, dst):
    def body(j, carry):
        block = src[pl.ds(pl.multiple_of(j * 64, 8), 64), :].reshape(8, 8, -1)
        place = iota((8, block.shape[-1]), 0)
        for t in range(7):
            lower = block[t] if t == 0 else pltpu.roll(block[t], 8 - t, 0)
            upper = pltpu.roll(block[t + 1], 7 - t, 0)
            dst[pl.ds(pl.multiple_of(j * 56 + t * 8, 8), 8), :] = jnp.where(
                place <= 6 - t, lower, upper
            )
        return carry

    lax.fori_loop(0, ROWS // 64, body, 0)


def norm_parts(x):
    centre = jnp.mean(x, axis=-1, keepdims=True)
    centred = x - centre
    rate = lax.rsqrt(jnp.mean(centred * centred, axis=-1, keepdims=True) + eps_norm)
    return centred * rate, rate


def norm_back(d_n, xhat, rate, gain):
    e = d_n * gain
    return rate * (
        e
        - jnp.mean(e, axis=-1, keepdims=True)
        - xhat * jnp.mean(e * xhat, axis=-1, keepdims=True)
    )


def colsum(x):
    return jnp.sum(x, axis=0, keepdims=True)


def rows_live(stripe, h, w, lanes):
    shape = (STRIPE, WG * GROUP, lanes)
    row = iota(shape, 0) + stripe * STRIPE
    place = iota(shape, 1)
    within = place & 7
    col = (place >> 3) * STRIPE + within
    live = (row < h) & (col < w) & (within < STRIPE)
    return jnp.where(live, 1.0, 0.0).reshape(CHUNK, lanes)


def cols_live(stripe, h, w, lanes):
    shape = (HP, GROUP, lanes)
    row = iota(shape, 0)
    within = iota(shape, 1)
    live = (row < h) & (within + stripe * STRIPE < w) & (within < STRIPE)
    return jnp.where(live, 1.0, 0.0).reshape(TALL, lanes)


def with_mask(keys, live):
    lane = iota(live.shape, 1)
    extra = jnp.where(lane == 0, jnp.where(live > 0.0, 0.0, masked_score), 0.0)
    return jnp.concatenate([keys, extra.astype(BF)], axis=-1)


def stack_heads(ref, x, wide):
    length = x.shape[0]
    lane = iota(x.shape, 1)
    for h in range(HEADS):
        kept = jnp.where((lane >> 5) == h, x, jnp.zeros_like(x))
        ref[h * wide : h * wide + length, 0:128] = kept


def widen(x, wide):
    length = x.shape[0]
    return jnp.concatenate([x, jnp.zeros((wide - length, x.shape[1]), x.dtype)], axis=0)


def attend(q, k_mask, vm, qs, out_t, inv, probs, stripe, wide):
    length = q.shape[0]
    stack_heads(qs, q, wide)
    scores = mm(k_mask, qs[0 : HEADS * wide, :], NT)
    v_t = widen(vm.astype(F32), wide).T.astype(BF)[:, 0:length]
    for h in range(HEADS):
        s = scores[:, h * wide : (h + 1) * wide]
        top = jnp.max(s, axis=0, keepdims=True)
        p = jnp.exp2(s - top)
        total = jnp.sum(p, axis=0, keepdims=True)
        p_low = p.astype(BF)
        probs[stripe, :, h * wide : (h + 1) * wide] = p_low
        rate = 1.0 / total
        inv[stripe, h : h + 1, :] = rate
        o = mm(v_t[HEAD * h : HEAD * (h + 1), :], p_low)
        out_t[stripe, HEAD * h : HEAD * (h + 1), :] = o * rate


def attend_back(q, k, vm, da, qs, da_stack, g_all, out_t, inv, probs, stripe, wide):
    length = q.shape[0]
    stack_heads(qs, q, wide)
    da_t = widen(da.astype(F32), wide).T
    k_t = widen(k.astype(F32), wide).T.astype(BF)[:, 0:length]
    inner = []
    for h in range(HEADS):
        rows = slice(HEAD * h, HEAD * (h + 1))
        scaled = (da_t[rows, :] * inv[stripe, h : h + 1, :]).astype(BF)
        da_stack[rows, h * wide : (h + 1) * wide] = scaled
        inner.append(colsum(scaled.astype(F32) * out_t[stripe, rows, :]))
    d_probs = mm(vm, da_stack[...])
    dq_t = []
    for h in range(HEADS):
        lanes = slice(h * wide, (h + 1) * wide)
        p = probs[stripe, :, lanes].astype(F32)
        g = (p * (d_probs[:, lanes] - inner[h])).astype(BF)
        g_all[0:length, lanes] = g
        dq_t.append(mm(k_t[HEAD * h : HEAD * (h + 1), :], g))
    dv = mm(probs[stripe], da_stack[...], NT)
    dk = mm(g_all[0:length, 0 : HEADS * wide], qs[0 : HEADS * wide, 0:128]) * LN2
    dq = jnp.concatenate(dq_t, axis=0).T[0:length, :] * SCALE
    return dq, dk, dv


def earlier(x):
    return jnp.concatenate([jnp.zeros_like(x[:1]), x[:-1]], axis=0)


def later(x):
    return jnp.concatenate([x[1:], jnp.zeros_like(x[:1])], axis=0)


def row_neighbours(x):
    groups = x.reshape(STRIPE * WG, GROUP, 128)
    place = iota(groups.shape, 1)
    edge = jnp.zeros((STRIPE, 1, GROUP, 128), x.dtype)
    far = pltpu.roll(groups, 2, 1).reshape(STRIPE, WG, GROUP, 128)
    far = jnp.concatenate([edge, far[:, :-1]], axis=1).reshape(groups.shape)
    left = jnp.where(place == 0, far, pltpu.roll(groups, 1, 1))
    far = pltpu.roll(groups, 6, 1).reshape(STRIPE, WG, GROUP, 128)
    far = jnp.concatenate([far[:, 1:], edge], axis=1).reshape(groups.shape)
    right = jnp.where(place == 6, far, pltpu.roll(groups, 7, 1))
    shape = (STRIPE, WG * GROUP, 128)
    return left.reshape(shape), x.reshape(shape), right.reshape(shape)


def col_neighbours(x):
    cells = x.reshape(HP, GROUP, 128)
    return pltpu.roll(cells, 1, 1), cells, pltpu.roll(cells, 7, 1)


def position(near, taps):
    rows = [sum(taps[3 * a + b] * near[b] for b in range(3)) for a in range(3)]
    return earlier(rows[0]) + rows[1] + later(rows[2])


def position_back(near, taps):
    rows = [sum(taps[3 * a + b] * near[2 - b] for b in range(3)) for a in range(3)]
    return later(rows[0]) + rows[1] + earlier(rows[2])


def tap_sums(da, near):
    sums = []
    for a in range(3):
        for b in range(3):
            x = near[b]
            x = earlier(x) if a == 0 else later(x) if a == 2 else x
            sums.append(colsum((da * x).reshape(-1, 128)))
    return sums


def forward_layer(l, h, w, wt, r, at):
    at(P_, l)
    vec = r.vec[l]

    def keep_row(rows, parts):
        for i, part in enumerate(parts):
            r.row[i, l, rows, :] = part.astype(BF)

    def keep_col(s, parts):
        for i, part in enumerate(parts):
            r.cells[i, map_rows(s)] = part.reshape(STRIPE, WG, GROUP, 128)

    def split(mixed, s, half, lanes):
        here = slice(128 * half, 128 * half + 128)
        q = (mixed[:, lanes[0]] + vec[2:3, here]) * (SCALE * LOG2E)
        v = (mixed[:, lanes[2]] + vec[3:4, here]) * rows_live(s, h, w, 128)
        return q, mixed[:, lanes[1]], v

    def norm(s):
        rows = span(s, CHUNK)
        xhat, rate = norm_parts(r.x[l, rows, :])
        n1 = (xhat * vec[0:1] + vec[1:2]).astype(BF)
        r.n1[l, rows, :] = n1
        return rows, n1

    alone = [slice(128 * i, 128 * i + 128) for i in range(3)]

    def project(s):
        rows, n1 = norm(s)
        mixed = mm(n1, wt.qkv(l))
        for half in range(2):
            lanes = [slice(256 * i + 128 * half, 256 * i + 128 * half + 128) for i in range(3)]
            parts = split(mixed, s, half, lanes)
            keep_col(s, parts) if half else keep_row(rows, parts)

    def project_row(s):
        rows, n1 = norm(s)
        keep_row(rows, split(mm(n1, wt.qkv_half(l, 0)), s, 0, alone))

    def project_col(s):
        n1 = r.n1[l, span(s, CHUNK), :]
        keep_col(s, split(mm(n1, wt.qkv_half(l, 1)), s, 1, alone))

    sweep(P_, l, HP // STRIPE, project if l else project_row, at)

    at(H_, l)

    def horizontal(s):
        rows = span(s, CHUNK)
        q, k, v = (r.row[i, l, rows, :] for i in range(3))
        attend(q, with_mask(k, rows_live(s, h, w, 128)), v, r.qs_r, r.o_r.at[l], r.inv_r.at[l], r.p_r, s, WIDE_R)
        near = row_neighbours(v.astype(F32))
        taps = vec[9:18, 0:128]
        pos = position(near, [taps[i : i + 1] for i in range(9)]) + vec[8:9, 0:128]
        o = r.o_r[l, s].T[0:CHUNK, :]
        r.a[l, rows, 0:128] = (o + pos.reshape(CHUNK, 128)).astype(BF)

    sweep(H_, l, HP // STRIPE, horizontal, at)
    at(PC_, l)
    if l == 0:
        sweep(PC_, l, HP // STRIPE, project_col, at)

    def vertical(s):
        q, k, v = (r.cells[i, :, s].reshape(TALL, 128).astype(BF) for i in range(3))
        for i, part in enumerate((q, k, v)):
            r.col[i, l, s] = part
        attend(q, with_mask(k, cols_live(s, h, w, 128)), v, r.qs_c, r.o_c.at[l], r.inv_c.at[l], r.p_c, s, WIDE_C)
        near = col_neighbours(v.astype(F32))
        taps = vec[9:18, 128:256]
        pos = position(near, [taps[i : i + 1] for i in range(9)]) + vec[8:9, 128:256]
        o = r.o_c[l, s].T[0:TALL, :]
        r.cells[3, :, s] = o.reshape(HP, GROUP, 128) + pos

    sweep(V_, l, WG, vertical, at)

    at(F_, l)

    def feed(s):
        rows = span(s, CHUNK)
        turned = r.cells[3, map_rows(s)].reshape(CHUNK, 128).astype(BF)
        r.a[l, rows, 128:256] = turned
        x1 = r.x[l, rows, :] + mm(r.a[l, rows, :], wt.proj(l)) + vec[4:5]
        r.after[l, rows, :] = x1
        xhat, rate = norm_parts(x1)
        n2 = (xhat * vec[5:6] + vec[6:7]).astype(BF)
        r.n2[l, rows, :] = n2
        hidden_bias = jnp.concatenate([vec[18 + j : 19 + j] for j in range(4)], axis=1)
        hid = mm(n2, wt.fc1(l)) + hidden_bias
        phi = 0.5 * lax.erf(hid * 0.7071067811865476) + 0.5
        slope = phi + hid * (jnp.exp2(hid * hid * (-0.5 * LOG2E)) * 0.3989422804014327)
        act = (hid * phi).astype(BF)
        r.act[l, rows, :] = act
        r.slope[l, rows, :] = slope.astype(BF)

    sweep(F_, l, HP // STRIPE, feed, at)
    at(G_, l)

    def close(s):
        rows = span(s, CHUNK)
        x1 = r.after[l, rows, :]
        r.x[l + 1, rows, :] = x1 + mm(r.act[l, rows, :], wt.fc2(l)) + vec[7:8]

    sweep(G_, l, HP // STRIPE, close, at)


def backward_layer(l, h, w, wt, r, out, at):
    vec = r.vec[l]
    r.gv[...] = jnp.zeros_like(r.gv)

    def add(row, value):
        r.gv[row : row + 1, :] += value

    def feed(s):
        rows = span(s, CHUNK)
        g = r.g[rows, :]
        add(7, colsum(g))
        gy = g.astype(BF)
        r.gy[rows, :] = gy
        d_hid = mm(gy, wt.fc2(l), NT) * r.slope[l, rows, :].astype(F32)
        for j in range(4):
            add(18 + j, colsum(d_hid[:, 256 * j : 256 * (j + 1)]))
        dh = d_hid.astype(BF)
        r.slope[l, rows, :] = dh
        d_n2 = mm(dh, wt.fc1(l), NT)
        xhat, rate = norm_parts(r.after[l, rows, :])
        add(5, colsum(d_n2 * xhat))
        add(6, colsum(d_n2))
        g1 = g + norm_back(d_n2, xhat, rate, vec[5:6])
        r.g[rows, :] = g1
        add(4, colsum(g1))
        g1_low = g1.astype(BF)
        r.g1[rows, :] = g1_low
        da = mm(g1_low, wt.proj(l), NT)
        r.da_r[rows, :] = da[:, 0:128].astype(BF)
        add(8, colsum(da.astype(BF).astype(F32)))
        r.cells[3, map_rows(s)] = da[:, 128:256].reshape(STRIPE, WG, GROUP, 128)

    sweep(BF_, l, HP // STRIPE, feed, at)
    out.put(FC2, l, mm(r.gy[...], r.act[l], TN).astype(BF).T)
    at(B2_, l)
    out.put(FC1, l, mm(r.n2[l], r.slope[l], TN))
    out.put(PROJ, l, mm(r.a[l], r.g1[...], TN))
    at(BS_, l)

    def horizontal(s):
        rows = span(s, CHUNK)
        q, k, v = (r.row[i, l, rows, :] for i in range(3))
        da = r.da_r[rows, :]
        live = rows_live(s, h, w, 128)
        dq, dk, dv = attend_back(
            q, k, v, da, r.qs_r, r.dt_r, r.g_all, r.o_r.at[l], r.inv_r.at[l], r.p_r, s, WIDE_R
        )
        taps = [vec[9 + i : 10 + i, 0:128] for i in range(9)]
        da_near = row_neighbours(da.astype(F32))
        dv = (dv + position_back(da_near, taps).reshape(CHUNK, 128)) * live
        sums = tap_sums(da_near[1], row_neighbours(v.astype(F32)))
        for i in range(9):
            r.gv[9 + i : 10 + i, 0:128] += sums[i]
        r.gv[2:3, 0:128] += colsum(dq)
        r.gv[3:4, 0:128] += colsum(dv)
        for i, part in enumerate((dq, dk, dv)):
            r.dqkv_r[rows, 128 * i : 128 * i + 128] = part.astype(BF)

    sweep(BH_, l, HP // STRIPE, horizontal, at)
    out.put(QKV_R, l, mm(r.n1[l], r.dqkv_r[...], TN))
    at(BR_, l)

    def vertical(s):
        q, k, v = (r.col[i, l, s] for i in range(3))
        da = r.cells[3, :, s].reshape(TALL, 128).astype(BF)
        live = cols_live(s, h, w, 128)
        dq, dk, dv = attend_back(
            q, k, v, da, r.qs_c, r.dt_c, r.g_all, r.o_c.at[l], r.inv_c.at[l], r.p_c, s, WIDE_C
        )
        taps = [vec[9 + i : 10 + i, 128:256] for i in range(9)]
        da_near = col_neighbours(da.astype(F32))
        dv = (dv + position_back(da_near, taps).reshape(TALL, 128)) * live
        sums = tap_sums(da_near[1], col_neighbours(v.astype(F32)))
        for i in range(9):
            r.gv[9 + i : 10 + i, 128:256] += sums[i]
        r.gv[2:3, 128:256] += colsum(dq)
        r.gv[3:4, 128:256] += colsum(dv)
        for i, part in enumerate((dq, dk, dv)):
            r.cells[i, :, s] = part.reshape(HP, GROUP, 128)

    sweep(BV_, l, WG, vertical, at)

    def turn(s):
        rows = span(s, CHUNK)
        for i in range(3):
            cells = r.cells[i, map_rows(s)].reshape(CHUNK, 128)
            r.dqkv_c[rows, 128 * i : 128 * i + 128] = cells.astype(BF)

    sweep(BT_, l, HP // STRIPE, turn, at)
    out.put(QKV_C, l, mm(r.n1[l], r.dqkv_c[...], TN))
    at(BC_, l)

    def mix(s):
        rows = span(s, CHUNK)
        parts = []
        for i in range(3):
            lanes = slice(128 * i, 128 * i + 128)
            parts += [r.dqkv_r[rows, lanes], r.dqkv_c[rows, lanes]]
        d_n1 = mm(jnp.concatenate(parts, axis=1), wt.qkv(l), NT)
        xhat, rate = norm_parts(r.x[l, rows, :])
        add(0, colsum(d_n1 * xhat))
        add(1, colsum(d_n1))
        r.g[rows, :] += norm_back(d_n1, xhat, rate, vec[0:1])

    sweep(BM_, l, HP // STRIPE, mix, at)
    out.put(VEC, l, r.gv[...].T)
    at(BX_, l)


MESH = pl.DeviceIdType.MESH


class Grid:
    def __init__(self, shards, copies):
        self.cores = 2
        self.zs = 4
        self.xs = shards // 8
        self.copies = copies
        index = lax.axis_index("fsdp")
        self.rep = lax.axis_index("rep")
        self.core = lax.rem(index, 2)
        chip = lax.div(index, 2)
        self.x = lax.rem(chip, self.xs)
        self.z = lax.div(chip, self.xs)

    def at(self, z, x, core, rep=None):
        index = (z * self.xs + x) * 2 + core
        return {"fsdp": index, "rep": self.rep if rep is None else rep}

    def z_peers(self):
        return [(d, lax.rem(self.z + d, self.zs)) for d in range(1, self.zs)]

    def x_peers(self):
        return [(d, lax.rem(self.x + d, self.xs)) for d in range(1, self.xs)]

    def rep_peers(self):
        return [(d, lax.rem(self.rep + d, self.copies)) for d in range(1, self.copies)]

    def z_device(self, z):
        return self.at(z, self.x, self.core)

    def x_device(self, x):
        return self.at(self.z, x, self.core)

    def sibling(self):
        return self.at(self.z, self.x, 1 - self.core)

    def peers(self):
        devices = [self.sibling()]
        for dz in range(self.zs):
            for dx in range(self.xs):
                for dr in range(self.copies):
                    if dz + dx + dr:
                        z, x = lax.rem(self.z + dz, self.zs), lax.rem(self.x + dx, self.xs)
                        rep = lax.rem(self.rep + dr, self.copies)
                        devices.append(self.at(z, x, self.core, rep))
        return devices

    def signal(self):
        for device in self.peers():
            pl.semaphore_signal(
                pltpu.get_barrier_semaphore(), inc=1, device_id=device, device_id_type=MESH
            )

    def wait(self):
        pl.semaphore_wait(pltpu.get_barrier_semaphore(), len(self.peers()))


def remote(src, dst, send, recv, device):
    return pltpu.make_async_remote_copy(
        src_ref=src, dst_ref=dst, send_sem=send, recv_sem=recv,
        device_id=device, device_id_type=MESH,
    )


def take_all(ref, sem):
    pltpu.make_async_copy(ref, ref, sem).wait()


class Gather:
    def __init__(self, grid, parts, like, sems, row):
        self.grid, self.like = grid, like
        g = grid
        send, recv, local = sems
        self.send, self.local = send.at[row], local.at[row]
        self.recv = [recv.at[row, i] for i in range(3)]
        self.keep, self.along_z, self.along_x, self.across = [], [], [], []
        for own, full in parts:
            mine = full.at[g.z, g.x, g.core]
            line, plane = full.at[:, g.x, g.core], full.at[:, :, g.core]
            self.keep.append(pltpu.make_async_copy(own, mine, self.local))
            for _, z in g.z_peers():
                self.along_z.append(remote(own, mine, self.send, self.recv[0], g.z_device(z)))
            for _, x in g.x_peers():
                self.along_x.append(remote(line, line, self.send, self.recv[1], g.x_device(x)))
            self.across.append(remote(plane, plane, self.send, self.recv[2], g.sibling()))

    def start(self, copies):
        for copy in copies:
            copy.start()

    def taken(self, phase, ref):
        take_all(ref, self.recv[phase])
        take_all(ref, self.send)

    def begin(self):
        self.start(self.keep)
        self.start(self.along_z)

    def second(self):
        g = self.grid
        take_all(self.like.at[0, 0, 0], self.local)
        self.taken(0, self.like.at[0 : g.zs - 1, g.x, g.core])
        self.start(self.along_x)

    def third(self):
        g = self.grid
        self.taken(1, self.like.at[:, 0 : g.xs - 1, g.core])
        self.start(self.across)

    def finish(self):
        self.taken(2, self.like.at[:, :, self.grid.core])


class Reduce:
    def __init__(self, grid, part, bufs, out, sems, row, wide):
        self.grid, self.part, self.out, self.wide = grid, part, out, wide
        send, recv = sems
        g = grid
        self.send = send.at[row]
        self.recv = [recv.at[row, i] for i in range(4)]
        self.chip, self.last = bufs[0], bufs[-1]
        self.across = [
            remote(part.at[:, :, 1 - g.core], self.chip, self.send, self.recv[0], g.sibling())
        ]
        self.along_x, self.along_z, self.along_rep = [], [], []
        if wide < 2:
            self.from_x = bufs[1]
            self.line = self.from_x.at[0]
            for d, x in g.x_peers():
                here = self.from_x.at[d - 1]
                device = g.x_device(x)
                self.along_x.append(remote(self.chip.at[:, x], here, self.send, self.recv[1], device))
        if wide:
            for dz, dx, dr in self.steps():
                z, to = lax.rem(g.z + dz, g.zs), lax.rem(g.rep + dr, g.copies)
                x = lax.rem(g.x + dx, g.xs)
                source = self.line.at[z] if wide == 1 else self.chip.at[z, x]
                if dz + dx + dr:
                    here = self.last.at[self.slot(dz, dx, dr)]
                    device = g.at(z, x, g.core, to)
                    self.along_rep.append(remote(source, here, self.send, self.recv[3], device))
            return
        self.from_z = bufs[2]
        self.own = self.from_z.at[0]
        for d, z in g.z_peers():
            self.along_z.append(
                remote(self.line.at[z], self.from_z.at[d - 1], self.send, self.recv[2], g.z_device(z))
            )
        for d, to in g.rep_peers():
            device = g.at(g.z, g.x, g.core, to)
            self.along_rep.append(remote(self.own, self.last.at[d], self.send, self.recv[3], device))

    def steps(self):
        g = self.grid
        zs, xs = (g.zs if self.wide else 1), (g.xs if self.wide == 2 else 1)
        return [(a, b, c) for a in range(zs) for b in range(xs) for c in range(g.copies)]

    def slot(self, dz, dx, dr):
        g = self.grid
        return (dz * (g.xs if self.wide == 2 else 1) + dx) * g.copies + dr

    def start(self, copies):
        for copy in copies:
            copy.start()

    def taken(self, phase, ref):
        take_all(ref, self.recv[phase])
        take_all(ref, self.send)

    def begin(self):
        self.start(self.across)

    def second(self):
        self.taken(0, self.chip)
        mine = self.part[:, :, self.grid.core].astype(F32)
        self.chip[...] = (mine + self.chip[...].astype(F32)).astype(BF)
        if self.wide == 2:
            self.last[0] = self.chip[self.grid.z, self.grid.x]
            self.start(self.along_rep)
        else:
            self.start(self.along_x)

    def third(self):
        g = self.grid
        self.taken(1, self.from_x)
        total = self.chip[:, g.x].astype(F32)
        for d, _ in g.x_peers():
            total = total + self.from_x[d - 1].astype(F32)
        self.line[...] = total.astype(BF)
        if self.wide:
            self.last[0] = self.line[g.z]
            self.start(self.along_rep)
        else:
            self.start(self.along_z)

    def fourth(self):
        g = self.grid
        self.taken(2, self.from_z)
        total = self.line[g.z].astype(F32)
        for d, _ in g.z_peers():
            total = total + self.from_z[d - 1].astype(F32)
        self.own[...] = total.astype(BF)
        self.last[0] = self.own[...]
        self.start(self.along_rep)

    def finish(self):
        g = self.grid
        slots = self.last.shape[0]
        self.taken(3, self.last.at[1:slots])
        total = None
        for z, x, rep in self.steps():
            dz = lax.rem(g.z - z + g.zs, g.zs) if self.wide else 0
            dx = lax.rem(g.x - x + g.xs, g.xs) if self.wide == 2 else 0
            value = self.last[self.slot(dz, dx, lax.rem(g.rep - rep + g.copies, g.copies))]
            total = value.astype(F32) if total is None else total + value.astype(F32)
        held, half, self.leave = self.out
        if half is None:
            held[...] = total[:, 0 : held.shape[1]]
        else:
            for i in range(3):
                held[:, lanes_of(i, half)] = total[:, 128 * i : 128 * i + 128]
        if self.leave is not None:
            self.leave.start()

    def drain(self):
        if self.leave is not None:
            self.leave.wait()


def reduce_bufs(zs, xs, copies, shape, wide):
    dims = [(zs, xs)]
    if wide < 2:
        dims.append((xs - 1, zs))
    if wide == 0:
        dims.append((zs - 1,))
    dims.append((copies * (1, zs, zs * xs)[wide],))
    return [pltpu.VMEM(d + tuple(shape), BF) for d in dims]


SCRATCH = dict(
    x=((3, ROWS, 256), F32),
    after=((2, ROWS, 256), F32),
    n1=((2, ROWS, 256), BF),
    n2=((2, ROWS, 256), BF),
    a=((2, ROWS, 256), BF),
    act=((2, ROWS, 1024), BF),
    slope=((2, ROWS, 1024), BF),
    row=((3, 2, ROWS, 128), BF),
    col=((3, 2, WG, TALL, 128), BF),
    cells=((4, HP, WG, GROUP, 128), F32),
    o_r=((2, HP // STRIPE, 128, WIDE_R), F32),
    o_c=((2, WG, 128, WIDE_C), F32),
    inv_r=((2, HP // STRIPE, 8, WIDE_R), F32),
    inv_c=((2, WG, 8, WIDE_C), F32),
    p_r=((HP // STRIPE, CHUNK, HEADS * WIDE_R), BF),
    p_c=((WG, TALL, HEADS * WIDE_C), BF),
    qs_r=((HEADS * WIDE_R, 256), BF),
    qs_c=((HEADS * WIDE_C, 256), BF),
    dt_r=((128, HEADS * WIDE_R), BF),
    dt_c=((128, HEADS * WIDE_C), BF),
    g_all=((CHUNK, HEADS * WIDE_R), BF),
    g=((ROWS, 256), F32),
    gy=((ROWS, 256), BF),
    g1=((ROWS, 256), BF),
    da_r=((ROWS, 128), BF),
    dqkv_r=((ROWS, 384), BF),
    dqkv_c=((ROWS, 384), BF),
    gv=((128, 256), F32),
    vec=((2, 128, 256), F32),
)


KEPT = ("p_r", "p_c")


class Refs:
    def __init__(self, names, refs):
        self.__dict__.update(zip(names, refs))


QKV, PROJ, FC1, FC2, QKV_R, QKV_C, VEC, SAVE, LOAD_R, LOAD_C = range(10)
MATRICES = (QKV, PROJ, FC1, FC2)
SUMMED = (FC2, FC1, PROJ, QKV_R, QKV_C, VEC)
BEGIN, SECOND, THIRD, FOURTH, FINISH = range(5)
VERBS = ("begin", "second", "third", "fourth", "finish")
P_, H_, V_, F_, G_, BF_, B2_, BS_, BH_, BR_, BV_, BT_, BC_, BM_, BX_, PC_ = range(16)
STRIDE = {P_: 4, F_: 4, BM_: 4, BT_: 4, G_: 4}


def lanes_of(block, half):
    return slice(256 * block + 128 * half, 256 * block + 128 * half + 128)


class Weights:
    def __init__(self, full):
        self.full = full

    def whole(self, name, l):
        value = self.full[name][l]
        return value.reshape(-1, value.shape[-1])

    def qkv_half(self, l, half):
        parts = []
        for i in range(3):
            value = self.full[QKV][l, :, :, :, :, lanes_of(i, half)]
            parts.append(value.reshape(-1, 128))
        return jnp.concatenate(parts, axis=1)

    def qkv(self, l):
        return self.whole(QKV, l)

    def proj(self, l):
        return self.whole(PROJ, l)

    def fc1(self, l):
        return self.whole(FC1, l)

    def fc2(self, l):
        return self.whole(FC2, l)


GATHER_MOVES = {
    (P_, 0, 3): [(QKV_C, 0, SECOND)],
    (H_, 0, 2): [(PROJ, 0, SECOND), (FC1, 0, SECOND), (QKV_C, 0, THIRD)],
    (H_, 0, 3): [(QKV, 1, BEGIN)],
    (PC_, 0, None): [(QKV_C, 0, FINISH)],
    (V_, 0, 0): [(FC2, 0, SECOND), (PROJ, 1, BEGIN)],
    (V_, 0, 3): [(FC1, 1, BEGIN)],
    (V_, 0, 4): [(PROJ, 0, THIRD), (FC1, 0, THIRD), (QKV, 1, SECOND)],
    (F_, 0, None): [(PROJ, 0, FINISH), (FC1, 0, FINISH), (SAVE, 0, BEGIN)],
    (F_, 0, 1): [(FC2, 0, THIRD), (FC2, 1, BEGIN)],
    (G_, 0, None): [(FC2, 0, FINISH)],
    (G_, 0, 1): [(QKV, 1, THIRD)],
    (P_, 1, None): [(QKV, 1, FINISH), (PROJ, 1, SECOND), (FC1, 1, SECOND)],
    (P_, 1, 3): [(SAVE, 0, FINISH)],
    (H_, 1, 1): [(FC2, 1, SECOND)],
    (V_, 1, 1): [(PROJ, 1, THIRD), (FC1, 1, THIRD)],
    (V_, 1, 4): [(FC2, 1, THIRD)],
    (F_, 1, None): [(PROJ, 1, FINISH), (FC1, 1, FINISH)],
    (G_, 1, None): [(FC2, 1, FINISH)],
}
SUM_MOVES = {
    (B2_, 1, None): [(FC2, 1, BEGIN)],
    (BS_, 1, None): [(FC1, 1, BEGIN), (PROJ, 1, BEGIN)],
    (BH_, 1, 0): [(FC2, 1, SECOND)],
    (BH_, 1, 1): [(FC1, 1, SECOND), (PROJ, 1, SECOND)],
    (BR_, 1, None): [(QKV_R, 1, BEGIN), (LOAD_R, 0, BEGIN)],
    (BV_, 1, 0): [(FC2, 1, THIRD)],
    (BV_, 1, 1): [(QKV_R, 1, SECOND)],
    (BV_, 1, 3): [(FC1, 1, THIRD), (PROJ, 1, THIRD)],
    (BV_, 1, 5): [(QKV_R, 1, THIRD)],
    (BC_, 1, None): [(QKV_C, 1, BEGIN), (LOAD_C, 0, BEGIN)],
    (BM_, 1, 1): [(FC2, 1, FOURTH)],
    (BM_, 1, 3): [(QKV_C, 1, SECOND)],
    (BX_, 1, None): [(VEC, 1, BEGIN)],
    (BF_, 0, 1): [(VEC, 1, SECOND)],
    (BF_, 0, 3): [(QKV_C, 1, THIRD), (FC1, 1, FOURTH), (PROJ, 1, FOURTH), (QKV_R, 1, FOURTH)],
    (B2_, 0, None): [(FC2, 0, BEGIN), (FC2, 1, FINISH)],
    (BS_, 0, None): [(FC1, 0, BEGIN), (PROJ, 0, BEGIN), (LOAD_R, 0, FINISH), (VEC, 1, THIRD)],
    (BH_, 0, 0): [(FC2, 0, SECOND)],
    (BH_, 0, 1): [
        (FC1, 0, SECOND), (PROJ, 0, SECOND), (FC1, 1, FINISH), (PROJ, 1, FINISH),
        (QKV_R, 1, FINISH),
    ],
    (BH_, 0, 3): [(QKV_C, 1, FOURTH), (VEC, 1, FOURTH)],
    (BR_, 0, None): [(QKV_R, 0, BEGIN), (LOAD_C, 0, FINISH)],
    (BV_, 0, 0): [(FC2, 0, THIRD)],
    (BV_, 0, 1): [(QKV_R, 0, SECOND)],
    (BV_, 0, 2): [(QKV_C, 1, FINISH), (VEC, 1, FINISH)],
    (BV_, 0, 3): [(FC1, 0, THIRD), (PROJ, 0, THIRD)],
    (BV_, 0, 5): [(QKV_R, 0, THIRD)],
    (BC_, 0, None): [(QKV_C, 0, BEGIN)],
    (BM_, 0, 1): [(FC2, 0, FOURTH), (QKV_C, 0, SECOND)],
    (BX_, 0, None): [(VEC, 0, BEGIN)],
}
LAST_MOVES = [
    (VEC, 0, SECOND), (QKV_C, 0, THIRD), (QKV_R, 0, FOURTH), (FC1, 0, FOURTH), (PROJ, 0, FOURTH),
    (FC2, 0, FINISH), (QKV_R, 0, FINISH), (FC1, 0, FINISH), (PROJ, 0, FINISH),
    (VEC, 0, FINISH), (QKV_C, 0, FINISH),
]
WIDE = {(QKV_C, 0): 1, (VEC, 0): 2}


class Local:
    def __init__(self, *copies):
        self.copies = copies

    def begin(self):
        for copy in self.copies:
            copy.start()

    def finish(self):
        for copy in self.copies:
            copy.wait()


class Moves:
    def __init__(self, table, parts):
        self.table, self.parts = table, parts

    def take(self, moves):
        for move in moves:
            name, l, verb = move
            getattr(self.parts[name, l], VERBS[verb])()

    def __call__(self, phase, l, step=None):
        if step is None:
            self.take(self.table.get((phase, l, None), []))
            return
        start, turn, stride = step
        for (name, block, when), moves in self.table.items():
            if (name, block) != (phase, l) or when is None or when % stride != turn:
                continue
            if start is None:
                self.take(moves)
            else:
                pl.when(start == when // stride)(functools.partial(self.take, moves))


def sweep(phase, l, count, body, at):
    stride = STRIDE.get(phase, 1)
    if stride == count:
        for s in range(count):
            body(s)
            at(phase, l, (None, s, stride))
        return

    def steps(i, carry):
        for turn in range(stride):
            body(i * stride + turn)
            at(phase, l, (i, turn, stride))
        return carry

    lax.fori_loop(0, count // stride, steps, 0)


class Gradients:
    def __init__(self, parts):
        self.parts = parts

    def put(self, name, l, value):
        ref = self.parts[name, l]
        ref[...] = value.astype(BF).reshape(ref.shape)


def plan(shards, copies, layers, width, hidden, held):
    zs, xs = 4, shards // 8
    place = (zs, xs, 2)
    d, f = width // shards, hidden // shards
    shapes = {k: pltpu.VMEM(*v) for k, v in SCRATCH.items()}
    own = {QKV: (d, 3 * width), PROJ: (d, width), FC1: (d, hidden), FC2: (f, width)}
    for name in MATRICES:
        shapes["full", name] = pltpu.VMEM((layers,) + place + own[name], BF)
    shapes["full", VEC] = pltpu.VMEM(place + (layers, d, held), BF)
    gathers = len(MATRICES) * layers + 2
    shapes["gather send"] = pltpu.SemaphoreType.DMA((gathers,))
    shapes["gather recv"] = pltpu.SemaphoreType.DMA((gathers, 3))
    shapes["gather local"] = pltpu.SemaphoreType.DMA((gathers,))
    half = (d, 3 * width // 2)
    own.update({QKV_R: half, QKV_C: half, VEC: (d, 128)})
    sums = len(SUMMED) * layers
    for l in range(layers):
        for name in SUMMED:
            shapes["part", name, l] = pltpu.VMEM(place + own[name], BF)
            for i, buf in enumerate(reduce_bufs(zs, xs, copies, own[name], WIDE.get((name, l), 0))):
                shapes["buf", name, l, i] = buf
    shapes["sum send"] = pltpu.SemaphoreType.DMA((sums,))
    shapes["sum recv"] = pltpu.SemaphoreType.DMA((sums, 4))
    shapes["out"] = pltpu.SemaphoreType.DMA((8 + 6 * layers,))
    for name in MATRICES:
        shapes["sum", name] = pltpu.VMEM((layers,) + own[name], F32)
    shapes["sum", VEC] = pltpu.VMEM((layers, d, held), F32)
    for name in ("tok", "cot"):
        shapes[name] = pltpu.VMEM((HP * WP, width), BF)
    return shapes


def step_kernel(shards, copies, names, *refs):
    h_ref, w_ref, tok, cot = refs[:4]
    own = dict(zip(MATRICES, refs[4:8]))
    vec_own = refs[8]
    y_ref, gt_ref = refs[9:11]
    outs = dict(zip(MATRICES + (VEC,), refs[11:16]))
    p_r_ref, p_c_ref = refs[16:18]
    s = dict(zip(names, refs[18:]))
    r = Refs(SCRATCH, [s[k] for k in SCRATCH])
    layers = own[QKV].shape[0]
    grid = Grid(shards, copies)
    grid.signal()
    h, w = h_ref[0], w_ref[0]

    sems = [s["gather send"], s["gather recv"], s["gather local"]]
    order = [(name, l) for l in range(layers) for name in MATRICES][1:]
    gathers = {}
    for i, (name, l) in enumerate(order):
        full = s["full", name].at[l]
        gathers[name, l] = Gather(grid, [(own[name].at[l], full)], full, sems, i)
    full = s["full", VEC]
    gathers[VEC, 0] = Gather(grid, [(vec_own, full)], full, sems, len(order))
    full = s["full", QKV].at[0]
    for half, name in enumerate((QKV_R, QKV_C)):
        parts = []
        for i in range(3):
            lanes = lanes_of(i, half)
            parts.append((own[QKV].at[0, :, lanes], full.at[:, :, :, :, lanes]))
        like = full.at[:, :, :, :, 0 : full.shape[-1] // 2]
        gathers[name, 0] = Gather(grid, parts, like, sems, len(order) + 1 + half)
    wt = Weights({name: s["full", name] for name in MATRICES})

    def local(src, dst, i):
        return pltpu.make_async_copy(src, dst, s["out"].at[i])

    tok_copy, cot_copy = local(tok, s["tok"], 6), local(cot, s["cot"], 7)
    tok_copy.start()
    cot_copy.start()
    grid.wait()
    first = [gathers[QKV_R, 0], gathers[VEC, 0]]
    for one in first:
        one.begin()
    for stack in (r.qs_r, r.qs_c):
        stack[...] = jnp.where(iota(stack.shape, 1) == 128, 1.0, 0.0).astype(BF)
    for stack in (r.dt_r, r.dt_c):
        stack[...] = jnp.zeros_like(stack)
    r.gv[...] = jnp.zeros_like(r.gv)
    tok_copy.wait()
    pad_groups(s["tok"], r.x.at[0])
    cot_copy.wait()
    pad_groups(s["cot"], r.g)
    for one in first:
        one.second()
    gathers[QKV_C, 0].begin()
    for one in first:
        one.third()
    gathers[PROJ, 0].begin()
    gathers[FC1, 0].begin()
    for one in first:
        one.finish()
    gathers[FC2, 0].begin()
    for l in range(layers):
        value = s["full", VEC][:, :, :, l].astype(F32)
        value = value.reshape(-1, value.shape[-1])
        value = jnp.concatenate([value, jnp.zeros((value.shape[0], 128 - value.shape[1]), F32)], axis=1)
        r.vec[l] = value.T

    save = Local(local(r.p_r, p_r_ref, 2), local(r.p_c, p_c_ref, 3))
    at = Moves(GATHER_MOVES, {**gathers, (SAVE, 0): save})
    for l in range(layers):
        forward_layer(l, h, w, wt, r, at)

    sums = {}
    for l in range(layers):
        for i, name in enumerate(SUMMED):
            whole = QKV if name in (QKV_R, QKV_C) else name
            held = s["sum", whole].at[l]
            half = {QKV_R: 0, QKV_C: 1}.get(name)
            leave = None if half == 0 else local(held, outs[whole].at[l], 8 + l * 6 + i)
            out = (held, half, leave)
            wide = WIDE.get((name, l), 0)
            bufs = [s["buf", name, l, j] for j in range(4 - wide)]
            row = l * len(SUMMED) + i
            sums[name, l] = Reduce(
                grid, s["part", name, l], bufs, out, [s["sum send"], s["sum recv"]], row, wide
            )
    gradients = Gradients({(name, l): s["part", name, l] for l in range(layers) for name in SUMMED})

    load_r = Local(local(p_r_ref, r.p_r, 4))
    load_c = Local(local(p_c_ref, r.p_c, 5))
    at = Moves(SUM_MOVES, {**sums, (LOAD_R, 0): load_r, (LOAD_C, 0): load_c})
    for l in reversed(range(layers)):
        backward_layer(l, h, w, wt, r, gradients, at)
    flat = pl.ds(0, HP * WP)
    drop_groups(r.g, r.g)
    g_copy = local(r.g.at[flat], gt_ref, 1)
    g_copy.start()
    at.take(LAST_MOVES[:1])
    drop_groups(r.x.at[layers], r.x.at[layers])
    y_copy = local(r.x.at[layers, flat], y_ref, 0)
    y_copy.start()
    at.take(LAST_MOVES[1:])
    for one in sums.values():
        one.drain()
    y_copy.wait()
    g_copy.wait()


PIECES = 3


def finish_kernel(count, *refs):
    src, dst, held = refs[:count], refs[count : 2 * count], refs[2 * count : 3 * count]
    sems = refs[3 * count]
    moves = []
    for i in range(count):
        pieces = PIECES if i < 2 else 1
        size = src[i].shape[0] // pieces
        for j in range(pieces):
            part, sem = pl.ds(j * size, size), sems.at[len(moves)]
            first = pltpu.make_async_copy(src[i].at[part], held[i].at[part], sem)
            moves.append((first, pltpu.make_async_copy(held[i].at[part], dst[i].at[part], sem)))
    for first, _ in moves:
        first.start()
    for first, last in moves:
        first.wait()
        last.start()
    for _, last in moves:
        last.wait()


def shards_step(shards, copies, tokens, heights, widths, w_qkv, w_proj, w_fc1, w_fc2, vectors, cotangent):
    layers, _, hidden = w_fc1.shape
    count, width = tokens.shape
    vmem = pl.BlockSpec(memory_space=pltpu.VMEM)
    smem = pl.BlockSpec(memory_space=pltpu.SMEM)
    hbm = pl.BlockSpec(memory_space=pl.ANY)
    turned = vectors.transpose(0, 2, 1)
    scratch = plan(shards, copies, layers, width, hidden, turned.shape[2])
    matrices = [w_qkv, w_proj, w_fc1, w_fc2]
    results = [jax.ShapeDtypeStruct((count, width), F32)] * 2
    results += [jax.ShapeDtypeStruct(m.shape, F32) for m in matrices]
    results += [jax.ShapeDtypeStruct(turned.shape, F32)]
    results += [jax.ShapeDtypeStruct(*SCRATCH[k]) for k in KEPT]
    *raw, _, _ = pl.pallas_call(
        functools.partial(step_kernel, shards, copies, list(scratch)),
        out_shape=results,
        in_specs=[smem, smem, hbm, hbm] + [hbm] * 5,
        out_specs=[hbm] * 9,
        scratch_shapes=list(scratch.values()),
        compiler_params=pltpu.CompilerParams(
            collective_id=0, has_side_effects=True, vmem_limit_bytes=67043328
        ),
    )(heights, widths, tokens, cotangent, *matrices, turned)
    final = [jax.ShapeDtypeStruct((count, width), F32)] * 2
    final += [jax.ShapeDtypeStruct(m.shape, F32) for m in matrices + [turned]]
    sems = pltpu.SemaphoreType.DMA((2 * PIECES + len(raw) - 2,))
    *arrays, vec = pl.pallas_call(
        functools.partial(finish_kernel, len(raw)),
        out_shape=final,
        in_specs=[hbm] * len(raw),
        out_specs=[hbm] * len(raw),
        scratch_shapes=[pltpu.VMEM(f.shape, F32) for f in final] + [sems],
        compiler_params=pltpu.CompilerParams(vmem_limit_bytes=67043328),
    )(*raw)
    return (*arrays, vec.transpose(0, 2, 1))


def solution(mesh):
    images = P(("fsdp", "rep"), None)
    weights = P(None, "fsdp", None)
    return jax.shard_map(
        functools.partial(shards_step, mesh.shape["fsdp"], mesh.shape["rep"]),
        mesh=mesh,
        in_specs=(images, P(("fsdp", "rep")), P(("fsdp", "rep")), weights, weights, weights, weights, P(None, None, "fsdp"), images),
        out_specs=(images, images, weights, weights, weights, weights, P(None, None, "fsdp")),
        check_vma=False,
    )
```

```python
import functools
import jax
import jax.numpy as jnp
from jax import lax
from jax.experimental import pallas as pl
from jax.experimental.pallas import tpu as pltpu
from jax.sharding import PartitionSpec as P

HEAD = 32
STRIPE = 7
HP = 28
WP = 42
HEADS = 4
GROUP = 8
WG = WP // STRIPE
ROWS = HP * WG * GROUP
CHUNK = STRIPE * WG * GROUP
TALL = HP * GROUP
WIDE_R = 384
WIDE_C = 256
BF = jnp.bfloat16
F32 = jnp.float32
eps_norm = 1e-05
masked_score = -1000000000.0
LOG2E = 1.4426950408889634
LN2 = 0.6931471805599453
SCALE = HEAD ** (-0.5)
NN = (((1,), (0,)), ((), ()))
NT = (((1,), (1,)), ((), ()))
TN = (((0,), (0,)), ((), ()))


def mm(a, b, dims=NN):
    return lax.dot_general(a, b, dims, preferred_element_type=F32)


def iota(shape, dim):
    return lax.broadcasted_iota(jnp.int32, shape, dim)


def span(index, size):
    return pl.ds(pl.multiple_of(index * size, size), size)


def map_rows(stripe):
    return pl.ds(stripe * STRIPE, STRIPE)


def pad_groups(src, dst, scale=None):
    def body(j, carry):
        block = src[pl.ds(pl.multiple_of(j * 56, 8), 56), :].astype(F32).reshape(7, 8, -1)
        place = iota((8, block.shape[-1]), 0)
        for u in range(8):
            if u == 0:
                group = block[0]
            elif u == 7:
                group = pltpu.roll(block[6], 7, 0)
            else:
                group = jnp.where(
                    place < u, pltpu.roll(block[u - 1], u, 0), pltpu.roll(block[u], u, 0)
                )
            group = jnp.where(place < 7, group, 0.0)
            dst[pl.ds(pl.multiple_of(j * 64 + u * 8, 8), 8), :] = group
        return carry

    lax.fori_loop(0, ROWS // 64, body, 0)


def drop_groups(src, dst):
    def body(j, carry):
        block = src[pl.ds(pl.multiple_of(j * 64, 8), 64), :].reshape(8, 8, -1)
        place = iota((8, block.shape[-1]), 0)
        for t in range(7):
            lower = block[t] if t == 0 else pltpu.roll(block[t], 8 - t, 0)
            upper = pltpu.roll(block[t + 1], 7 - t, 0)
            dst[pl.ds(pl.multiple_of(j * 56 + t * 8, 8), 8), :] = jnp.where(
                place <= 6 - t, lower, upper
            )
        return carry

    lax.fori_loop(0, ROWS // 64, body, 0)


def norm_parts(x):
    centre = jnp.mean(x, axis=-1, keepdims=True)
    centred = x - centre
    rate = lax.rsqrt(jnp.mean(centred * centred, axis=-1, keepdims=True) + eps_norm)
    return centred * rate, rate


def norm_back(d_n, xhat, rate, gain):
    e = d_n * gain
    return rate * (
        e
        - jnp.mean(e, axis=-1, keepdims=True)
        - xhat * jnp.mean(e * xhat, axis=-1, keepdims=True)
    )


def colsum(x):
    return jnp.sum(x, axis=0, keepdims=True)


def rows_live(stripe, h, w, lanes):
    shape = (STRIPE, WG * GROUP, lanes)
    row = iota(shape, 0) + stripe * STRIPE
    place = iota(shape, 1)
    within = place & 7
    col = (place >> 3) * STRIPE + within
    live = (row < h) & (col < w) & (within < STRIPE)
    return jnp.where(live, 1.0, 0.0).reshape(CHUNK, lanes)


def cols_live(stripe, h, w, lanes):
    shape = (HP, GROUP, lanes)
    row = iota(shape, 0)
    within = iota(shape, 1)
    live = (row < h) & (within + stripe * STRIPE < w) & (within < STRIPE)
    return jnp.where(live, 1.0, 0.0).reshape(TALL, lanes)


def with_mask(keys, live):
    lane = iota(live.shape, 1)
    extra = jnp.where(lane == 0, jnp.where(live > 0.0, 0.0, masked_score), 0.0)
    return jnp.concatenate([keys, extra.astype(BF)], axis=-1)


def stack_heads(ref, x, wide):
    length = x.shape[0]
    lane = iota(x.shape, 1)
    for h in range(HEADS):
        kept = jnp.where((lane >> 5) == h, x, jnp.zeros_like(x))
        ref[h * wide : h * wide + length, 0:128] = kept


def widen(x, wide):
    length = x.shape[0]
    return jnp.concatenate([x, jnp.zeros((wide - length, x.shape[1]), x.dtype)], axis=0)


def attend(q, k_mask, vm, qs, out_t, inv, probs, stripe, wide):
    length = q.shape[0]
    stack_heads(qs, q, wide)
    scores = mm(k_mask, qs[0 : HEADS * wide, :], NT)
    v_t = widen(vm.astype(F32), wide).T.astype(BF)[:, 0:length]
    for h in range(HEADS):
        s = scores[:, h * wide : (h + 1) * wide]
        top = jnp.max(s, axis=0, keepdims=True)
        p = jnp.exp2(s - top)
        total = jnp.sum(p, axis=0, keepdims=True)
        p_low = p.astype(BF)
        probs[stripe, :, h * wide : (h + 1) * wide] = p_low
        rate = 1.0 / total
        inv[stripe, h : h + 1, :] = rate
        o = mm(v_t[HEAD * h : HEAD * (h + 1), :], p_low)
        out_t[stripe, HEAD * h : HEAD * (h + 1), :] = o * rate


def attend_back(q, k, vm, da, qs, da_stack, g_all, out_t, inv, probs, stripe, wide):
    length = q.shape[0]
    stack_heads(qs, q, wide)
    da_t = widen(da.astype(F32), wide).T
    k_t = widen(k.astype(F32), wide).T.astype(BF)[:, 0:length]
    inner = []
    for h in range(HEADS):
        rows = slice(HEAD * h, HEAD * (h + 1))
        scaled = (da_t[rows, :] * inv[stripe, h : h + 1, :]).astype(BF)
        da_stack[rows, h * wide : (h + 1) * wide] = scaled
        inner.append(colsum(scaled.astype(F32) * out_t[stripe, rows, :]))
    d_probs = mm(vm, da_stack[...])
    dq_t = []
    for h in range(HEADS):
        lanes = slice(h * wide, (h + 1) * wide)
        p = probs[stripe, :, lanes].astype(F32)
        g = (p * (d_probs[:, lanes] - inner[h])).astype(BF)
        g_all[0:length, lanes] = g
        dq_t.append(mm(k_t[HEAD * h : HEAD * (h + 1), :], g))
    dv = mm(probs[stripe], da_stack[...], NT)
    dk = mm(g_all[0:length, 0 : HEADS * wide], qs[0 : HEADS * wide, 0:128]) * LN2
    dq = jnp.concatenate(dq_t, axis=0).T[0:length, :] * SCALE
    return dq, dk, dv


def earlier(x):
    return jnp.concatenate([jnp.zeros_like(x[:1]), x[:-1]], axis=0)


def later(x):
    return jnp.concatenate([x[1:], jnp.zeros_like(x[:1])], axis=0)


def row_neighbours(x):
    groups = x.reshape(STRIPE * WG, GROUP, 128)
    place = iota(groups.shape, 1)
    edge = jnp.zeros((STRIPE, 1, GROUP, 128), x.dtype)
    far = pltpu.roll(groups, 2, 1).reshape(STRIPE, WG, GROUP, 128)
    far = jnp.concatenate([edge, far[:, :-1]], axis=1).reshape(groups.shape)
    left = jnp.where(place == 0, far, pltpu.roll(groups, 1, 1))
    far = pltpu.roll(groups, 6, 1).reshape(STRIPE, WG, GROUP, 128)
    far = jnp.concatenate([far[:, 1:], edge], axis=1).reshape(groups.shape)
    right = jnp.where(place == 6, far, pltpu.roll(groups, 7, 1))
    shape = (STRIPE, WG * GROUP, 128)
    return left.reshape(shape), x.reshape(shape), right.reshape(shape)


def col_neighbours(x):
    cells = x.reshape(HP, GROUP, 128)
    return pltpu.roll(cells, 1, 1), cells, pltpu.roll(cells, 7, 1)


def position(near, taps):
    rows = [sum(taps[3 * a + b] * near[b] for b in range(3)) for a in range(3)]
    return earlier(rows[0]) + rows[1] + later(rows[2])


def position_back(near, taps):
    rows = [sum(taps[3 * a + b] * near[2 - b] for b in range(3)) for a in range(3)]
    return later(rows[0]) + rows[1] + earlier(rows[2])


def tap_sums(da, near):
    sums = []
    for a in range(3):
        for b in range(3):
            x = near[b]
            x = earlier(x) if a == 0 else later(x) if a == 2 else x
            sums.append(colsum((da * x).reshape(-1, 128)))
    return sums


def forward_layer(l, h, w, wt, r, at):
    at(P_, l)
    vec = r.vec[l]

    def keep_row(rows, parts):
        for i, part in enumerate(parts):
            r.row[i, l, rows, :] = part.astype(BF)

    def keep_col(s, parts):
        for i, part in enumerate(parts):
            r.cells[i, map_rows(s)] = part.reshape(STRIPE, WG, GROUP, 128)

    def split(mixed, s, half, lanes):
        here = slice(128 * half, 128 * half + 128)
        q = (mixed[:, lanes[0]] + vec[2:3, here]) * (SCALE * LOG2E)
        v = (mixed[:, lanes[2]] + vec[3:4, here]) * rows_live(s, h, w, 128)
        return q, mixed[:, lanes[1]], v

    def norm(s):
        rows = span(s, CHUNK)
        xhat = norm_parts(r.x[l, rows, :])[0] if l else r.after[0, rows, :]
        n1 = (xhat * vec[0:1] + vec[1:2]).astype(BF)
        r.n1[l, rows, :] = n1
        return rows, n1

    alone = [slice(128 * i, 128 * i + 128) for i in range(3)]

    def project(s):
        rows, n1 = norm(s)
        mixed = mm(n1, wt.qkv(l))
        for half in range(2):
            lanes = [slice(256 * i + 128 * half, 256 * i + 128 * half + 128) for i in range(3)]
            parts = split(mixed, s, half, lanes)
            keep_col(s, parts) if half else keep_row(rows, parts)

    def project_row(s):
        rows, n1 = norm(s)
        keep_row(rows, split(mm(n1, wt.qkv_half(l, 0)), s, 0, alone))

    def project_col(s):
        n1 = r.n1[l, span(s, CHUNK), :]
        keep_col(s, split(mm(n1, wt.qkv_half(l, 1)), s, 1, alone))

    sweep(P_, l, HP // STRIPE, project if l else project_row, at)

    at(H_, l)

    def horizontal(s):
        rows = span(s, CHUNK)
        q, k, v = (r.row[i, l, rows, :] for i in range(3))
        attend(q, with_mask(k, rows_live(s, h, w, 128)), v, r.qs_r, r.o_r.at[l], r.inv_r.at[l], r.p_r, s, WIDE_R)
        near = row_neighbours(v.astype(F32))
        taps = vec[9:18, 0:128]
        pos = position(near, [taps[i : i + 1] for i in range(9)]) + vec[8:9, 0:128]
        o = r.o_r[l, s].T[0:CHUNK, :]
        r.a[l, rows, 0:128] = (o + pos.reshape(CHUNK, 128)).astype(BF)

    sweep(H_, l, HP // STRIPE, horizontal, at)
    at(PC_, l)
    if l == 0:
        sweep(PC_, l, HP // STRIPE, project_col, at)

    def vertical(s):
        q, k, v = (r.cells[i, :, s].reshape(TALL, 128).astype(BF) for i in range(3))
        for i, part in enumerate((q, k, v)):
            r.col[i, l, s] = part
        attend(q, with_mask(k, cols_live(s, h, w, 128)), v, r.qs_c, r.o_c.at[l], r.inv_c.at[l], r.p_c, s, WIDE_C)
        near = col_neighbours(v.astype(F32))
        taps = vec[9:18, 128:256]
        pos = position(near, [taps[i : i + 1] for i in range(9)]) + vec[8:9, 128:256]
        o = r.o_c[l, s].T[0:TALL, :]
        r.cells[3, :, s] = o.reshape(HP, GROUP, 128) + pos

    sweep(V_, l, WG, vertical, at)

    at(F_, l)

    def feed(s):
        rows = span(s, CHUNK)
        turned = r.cells[3, map_rows(s)].reshape(CHUNK, 128).astype(BF)
        r.a[l, rows, 128:256] = turned
        x1 = r.x[l, rows, :] + mm(r.a[l, rows, :], wt.proj(l)) + vec[4:5]
        r.after[l, rows, :] = x1
        xhat, rate = norm_parts(x1)
        n2 = (xhat * vec[5:6] + vec[6:7]).astype(BF)
        r.n2[l, rows, :] = n2
        for j in range(4):
            lanes = slice(256 * j, 256 * j + 256)
            hid = mm(n2, wt.fc1(l)[:, lanes]) + vec[18 + j : 19 + j]
            phi = 0.5 * lax.erf(hid * 0.7071067811865476) + 0.5
            bell = jnp.exp2(hid * hid * (-0.5 * LOG2E)) * 0.3989422804014327
            r.act[l, rows, lanes] = (hid * phi).astype(BF)
            r.slope[l, rows, lanes] = (phi + hid * bell).astype(BF)

    sweep(F_, l, HP // STRIPE, feed, at)
    at(G_, l)

    def close(s):
        rows = span(s, CHUNK)
        x1 = r.after[l, rows, :]
        r.x[l + 1, rows, :] = x1 + mm(r.act[l, rows, :], wt.fc2(l)) + vec[7:8]

    sweep(G_, l, HP // STRIPE, close, at)


def backward_layer(l, h, w, wt, r, out, at):
    vec = r.vec[l]
    r.gv[...] = jnp.zeros_like(r.gv)

    def add(row, value):
        r.gv[row : row + 1, :] += value

    def feed(s):
        rows = span(s, CHUNK)
        g = r.g[rows, :]
        add(7, colsum(g))
        gy = g.astype(BF)
        r.gy[rows, :] = gy
        for j in range(4):
            lanes = slice(256 * j, 256 * j + 256)
            d_hid = mm(gy, wt.fc2(l)[lanes], NT) * r.slope[l, rows, lanes].astype(F32)
            add(18 + j, colsum(d_hid))
            r.slope[l, rows, lanes] = d_hid.astype(BF)
        dh = r.slope[l, rows, :]
        d_n2 = mm(dh, wt.fc1(l), NT)
        xhat, rate = norm_parts(r.after[l, rows, :])
        add(5, colsum(d_n2 * xhat))
        add(6, colsum(d_n2))
        g1 = g + norm_back(d_n2, xhat, rate, vec[5:6])
        r.g[rows, :] = g1
        add(4, colsum(g1))
        g1_low = g1.astype(BF)
        r.g1[rows, :] = g1_low
        da = mm(g1_low, wt.proj(l), NT)
        r.da_r[rows, :] = da[:, 0:128].astype(BF)
        add(8, colsum(da.astype(BF).astype(F32)))
        r.cells[3, map_rows(s)] = da[:, 128:256].reshape(STRIPE, WG, GROUP, 128)

    sweep(BF_, l, HP // STRIPE, feed, at)
    out.put(FC2, l, mm(r.gy[...], r.act[l], TN).astype(BF).T)
    at(B2_, l)
    out.put(FC1, l, mm(r.n2[l], r.slope[l], TN))
    out.put(PROJ, l, mm(r.a[l], r.g1[...], TN))
    at(BS_, l)

    def horizontal(s):
        rows = span(s, CHUNK)
        q, k, v = (r.row[i, l, rows, :] for i in range(3))
        da = r.da_r[rows, :]
        live = rows_live(s, h, w, 128)
        dq, dk, dv = attend_back(
            q, k, v, da, r.qs_r, r.dt_r, r.g_all, r.o_r.at[l], r.inv_r.at[l], r.p_r, s, WIDE_R
        )
        taps = [vec[9 + i : 10 + i, 0:128] for i in range(9)]
        da_near = row_neighbours(da.astype(F32))
        dv = (dv + position_back(da_near, taps).reshape(CHUNK, 128)) * live
        sums = tap_sums(da_near[1], row_neighbours(v.astype(F32)))
        for i in range(9):
            r.gv[9 + i : 10 + i, 0:128] += sums[i]
        r.gv[2:3, 0:128] += colsum(dq)
        r.gv[3:4, 0:128] += colsum(dv)
        for i, part in enumerate((dq, dk, dv)):
            r.dqkv_r[rows, 128 * i : 128 * i + 128] = part.astype(BF)

    sweep(BH_, l, HP // STRIPE, horizontal, at)
    out.put(QKV_R, l, mm(r.n1[l], r.dqkv_r[...], TN))
    at(BR_, l)

    def vertical(s):
        q, k, v = (r.col[i, l, s] for i in range(3))
        da = r.cells[3, :, s].reshape(TALL, 128).astype(BF)
        live = cols_live(s, h, w, 128)
        dq, dk, dv = attend_back(
            q, k, v, da, r.qs_c, r.dt_c, r.g_all, r.o_c.at[l], r.inv_c.at[l], r.p_c, s, WIDE_C
        )
        taps = [vec[9 + i : 10 + i, 128:256] for i in range(9)]
        da_near = col_neighbours(da.astype(F32))
        dv = (dv + position_back(da_near, taps).reshape(TALL, 128)) * live
        sums = tap_sums(da_near[1], col_neighbours(v.astype(F32)))
        for i in range(9):
            r.gv[9 + i : 10 + i, 128:256] += sums[i]
        r.gv[2:3, 128:256] += colsum(dq)
        r.gv[3:4, 128:256] += colsum(dv)
        for i, part in enumerate((dq, dk, dv)):
            r.cells[i, :, s] = part.reshape(HP, GROUP, 128)

    sweep(BV_, l, WG, vertical, at)

    def turn(s):
        rows = span(s, CHUNK)
        for i in range(3):
            cells = r.cells[i, map_rows(s)].reshape(CHUNK, 128)
            r.dqkv_c[rows, 128 * i : 128 * i + 128] = cells.astype(BF)

    sweep(BT_, l, HP // STRIPE, turn, at)
    out.put(QKV_C, l, mm(r.n1[l], r.dqkv_c[...], TN))
    at(BC_, l)

    def mix(s):
        rows = span(s, CHUNK)
        parts = []
        for i in range(3):
            lanes = slice(128 * i, 128 * i + 128)
            parts += [r.dqkv_r[rows, lanes], r.dqkv_c[rows, lanes]]
        d_n1 = mm(jnp.concatenate(parts, axis=1), wt.qkv(l), NT)
        xhat, rate = norm_parts(r.x[l, rows, :])
        add(0, colsum(d_n1 * xhat))
        add(1, colsum(d_n1))
        r.g[rows, :] += norm_back(d_n1, xhat, rate, vec[0:1])

    sweep(BM_, l, HP // STRIPE, mix, at)
    out.put(VEC, l, r.gv[...].T)
    at(BX_, l)


MESH = pl.DeviceIdType.MESH


class Grid:
    def __init__(self, shards, copies):
        self.cores = 2
        self.zs = 4
        self.xs = shards // 8
        self.copies = copies
        index = lax.axis_index("fsdp")
        self.rep = lax.axis_index("rep")
        self.core = lax.rem(index, 2)
        chip = lax.div(index, 2)
        self.x = lax.rem(chip, self.xs)
        self.z = lax.div(chip, self.xs)

    def at(self, z, x, core, rep=None):
        index = (z * self.xs + x) * 2 + core
        return {"fsdp": index, "rep": self.rep if rep is None else rep}

    def z_peers(self):
        return [(d, lax.rem(self.z + d, self.zs)) for d in range(1, self.zs)]

    def x_peers(self):
        return [(d, lax.rem(self.x + d, self.xs)) for d in range(1, self.xs)]

    def rep_peers(self):
        return [(d, lax.rem(self.rep + d, self.copies)) for d in range(1, self.copies)]

    def z_device(self, z):
        return self.at(z, self.x, self.core)

    def x_device(self, x):
        return self.at(self.z, x, self.core)

    def sibling(self):
        return self.at(self.z, self.x, 1 - self.core)

    def peers(self):
        devices = [self.sibling()]
        for dz in range(self.zs):
            for dx in range(self.xs):
                for dr in range(self.copies):
                    if dz + dx + dr:
                        z, x = lax.rem(self.z + dz, self.zs), lax.rem(self.x + dx, self.xs)
                        rep = lax.rem(self.rep + dr, self.copies)
                        devices.append(self.at(z, x, self.core, rep))
        return devices

    def signal(self):
        for device in self.peers():
            pl.semaphore_signal(
                pltpu.get_barrier_semaphore(), inc=1, device_id=device, device_id_type=MESH
            )

    def wait(self):
        pl.semaphore_wait(pltpu.get_barrier_semaphore(), len(self.peers()))


def remote(src, dst, send, recv, device):
    return pltpu.make_async_remote_copy(
        src_ref=src, dst_ref=dst, send_sem=send, recv_sem=recv,
        device_id=device, device_id_type=MESH,
    )


def take_all(ref, sem):
    pltpu.make_async_copy(ref, ref, sem).wait()


class Gather:
    def __init__(self, grid, parts, like, sems, row):
        self.grid, self.like = grid, like
        g = grid
        send, recv, local = sems
        self.send, self.local = send.at[row], local.at[row]
        self.recv = [recv.at[row, i] for i in range(3)]
        self.keep, self.along_z, self.along_x, self.across = [], [], [], []
        for own, full in parts:
            mine = full.at[g.z, g.x, g.core]
            line, plane = full.at[:, g.x, g.core], full.at[:, :, g.core]
            self.keep.append(pltpu.make_async_copy(own, mine, self.local))
            for _, z in g.z_peers():
                self.along_z.append(remote(own, mine, self.send, self.recv[0], g.z_device(z)))
            for _, x in g.x_peers():
                self.along_x.append(remote(line, line, self.send, self.recv[1], g.x_device(x)))
            self.across.append(remote(plane, plane, self.send, self.recv[2], g.sibling()))

    def start(self, copies):
        for copy in copies:
            copy.start()

    def taken(self, phase, ref):
        take_all(ref, self.recv[phase])
        take_all(ref, self.send)

    def begin(self):
        self.start(self.keep)
        self.start(self.along_z)

    def second(self):
        g = self.grid
        take_all(self.like.at[0, 0, 0], self.local)
        self.taken(0, self.like.at[0 : g.zs - 1, g.x, g.core])
        self.start(self.along_x)

    def third(self):
        g = self.grid
        self.taken(1, self.like.at[:, 0 : g.xs - 1, g.core])
        self.start(self.across)

    def finish(self):
        self.taken(2, self.like.at[:, :, self.grid.core])


class Reduce:
    def __init__(self, grid, part, bufs, out, sems, row, wide):
        self.grid, self.part, self.out, self.wide = grid, part, out, wide
        send, recv = sems
        g = grid
        self.send = send.at[row]
        self.recv = [recv.at[row, i] for i in range(4)]
        self.chip, self.last = bufs[0], bufs[-1]
        self.across = [
            remote(part.at[:, :, 1 - g.core], self.chip, self.send, self.recv[0], g.sibling())
        ]
        self.along_x, self.along_z, self.along_rep = [], [], []
        if wide < 2:
            self.from_x = bufs[1]
            self.line = self.from_x.at[0]
            for d, x in g.x_peers():
                here = self.from_x.at[d - 1]
                device = g.x_device(x)
                self.along_x.append(remote(self.chip.at[:, x], here, self.send, self.recv[1], device))
        if wide:
            for dz, dx, dr in self.steps():
                z, to = lax.rem(g.z + dz, g.zs), lax.rem(g.rep + dr, g.copies)
                x = lax.rem(g.x + dx, g.xs)
                source = self.line.at[z] if wide == 1 else self.chip.at[z, x]
                if dz + dx + dr:
                    here = self.last.at[self.slot(dz, dx, dr)]
                    device = g.at(z, x, g.core, to)
                    self.along_rep.append(remote(source, here, self.send, self.recv[3], device))
            return
        self.from_z = bufs[2]
        self.own = self.from_z.at[0]
        for d, z in g.z_peers():
            self.along_z.append(
                remote(self.line.at[z], self.from_z.at[d - 1], self.send, self.recv[2], g.z_device(z))
            )
        for d, to in g.rep_peers():
            device = g.at(g.z, g.x, g.core, to)
            self.along_rep.append(remote(self.own, self.last.at[d], self.send, self.recv[3], device))

    def steps(self):
        g = self.grid
        zs, xs = (g.zs if self.wide else 1), (g.xs if self.wide == 2 else 1)
        return [(a, b, c) for a in range(zs) for b in range(xs) for c in range(g.copies)]

    def slot(self, dz, dx, dr):
        g = self.grid
        return (dz * (g.xs if self.wide == 2 else 1) + dx) * g.copies + dr

    def start(self, copies):
        for copy in copies:
            copy.start()

    def taken(self, phase, ref):
        take_all(ref, self.recv[phase])
        take_all(ref, self.send)

    def begin(self):
        self.start(self.across)

    def second(self):
        self.taken(0, self.chip)
        mine = self.part[:, :, self.grid.core].astype(F32)
        self.chip[...] = (mine + self.chip[...].astype(F32)).astype(BF)
        if self.wide == 2:
            self.last[0] = self.chip[self.grid.z, self.grid.x]
            self.start(self.along_rep)
        else:
            self.start(self.along_x)

    def third(self):
        g = self.grid
        self.taken(1, self.from_x)
        total = self.chip[:, g.x].astype(F32)
        for d, _ in g.x_peers():
            total = total + self.from_x[d - 1].astype(F32)
        self.line[...] = total.astype(BF)
        if self.wide:
            self.last[0] = self.line[g.z]
            self.start(self.along_rep)
        else:
            self.start(self.along_z)

    def fourth(self):
        g = self.grid
        self.taken(2, self.from_z)
        total = self.line[g.z].astype(F32)
        for d, _ in g.z_peers():
            total = total + self.from_z[d - 1].astype(F32)
        self.own[...] = total.astype(BF)
        self.last[0] = self.own[...]
        self.start(self.along_rep)

    def finish(self):
        g = self.grid
        slots = self.last.shape[0]
        self.taken(3, self.last.at[1:slots])
        total = None
        for z, x, rep in self.steps():
            dz = lax.rem(g.z - z + g.zs, g.zs) if self.wide else 0
            dx = lax.rem(g.x - x + g.xs, g.xs) if self.wide == 2 else 0
            value = self.last[self.slot(dz, dx, lax.rem(g.rep - rep + g.copies, g.copies))]
            total = value.astype(F32) if total is None else total + value.astype(F32)
        held, half, self.leave = self.out
        if half is None:
            held[...] = total[:, 0 : held.shape[1]]
        else:
            for i in range(3):
                held[:, lanes_of(i, half)] = total[:, 128 * i : 128 * i + 128]
        if self.leave is not None:
            self.leave.start()

    def drain(self):
        if self.leave is not None:
            self.leave.wait()


def reduce_bufs(zs, xs, copies, shape, wide):
    dims = [(zs, xs)]
    if wide < 2:
        dims.append((xs - 1, zs))
    if wide == 0:
        dims.append((zs - 1,))
    dims.append((copies * (1, zs, zs * xs)[wide],))
    return [pltpu.VMEM(d + tuple(shape), BF) for d in dims]


SCRATCH = dict(
    x=((3, ROWS, 256), F32),
    after=((2, ROWS, 256), F32),
    n1=((2, ROWS, 256), BF),
    n2=((2, ROWS, 256), BF),
    a=((2, ROWS, 256), BF),
    act=((2, ROWS, 1024), BF),
    slope=((2, ROWS, 1024), BF),
    row=((3, 2, ROWS, 128), BF),
    col=((3, 2, WG, TALL, 128), BF),
    cells=((4, HP, WG, GROUP, 128), F32),
    o_r=((2, HP // STRIPE, 128, WIDE_R), F32),
    o_c=((2, WG, 128, WIDE_C), F32),
    inv_r=((2, HP // STRIPE, 8, WIDE_R), F32),
    inv_c=((2, WG, 8, WIDE_C), F32),
    p_r=((HP // STRIPE, CHUNK, HEADS * WIDE_R), BF),
    p_c=((WG, TALL, HEADS * WIDE_C), BF),
    qs_r=((HEADS * WIDE_R, 256), BF),
    qs_c=((HEADS * WIDE_C, 256), BF),
    dt_r=((128, HEADS * WIDE_R), BF),
    dt_c=((128, HEADS * WIDE_C), BF),
    g_all=((CHUNK, HEADS * WIDE_R), BF),
    g=((ROWS, 256), F32),
    gy=((ROWS, 256), BF),
    g1=((ROWS, 256), BF),
    da_r=((ROWS, 128), BF),
    dqkv_r=((ROWS, 384), BF),
    dqkv_c=((ROWS, 384), BF),
    gv=((128, 256), F32),
    vec=((2, 128, 256), F32),
)


KEPT = ("p_r", "p_c")


class Refs:
    def __init__(self, names, refs):
        self.__dict__.update(zip(names, refs))


QKV, PROJ, FC1, FC2, QKV_R, QKV_C, VEC, SAVE, LOAD_R, LOAD_C = range(10)
MATRICES = (QKV, PROJ, FC1, FC2)
SUMMED = (FC2, FC1, PROJ, QKV_R, QKV_C, VEC)
BEGIN, SECOND, THIRD, FOURTH, FINISH = range(5)
VERBS = ("begin", "second", "third", "fourth", "finish")
P_, H_, V_, F_, G_, BF_, B2_, BS_, BH_, BR_, BV_, BT_, BC_, BM_, BX_, PC_ = range(16)
STRIDE = {P_: 4, F_: 4, BM_: 4, BT_: 4, G_: 4}


def lanes_of(block, half):
    return slice(256 * block + 128 * half, 256 * block + 128 * half + 128)


class Weights:
    def __init__(self, full):
        self.full = full

    def whole(self, name, l):
        value = self.full[name][l]
        return value.reshape(-1, value.shape[-1])

    def qkv_half(self, l, half):
        parts = []
        for i in range(3):
            value = self.full[QKV][l, :, :, :, :, lanes_of(i, half)]
            parts.append(value.reshape(-1, 128))
        return jnp.concatenate(parts, axis=1)

    def qkv(self, l):
        return self.whole(QKV, l)

    def proj(self, l):
        return self.whole(PROJ, l)

    def fc1(self, l):
        return self.whole(FC1, l)

    def fc2(self, l):
        return self.whole(FC2, l)


GATHER_MOVES = {
    (P_, 0, 3): [(QKV_C, 0, SECOND)],
    (H_, 0, 2): [(PROJ, 0, SECOND), (FC1, 0, SECOND), (QKV_C, 0, THIRD)],
    (H_, 0, 3): [(QKV, 1, BEGIN)],
    (PC_, 0, None): [(QKV_C, 0, FINISH)],
    (V_, 0, 0): [(FC2, 0, SECOND), (PROJ, 1, BEGIN)],
    (V_, 0, 3): [(FC1, 1, BEGIN)],
    (V_, 0, 4): [(PROJ, 0, THIRD), (FC1, 0, THIRD), (QKV, 1, SECOND)],
    (F_, 0, None): [(PROJ, 0, FINISH), (FC1, 0, FINISH), (SAVE, 0, BEGIN)],
    (F_, 0, 1): [(FC2, 0, THIRD), (FC2, 1, BEGIN)],
    (G_, 0, None): [(FC2, 0, FINISH)],
    (G_, 0, 1): [(QKV, 1, THIRD)],
    (P_, 1, None): [(QKV, 1, FINISH), (PROJ, 1, SECOND), (FC1, 1, SECOND)],
    (P_, 1, 3): [(SAVE, 0, FINISH)],
    (H_, 1, 1): [(FC2, 1, SECOND)],
    (V_, 1, 1): [(PROJ, 1, THIRD), (FC1, 1, THIRD)],
    (V_, 1, 4): [(FC2, 1, THIRD)],
    (F_, 1, None): [(PROJ, 1, FINISH), (FC1, 1, FINISH)],
    (G_, 1, None): [(FC2, 1, FINISH)],
}
SUM_MOVES = {
    (B2_, 1, None): [(FC2, 1, BEGIN)],
    (BS_, 1, None): [(FC1, 1, BEGIN), (PROJ, 1, BEGIN)],
    (BH_, 1, 0): [(FC2, 1, SECOND)],
    (BH_, 1, 1): [(FC1, 1, SECOND), (PROJ, 1, SECOND)],
    (BR_, 1, None): [(QKV_R, 1, BEGIN), (LOAD_R, 0, BEGIN)],
    (BV_, 1, 0): [(FC2, 1, THIRD)],
    (BV_, 1, 1): [(QKV_R, 1, SECOND)],
    (BV_, 1, 3): [(FC1, 1, THIRD), (PROJ, 1, THIRD)],
    (BV_, 1, 5): [(QKV_R, 1, THIRD)],
    (BC_, 1, None): [(QKV_C, 1, BEGIN), (LOAD_C, 0, BEGIN)],
    (BM_, 1, 1): [(FC2, 1, FOURTH)],
    (BM_, 1, 3): [(QKV_C, 1, SECOND)],
    (BX_, 1, None): [(VEC, 1, BEGIN)],
    (BF_, 0, 1): [(VEC, 1, SECOND)],
    (BF_, 0, 3): [(QKV_C, 1, THIRD), (FC1, 1, FOURTH), (PROJ, 1, FOURTH), (QKV_R, 1, FOURTH)],
    (B2_, 0, None): [(FC2, 0, BEGIN), (FC2, 1, FINISH)],
    (BS_, 0, None): [(FC1, 0, BEGIN), (PROJ, 0, BEGIN), (LOAD_R, 0, FINISH), (VEC, 1, THIRD)],
    (BH_, 0, 0): [(FC2, 0, SECOND)],
    (BH_, 0, 1): [
        (FC1, 0, SECOND), (PROJ, 0, SECOND), (FC1, 1, FINISH), (PROJ, 1, FINISH),
        (QKV_R, 1, FINISH),
    ],
    (BH_, 0, 3): [(QKV_C, 1, FOURTH), (VEC, 1, FOURTH)],
    (BR_, 0, None): [(QKV_R, 0, BEGIN), (LOAD_C, 0, FINISH)],
    (BV_, 0, 0): [(FC2, 0, THIRD)],
    (BV_, 0, 1): [(QKV_R, 0, SECOND)],
    (BV_, 0, 2): [(QKV_C, 1, FINISH), (VEC, 1, FINISH)],
    (BV_, 0, 3): [(FC1, 0, THIRD), (PROJ, 0, THIRD)],
    (BV_, 0, 5): [(QKV_R, 0, THIRD)],
    (BC_, 0, None): [(QKV_C, 0, BEGIN)],
    (BM_, 0, 1): [(FC2, 0, FOURTH), (QKV_C, 0, SECOND)],
    (BX_, 0, None): [(VEC, 0, BEGIN)],
}
LAST_MOVES = [
    (VEC, 0, SECOND), (QKV_C, 0, THIRD), (QKV_R, 0, FOURTH), (FC1, 0, FOURTH), (PROJ, 0, FOURTH),
    (FC2, 0, FINISH), (QKV_R, 0, FINISH), (FC1, 0, FINISH), (PROJ, 0, FINISH),
    (VEC, 0, FINISH), (QKV_C, 0, FINISH),
]
WIDE = {(QKV_C, 0): 1, (VEC, 0): 2}


class Local:
    def __init__(self, *copies):
        self.copies = copies

    def begin(self):
        for copy in self.copies:
            copy.start()

    def finish(self):
        for copy in self.copies:
            copy.wait()


class Moves:
    def __init__(self, table, parts):
        self.table, self.parts = table, parts

    def take(self, moves):
        for move in moves:
            name, l, verb = move
            getattr(self.parts[name, l], VERBS[verb])()

    def __call__(self, phase, l, step=None):
        if step is None:
            self.take(self.table.get((phase, l, None), []))
            return
        start, turn, stride = step
        for (name, block, when), moves in self.table.items():
            if (name, block) != (phase, l) or when is None or when % stride != turn:
                continue
            if start is None:
                self.take(moves)
            else:
                pl.when(start == when // stride)(functools.partial(self.take, moves))


def sweep(phase, l, count, body, at):
    stride = STRIDE.get(phase, 1)
    if stride == count:
        for s in range(count):
            body(s)
            at(phase, l, (None, s, stride))
        return

    def steps(i, carry):
        for turn in range(stride):
            body(i * stride + turn)
            at(phase, l, (i, turn, stride))
        return carry

    lax.fori_loop(0, count // stride, steps, 0)


class Gradients:
    def __init__(self, parts):
        self.parts = parts

    def put(self, name, l, value):
        ref = self.parts[name, l]
        ref[...] = value.astype(BF).reshape(ref.shape)


def plan(shards, copies, layers, width, hidden, held):
    zs, xs = 4, shards // 8
    place = (zs, xs, 2)
    d, f = width // shards, hidden // shards
    shapes = {k: pltpu.VMEM(*v) for k, v in SCRATCH.items()}
    own = {QKV: (d, 3 * width), PROJ: (d, width), FC1: (d, hidden), FC2: (f, width)}
    for name in MATRICES:
        shapes["full", name] = pltpu.VMEM((layers,) + place + own[name], BF)
    shapes["full", VEC] = pltpu.VMEM(place + (layers, d, held), BF)
    gathers = len(MATRICES) * layers + 2
    shapes["gather send"] = pltpu.SemaphoreType.DMA((gathers,))
    shapes["gather recv"] = pltpu.SemaphoreType.DMA((gathers, 3))
    shapes["gather local"] = pltpu.SemaphoreType.DMA((gathers,))
    half = (d, 3 * width // 2)
    own.update({QKV_R: half, QKV_C: half, VEC: (d, 128)})
    sums = len(SUMMED) * layers
    for l in range(layers):
        for name in SUMMED:
            shapes["part", name, l] = pltpu.VMEM(place + own[name], BF)
            for i, buf in enumerate(reduce_bufs(zs, xs, copies, own[name], WIDE.get((name, l), 0))):
                shapes["buf", name, l, i] = buf
    shapes["sum send"] = pltpu.SemaphoreType.DMA((sums,))
    shapes["sum recv"] = pltpu.SemaphoreType.DMA((sums, 4))
    shapes["out"] = pltpu.SemaphoreType.DMA((8 + 6 * layers,))
    for name in MATRICES:
        shapes["sum", name] = pltpu.VMEM((layers,) + own[name], F32)
    shapes["sum", VEC] = pltpu.VMEM((layers, d, held), F32)
    for name in ("tok", "cot"):
        shapes[name] = pltpu.VMEM((HP * WP, width), BF)
    return shapes


def step_kernel(shards, copies, names, *refs):
    h_ref, w_ref, tok, cot = refs[:4]
    own = dict(zip(MATRICES, refs[4:8]))
    vec_own = refs[8]
    y_ref, gt_ref = refs[9:11]
    outs = dict(zip(MATRICES + (VEC,), refs[11:16]))
    p_r_ref, p_c_ref = refs[16:18]
    s = dict(zip(names, refs[18:]))
    r = Refs(SCRATCH, [s[k] for k in SCRATCH])
    layers = own[QKV].shape[0]
    grid = Grid(shards, copies)
    grid.signal()
    h, w = h_ref[0], w_ref[0]

    sems = [s["gather send"], s["gather recv"], s["gather local"]]
    order = [(name, l) for l in range(layers) for name in MATRICES][1:]
    gathers = {}
    for i, (name, l) in enumerate(order):
        full = s["full", name].at[l]
        gathers[name, l] = Gather(grid, [(own[name].at[l], full)], full, sems, i)
    full = s["full", VEC]
    gathers[VEC, 0] = Gather(grid, [(vec_own, full)], full, sems, len(order))
    full = s["full", QKV].at[0]
    for half, name in enumerate((QKV_R, QKV_C)):
        parts = []
        for i in range(3):
            lanes = lanes_of(i, half)
            parts.append((own[QKV].at[0, :, lanes], full.at[:, :, :, :, lanes]))
        like = full.at[:, :, :, :, 0 : full.shape[-1] // 2]
        gathers[name, 0] = Gather(grid, parts, like, sems, len(order) + 1 + half)
    wt = Weights({name: s["full", name] for name in MATRICES})

    def local(src, dst, i):
        return pltpu.make_async_copy(src, dst, s["out"].at[i])

    tok_copy, cot_copy = local(tok, s["tok"], 6), local(cot, s["cot"], 7)
    tok_copy.start()
    cot_copy.start()
    grid.wait()
    first = [gathers[QKV_R, 0], gathers[VEC, 0]]
    for one in first:
        one.begin()
    for stack in (r.qs_r, r.qs_c):
        stack[...] = jnp.where(iota(stack.shape, 1) == 128, 1.0, 0.0).astype(BF)
    for stack in (r.dt_r, r.dt_c):
        stack[...] = jnp.zeros_like(stack)
    r.gv[...] = jnp.zeros_like(r.gv)
    tok_copy.wait()
    pad_groups(s["tok"], r.x.at[0])
    for i in range(HP // STRIPE):
        rows = slice(i * CHUNK, (i + 1) * CHUNK)
        r.after[0, rows, :] = norm_parts(r.x[0, rows, :])[0]
    cot_copy.wait()
    pad_groups(s["cot"], r.g)
    for one in first:
        one.second()
    gathers[QKV_C, 0].begin()
    for one in first:
        one.third()
    gathers[PROJ, 0].begin()
    gathers[FC1, 0].begin()
    for one in first:
        one.finish()
    gathers[FC2, 0].begin()
    for l in range(layers):
        value = s["full", VEC][:, :, :, l].astype(F32)
        value = value.reshape(-1, value.shape[-1])
        value = jnp.concatenate([value, jnp.zeros((value.shape[0], 128 - value.shape[1]), F32)], axis=1)
        r.vec[l] = value.T

    save = Local(local(r.p_r, p_r_ref, 2), local(r.p_c, p_c_ref, 3))
    at = Moves(GATHER_MOVES, {**gathers, (SAVE, 0): save})
    for l in range(layers):
        forward_layer(l, h, w, wt, r, at)

    sums = {}
    for l in range(layers):
        for i, name in enumerate(SUMMED):
            whole = QKV if name in (QKV_R, QKV_C) else name
            held = s["sum", whole].at[l]
            half = {QKV_R: 0, QKV_C: 1}.get(name)
            leave = None if half == 0 else local(held, outs[whole].at[l], 8 + l * 6 + i)
            out = (held, half, leave)
            wide = WIDE.get((name, l), 0)
            bufs = [s["buf", name, l, j] for j in range(4 - wide)]
            row = l * len(SUMMED) + i
            sums[name, l] = Reduce(
                grid, s["part", name, l], bufs, out, [s["sum send"], s["sum recv"]], row, wide
            )
    gradients = Gradients({(name, l): s["part", name, l] for l in range(layers) for name in SUMMED})

    load_r = Local(local(p_r_ref, r.p_r, 4))
    load_c = Local(local(p_c_ref, r.p_c, 5))
    at = Moves(SUM_MOVES, {**sums, (LOAD_R, 0): load_r, (LOAD_C, 0): load_c})
    for l in reversed(range(layers)):
        backward_layer(l, h, w, wt, r, gradients, at)
    flat = pl.ds(0, HP * WP)
    drop_groups(r.g, r.g)
    g_copy = local(r.g.at[flat], gt_ref, 1)
    g_copy.start()
    at.take(LAST_MOVES[:1])
    drop_groups(r.x.at[layers], r.x.at[layers])
    y_copy = local(r.x.at[layers, flat], y_ref, 0)
    y_copy.start()
    at.take(LAST_MOVES[1:])
    for one in sums.values():
        one.drain()
    y_copy.wait()
    g_copy.wait()


PIECES = 7


def finish_kernel(count, *refs):
    src, dst, held = refs[:count], refs[count : 2 * count], refs[2 * count : 3 * count]
    sems = refs[3 * count]
    moves = []
    for i in range(count):
        pieces = PIECES if i < 2 else 1
        size = src[i].shape[0] // pieces
        for j in range(pieces):
            part, sem = pl.ds(j * size, size), sems.at[len(moves)]
            first = pltpu.make_async_copy(src[i].at[part], held[i].at[part], sem)
            moves.append((first, pltpu.make_async_copy(held[i].at[part], dst[i].at[part], sem)))
    for first, _ in moves:
        first.start()
    for first, last in moves:
        first.wait()
        last.start()
    for _, last in moves:
        last.wait()


def shards_step(shards, copies, tokens, heights, widths, w_qkv, w_proj, w_fc1, w_fc2, vectors, cotangent):
    layers, _, hidden = w_fc1.shape
    count, width = tokens.shape
    vmem = pl.BlockSpec(memory_space=pltpu.VMEM)
    smem = pl.BlockSpec(memory_space=pltpu.SMEM)
    hbm = pl.BlockSpec(memory_space=pl.ANY)
    turned = vectors.transpose(0, 2, 1)
    scratch = plan(shards, copies, layers, width, hidden, turned.shape[2])
    matrices = [w_qkv, w_proj, w_fc1, w_fc2]
    results = [jax.ShapeDtypeStruct((count, width), F32)] * 2
    results += [jax.ShapeDtypeStruct(m.shape, F32) for m in matrices]
    results += [jax.ShapeDtypeStruct(turned.shape, F32)]
    results += [jax.ShapeDtypeStruct(*SCRATCH[k]) for k in KEPT]
    *raw, _, _ = pl.pallas_call(
        functools.partial(step_kernel, shards, copies, list(scratch)),
        out_shape=results,
        in_specs=[smem, smem, hbm, hbm] + [hbm] * 5,
        out_specs=[hbm] * 9,
        scratch_shapes=list(scratch.values()),
        compiler_params=pltpu.CompilerParams(
            collective_id=0,
            has_side_effects=True,
            vmem_limit_bytes=67043328,
        ),
    )(heights, widths, tokens, cotangent, *matrices, turned)
    final = [jax.ShapeDtypeStruct((count, width), F32)] * 2
    final += [jax.ShapeDtypeStruct(m.shape, F32) for m in matrices + [turned]]
    sems = pltpu.SemaphoreType.DMA((2 * PIECES + len(raw) - 2,))
    *arrays, vec = pl.pallas_call(
        functools.partial(finish_kernel, len(raw)),
        out_shape=final,
        in_specs=[hbm] * len(raw),
        out_specs=[hbm] * len(raw),
        scratch_shapes=[pltpu.VMEM(f.shape, F32) for f in final] + [sems],
        compiler_params=pltpu.CompilerParams(vmem_limit_bytes=67043328),
    )(*raw)
    return (*arrays, vec.transpose(0, 2, 1))


def solution(mesh):
    images = P(("fsdp", "rep"), None)
    weights = P(None, "fsdp", None)
    return jax.shard_map(
        functools.partial(shards_step, mesh.shape["fsdp"], mesh.shape["rep"]),
        mesh=mesh,
        in_specs=(images, P(("fsdp", "rep")), P(("fsdp", "rep")), weights, weights, weights, weights, P(None, None, "fsdp"), images),
        out_specs=(images, images, weights, weights, weights, weights, P(None, None, "fsdp")),
        check_vma=False,
    )
```

```python
import functools
import jax
import jax.numpy as jnp
from jax import lax
from jax.experimental import pallas as pl
from jax.experimental.pallas import tpu as pltpu
from jax.sharding import PartitionSpec as P

HEAD = 32
STRIPE = 7
HP = 28
WP = 42
HEADS = 4
GROUP = 8
WG = WP // STRIPE
ROWS = HP * WG * GROUP
CHUNK = STRIPE * WG * GROUP
TALL = HP * GROUP
WIDE_R = 384
WIDE_C = 256
BF = jnp.bfloat16
F32 = jnp.float32
eps_norm = 1e-05
masked_score = -1000000000.0
LOG2E = 1.4426950408889634
LN2 = 0.6931471805599453
SCALE = HEAD ** (-0.5)
NN = (((1,), (0,)), ((), ()))
NT = (((1,), (1,)), ((), ()))
TN = (((0,), (0,)), ((), ()))


def mm(a, b, dims=NN):
    return lax.dot_general(a, b, dims, preferred_element_type=F32)


def iota(shape, dim):
    return lax.broadcasted_iota(jnp.int32, shape, dim)


def span(index, size):
    return pl.ds(pl.multiple_of(index * size, size), size)


def map_rows(stripe):
    return pl.ds(stripe * STRIPE, STRIPE)


def pad_groups(src, dst, scale=None):
    def body(j, carry):
        block = src[pl.ds(pl.multiple_of(j * 56, 8), 56), :].astype(F32).reshape(7, 8, -1)
        place = iota((8, block.shape[-1]), 0)
        for u in range(8):
            if u == 0:
                group = block[0]
            elif u == 7:
                group = pltpu.roll(block[6], 7, 0)
            else:
                group = jnp.where(
                    place < u, pltpu.roll(block[u - 1], u, 0), pltpu.roll(block[u], u, 0)
                )
            group = jnp.where(place < 7, group, 0.0)
            dst[pl.ds(pl.multiple_of(j * 64 + u * 8, 8), 8), :] = group
        return carry

    lax.fori_loop(0, ROWS // 64, body, 0)


def drop_groups(src, dst):
    def body(j, carry):
        block = src[pl.ds(pl.multiple_of(j * 64, 8), 64), :].reshape(8, 8, -1)
        place = iota((8, block.shape[-1]), 0)
        for t in range(7):
            lower = block[t] if t == 0 else pltpu.roll(block[t], 8 - t, 0)
            upper = pltpu.roll(block[t + 1], 7 - t, 0)
            dst[pl.ds(pl.multiple_of(j * 56 + t * 8, 8), 8), :] = jnp.where(
                place <= 6 - t, lower, upper
            )
        return carry

    lax.fori_loop(0, ROWS // 64, body, 0)


def norm_parts(x):
    centre = jnp.mean(x, axis=-1, keepdims=True)
    centred = x - centre
    rate = lax.rsqrt(jnp.mean(centred * centred, axis=-1, keepdims=True) + eps_norm)
    return centred * rate, rate


def norm_back(d_n, xhat, rate, gain):
    e = d_n * gain
    return rate * (
        e
        - jnp.mean(e, axis=-1, keepdims=True)
        - xhat * jnp.mean(e * xhat, axis=-1, keepdims=True)
    )


def colsum(x):
    return jnp.sum(x, axis=0, keepdims=True)


def rows_live(stripe, h, w, lanes):
    shape = (STRIPE, WG * GROUP, lanes)
    row = iota(shape, 0) + stripe * STRIPE
    place = iota(shape, 1)
    within = place & 7
    col = (place >> 3) * STRIPE + within
    live = (row < h) & (col < w) & (within < STRIPE)
    return jnp.where(live, 1.0, 0.0).reshape(CHUNK, lanes)


def cols_live(stripe, h, w, lanes):
    shape = (HP, GROUP, lanes)
    row = iota(shape, 0)
    within = iota(shape, 1)
    live = (row < h) & (within + stripe * STRIPE < w) & (within < STRIPE)
    return jnp.where(live, 1.0, 0.0).reshape(TALL, lanes)


def with_mask(keys, live):
    lane = iota(live.shape, 1)
    extra = jnp.where(lane == 0, jnp.where(live > 0.0, 0.0, masked_score), 0.0)
    return jnp.concatenate([keys, extra.astype(BF)], axis=-1)


def stack_heads(ref, x, wide):
    length = x.shape[0]
    lane = iota(x.shape, 1)
    for h in range(HEADS):
        kept = jnp.where((lane >> 5) == h, x, jnp.zeros_like(x))
        ref[h * wide : h * wide + length, 0:128] = kept


def widen(x, wide):
    length = x.shape[0]
    return jnp.concatenate([x, jnp.zeros((wide - length, x.shape[1]), x.dtype)], axis=0)


def attend(q, k_mask, vm, qs, out_t, inv, probs, stripe, wide):
    length = q.shape[0]
    stack_heads(qs, q, wide)
    scores = mm(k_mask, qs[0 : HEADS * wide, :], NT)
    v_t = widen(vm.astype(F32), wide).T.astype(BF)[:, 0:length]
    for h in range(HEADS):
        s = scores[:, h * wide : (h + 1) * wide]
        top = jnp.max(s, axis=0, keepdims=True)
        p = jnp.exp2(s - top)
        total = jnp.sum(p, axis=0, keepdims=True)
        p_low = p.astype(BF)
        probs[stripe, :, h * wide : (h + 1) * wide] = p_low
        rate = 1.0 / total
        inv[stripe, h : h + 1, :] = rate
        o = mm(v_t[HEAD * h : HEAD * (h + 1), :], p_low)
        out_t[stripe, HEAD * h : HEAD * (h + 1), :] = o * rate


def attend_back(q, k, vm, da, qs, da_stack, g_all, out_t, inv, probs, stripe, wide):
    length = q.shape[0]
    stack_heads(qs, q, wide)
    da_t = widen(da.astype(F32), wide).T
    k_t = widen(k.astype(F32), wide).T.astype(BF)[:, 0:length]
    inner = []
    for h in range(HEADS):
        rows = slice(HEAD * h, HEAD * (h + 1))
        scaled = (da_t[rows, :] * inv[stripe, h : h + 1, :]).astype(BF)
        da_stack[rows, h * wide : (h + 1) * wide] = scaled
        inner.append(colsum(scaled.astype(F32) * out_t[stripe, rows, :]))
    d_probs = mm(vm, da_stack[...])
    dq_t = []
    for h in range(HEADS):
        lanes = slice(h * wide, (h + 1) * wide)
        p = probs[stripe, :, lanes].astype(F32)
        g = (p * (d_probs[:, lanes] - inner[h])).astype(BF)
        g_all[0:length, lanes] = g
        dq_t.append(mm(k_t[HEAD * h : HEAD * (h + 1), :], g))
    dv = mm(probs[stripe], da_stack[...], NT)
    dk = mm(g_all[0:length, 0 : HEADS * wide], qs[0 : HEADS * wide, 0:128]) * LN2
    dq = jnp.concatenate(dq_t, axis=0).T[0:length, :] * SCALE
    return dq, dk, dv


def earlier(x):
    return jnp.concatenate([jnp.zeros_like(x[:1]), x[:-1]], axis=0)


def later(x):
    return jnp.concatenate([x[1:], jnp.zeros_like(x[:1])], axis=0)


def row_neighbours(x):
    groups = x.reshape(STRIPE * WG, GROUP, 128)
    place = iota(groups.shape, 1)
    edge = jnp.zeros((STRIPE, 1, GROUP, 128), x.dtype)
    far = pltpu.roll(groups, 2, 1).reshape(STRIPE, WG, GROUP, 128)
    far = jnp.concatenate([edge, far[:, :-1]], axis=1).reshape(groups.shape)
    left = jnp.where(place == 0, far, pltpu.roll(groups, 1, 1))
    far = pltpu.roll(groups, 6, 1).reshape(STRIPE, WG, GROUP, 128)
    far = jnp.concatenate([far[:, 1:], edge], axis=1).reshape(groups.shape)
    right = jnp.where(place == 6, far, pltpu.roll(groups, 7, 1))
    shape = (STRIPE, WG * GROUP, 128)
    return left.reshape(shape), x.reshape(shape), right.reshape(shape)


def col_neighbours(x):
    cells = x.reshape(HP, GROUP, 128)
    return pltpu.roll(cells, 1, 1), cells, pltpu.roll(cells, 7, 1)


def position(near, taps):
    rows = [sum(taps[3 * a + b] * near[b] for b in range(3)) for a in range(3)]
    return earlier(rows[0]) + rows[1] + later(rows[2])


def position_back(near, taps):
    rows = [sum(taps[3 * a + b] * near[2 - b] for b in range(3)) for a in range(3)]
    return later(rows[0]) + rows[1] + earlier(rows[2])


def tap_sums(da, near):
    sums = []
    for a in range(3):
        for b in range(3):
            x = near[b]
            x = earlier(x) if a == 0 else later(x) if a == 2 else x
            sums.append(colsum((da * x).reshape(-1, 128)))
    return sums


def forward_layer(l, h, w, wt, r, at):
    at(P_, l)
    vec = r.vec[l]

    def keep_row(rows, parts):
        for i, part in enumerate(parts):
            r.row[i, l, rows, :] = part.astype(BF)

    def keep_col(s, parts):
        for i, part in enumerate(parts):
            r.cells[i, map_rows(s)] = part.reshape(STRIPE, WG, GROUP, 128)

    def split(mixed, s, half, lanes):
        here = slice(128 * half, 128 * half + 128)
        q = (mixed[:, lanes[0]] + vec[2:3, here]) * (SCALE * LOG2E)
        v = (mixed[:, lanes[2]] + vec[3:4, here]) * rows_live(s, h, w, 128)
        return q, mixed[:, lanes[1]], v

    def norm(s):
        rows = span(s, CHUNK)
        xhat = norm_parts(r.x[l, rows, :])[0] if l else r.after[0, rows, :]
        n1 = (xhat * vec[0:1] + vec[1:2]).astype(BF)
        r.n1[l, rows, :] = n1
        return rows, n1

    alone = [slice(128 * i, 128 * i + 128) for i in range(3)]

    def project(s):
        rows, n1 = norm(s)
        mixed = mm(n1, wt.qkv(l))
        for half in range(2):
            lanes = [slice(256 * i + 128 * half, 256 * i + 128 * half + 128) for i in range(3)]
            parts = split(mixed, s, half, lanes)
            keep_col(s, parts) if half else keep_row(rows, parts)

    def project_row(s):
        rows, n1 = norm(s)
        keep_row(rows, split(mm(n1, wt.qkv_half(l, 0)), s, 0, alone))

    def project_col(s):
        n1 = r.n1[l, span(s, CHUNK), :]
        keep_col(s, split(mm(n1, wt.qkv_half(l, 1)), s, 1, alone))

    sweep(P_, l, HP // STRIPE, project if l else project_row, at)

    at(H_, l)

    def horizontal(s):
        rows = span(s, CHUNK)
        q, k, v = (r.row[i, l, rows, :] for i in range(3))
        attend(q, with_mask(k, rows_live(s, h, w, 128)), v, r.qs_r, r.o_r.at[l], r.inv_r.at[l], r.p_r, s, WIDE_R)
        near = row_neighbours(v.astype(F32))
        taps = vec[9:18, 0:128]
        pos = position(near, [taps[i : i + 1] for i in range(9)]) + vec[8:9, 0:128]
        o = r.o_r[l, s].T[0:CHUNK, :]
        r.a[l, rows, 0:128] = (o + pos.reshape(CHUNK, 128)).astype(BF)

    sweep(H_, l, HP // STRIPE, horizontal, at)
    at(PC_, l)
    if l == 0:
        sweep(PC_, l, HP // STRIPE, project_col, at)

    def vertical(s):
        q, k, v = (r.cells[i, :, s].reshape(TALL, 128).astype(BF) for i in range(3))
        for i, part in enumerate((q, k, v)):
            r.col[i, l, s] = part
        attend(q, with_mask(k, cols_live(s, h, w, 128)), v, r.qs_c, r.o_c.at[l], r.inv_c.at[l], r.p_c, s, WIDE_C)
        near = col_neighbours(v.astype(F32))
        taps = vec[9:18, 128:256]
        pos = position(near, [taps[i : i + 1] for i in range(9)]) + vec[8:9, 128:256]
        o = r.o_c[l, s].T[0:TALL, :]
        r.cells[3, :, s] = o.reshape(HP, GROUP, 128) + pos

    sweep(V_, l, WG, vertical, at)

    at(F_, l)

    def feed(s):
        rows = span(s, CHUNK)
        turned = r.cells[3, map_rows(s)].reshape(CHUNK, 128).astype(BF)
        r.a[l, rows, 128:256] = turned
        x1 = r.x[l, rows, :] + mm(r.a[l, rows, :], wt.proj(l)) + vec[4:5]
        r.after[l, rows, :] = x1
        xhat, rate = norm_parts(x1)
        n2 = (xhat * vec[5:6] + vec[6:7]).astype(BF)
        r.n2[l, rows, :] = n2
        for j in range(4):
            lanes = slice(256 * j, 256 * j + 256)
            hid = mm(n2, wt.fc1(l)[:, lanes]) + vec[18 + j : 19 + j]
            phi = 0.5 * lax.erf(hid * 0.7071067811865476) + 0.5
            bell = jnp.exp2(hid * hid * (-0.5 * LOG2E)) * 0.3989422804014327
            r.act[l, rows, lanes] = (hid * phi).astype(BF)
            r.slope[l, rows, lanes] = (phi + hid * bell).astype(BF)

    sweep(F_, l, HP // STRIPE, feed, at)
    at(G_, l)

    def close(s):
        rows = span(s, CHUNK)
        x1 = r.after[l, rows, :]
        r.x[l + 1, rows, :] = x1 + mm(r.act[l, rows, :], wt.fc2(l)) + vec[7:8]

    sweep(G_, l, HP // STRIPE, close, at)


def backward_layer(l, h, w, wt, r, out, at):
    vec = r.vec[l]
    r.gv[...] = jnp.zeros_like(r.gv)

    def add(row, value):
        r.gv[row : row + 1, :] += value

    def feed(s):
        rows = span(s, CHUNK)
        g = r.g[rows, :]
        add(7, colsum(g))
        gy = g.astype(BF)
        r.gy[rows, :] = gy
        for j in range(4):
            lanes = slice(256 * j, 256 * j + 256)
            d_hid = mm(gy, wt.fc2(l)[lanes], NT) * r.slope[l, rows, lanes].astype(F32)
            add(18 + j, colsum(d_hid))
            r.slope[l, rows, lanes] = d_hid.astype(BF)
        dh = r.slope[l, rows, :]
        d_n2 = mm(dh, wt.fc1(l), NT)
        xhat, rate = norm_parts(r.after[l, rows, :])
        add(5, colsum(d_n2 * xhat))
        add(6, colsum(d_n2))
        g1 = g + norm_back(d_n2, xhat, rate, vec[5:6])
        r.g[rows, :] = g1
        add(4, colsum(g1))
        g1_low = g1.astype(BF)
        r.g1[rows, :] = g1_low
        da = mm(g1_low, wt.proj(l), NT)
        r.da_r[rows, :] = da[:, 0:128].astype(BF)
        add(8, colsum(da.astype(BF).astype(F32)))
        r.cells[3, map_rows(s)] = da[:, 128:256].reshape(STRIPE, WG, GROUP, 128)

    sweep(BF_, l, HP // STRIPE, feed, at)
    out.put(FC2, l, mm(r.gy[...], r.act[l], TN).astype(BF).T)
    at(B2_, l)
    out.put(FC1, l, mm(r.n2[l], r.slope[l], TN))
    out.put(PROJ, l, mm(r.a[l], r.g1[...], TN))
    at(BS_, l)

    def horizontal(s):
        rows = span(s, CHUNK)
        q, k, v = (r.row[i, l, rows, :] for i in range(3))
        da = r.da_r[rows, :]
        live = rows_live(s, h, w, 128)
        dq, dk, dv = attend_back(
            q, k, v, da, r.qs_r, r.dt_r, r.g_all, r.o_r.at[l], r.inv_r.at[l], r.p_r, s, WIDE_R
        )
        taps = [vec[9 + i : 10 + i, 0:128] for i in range(9)]
        da_near = row_neighbours(da.astype(F32))
        dv = (dv + position_back(da_near, taps).reshape(CHUNK, 128)) * live
        sums = tap_sums(da_near[1], row_neighbours(v.astype(F32)))
        for i in range(9):
            r.gv[9 + i : 10 + i, 0:128] += sums[i]
        r.gv[2:3, 0:128] += colsum(dq)
        r.gv[3:4, 0:128] += colsum(dv)
        for i, part in enumerate((dq, dk, dv)):
            r.dqkv_r[rows, 128 * i : 128 * i + 128] = part.astype(BF)

    sweep(BH_, l, HP // STRIPE, horizontal, at)
    out.put(QKV_R, l, mm(r.n1[l], r.dqkv_r[...], TN))
    at(BR_, l)

    def vertical(s):
        q, k, v = (r.col[i, l, s] for i in range(3))
        da = r.cells[3, :, s].reshape(TALL, 128).astype(BF)
        live = cols_live(s, h, w, 128)
        dq, dk, dv = attend_back(
            q, k, v, da, r.qs_c, r.dt_c, r.g_all, r.o_c.at[l], r.inv_c.at[l], r.p_c, s, WIDE_C
        )
        taps = [vec[9 + i : 10 + i, 128:256] for i in range(9)]
        da_near = col_neighbours(da.astype(F32))
        dv = (dv + position_back(da_near, taps).reshape(TALL, 128)) * live
        sums = tap_sums(da_near[1], col_neighbours(v.astype(F32)))
        for i in range(9):
            r.gv[9 + i : 10 + i, 128:256] += sums[i]
        r.gv[2:3, 128:256] += colsum(dq)
        r.gv[3:4, 128:256] += colsum(dv)
        for i, part in enumerate((dq, dk, dv)):
            r.cells[i, :, s] = part.reshape(HP, GROUP, 128)

    sweep(BV_, l, WG, vertical, at)

    def turn(s):
        rows = span(s, CHUNK)
        for i in range(3):
            cells = r.cells[i, map_rows(s)].reshape(CHUNK, 128)
            r.dqkv_c[rows, 128 * i : 128 * i + 128] = cells.astype(BF)

    sweep(BT_, l, HP // STRIPE, turn, at)
    out.put(QKV_C, l, mm(r.n1[l], r.dqkv_c[...], TN))
    at(BC_, l)

    def mix(s):
        rows = span(s, CHUNK)
        parts = []
        for i in range(3):
            lanes = slice(128 * i, 128 * i + 128)
            parts += [r.dqkv_r[rows, lanes], r.dqkv_c[rows, lanes]]
        d_n1 = mm(jnp.concatenate(parts, axis=1), wt.qkv(l), NT)
        xhat, rate = norm_parts(r.x[l, rows, :])
        add(0, colsum(d_n1 * xhat))
        add(1, colsum(d_n1))
        r.g[rows, :] += norm_back(d_n1, xhat, rate, vec[0:1])

    sweep(BM_, l, HP // STRIPE, mix, at)
    out.put(VEC, l, r.gv[...].T)
    at(BX_, l)


MESH = pl.DeviceIdType.MESH


class Grid:
    def __init__(self, shards, copies):
        self.cores = 2
        self.zs = 4
        self.xs = shards // 8
        self.copies = copies
        index = lax.axis_index("fsdp")
        self.rep = lax.axis_index("rep")
        self.core = lax.rem(index, 2)
        chip = lax.div(index, 2)
        self.x = lax.rem(chip, self.xs)
        self.z = lax.div(chip, self.xs)

    def at(self, z, x, core, rep=None):
        index = (z * self.xs + x) * 2 + core
        return {"fsdp": index, "rep": self.rep if rep is None else rep}

    def z_peers(self):
        return [(d, lax.rem(self.z + d, self.zs)) for d in range(1, self.zs)]

    def x_peers(self):
        return [(d, lax.rem(self.x + d, self.xs)) for d in range(1, self.xs)]

    def rep_peers(self):
        return [(d, lax.rem(self.rep + d, self.copies)) for d in range(1, self.copies)]

    def z_device(self, z):
        return self.at(z, self.x, self.core)

    def x_device(self, x):
        return self.at(self.z, x, self.core)

    def sibling(self):
        return self.at(self.z, self.x, 1 - self.core)

    def peers(self):
        devices = [self.sibling()]
        for dz in range(self.zs):
            for dx in range(self.xs):
                for dr in range(self.copies):
                    if dz + dx + dr:
                        z, x = lax.rem(self.z + dz, self.zs), lax.rem(self.x + dx, self.xs)
                        rep = lax.rem(self.rep + dr, self.copies)
                        devices.append(self.at(z, x, self.core, rep))
        return devices

    def signal(self):
        for device in self.peers():
            pl.semaphore_signal(
                pltpu.get_barrier_semaphore(), inc=1, device_id=device, device_id_type=MESH
            )

    def wait(self):
        pl.semaphore_wait(pltpu.get_barrier_semaphore(), len(self.peers()))


def remote(src, dst, send, recv, device):
    return pltpu.make_async_remote_copy(
        src_ref=src, dst_ref=dst, send_sem=send, recv_sem=recv,
        device_id=device, device_id_type=MESH,
    )


def take_all(ref, sem):
    pltpu.make_async_copy(ref, ref, sem).wait()


class Gather:
    def __init__(self, grid, parts, like, sems, row):
        self.grid, self.like = grid, like
        g = grid
        send, recv, local = sems
        self.send, self.local = send.at[row], local.at[row]
        self.recv = [recv.at[row, i] for i in range(3)]
        self.keep, self.along_z, self.along_x, self.across = [], [], [], []
        for own, full in parts:
            mine = full.at[g.z, g.x, g.core]
            line, plane = full.at[:, g.x, g.core], full.at[:, :, g.core]
            self.keep.append(pltpu.make_async_copy(own, mine, self.local))
            for _, z in g.z_peers():
                self.along_z.append(remote(own, mine, self.send, self.recv[0], g.z_device(z)))
            for _, x in g.x_peers():
                self.along_x.append(remote(line, line, self.send, self.recv[1], g.x_device(x)))
            self.across.append(remote(plane, plane, self.send, self.recv[2], g.sibling()))

    def start(self, copies):
        for copy in copies:
            copy.start()

    def taken(self, phase, ref):
        take_all(ref, self.recv[phase])
        take_all(ref, self.send)

    def begin(self):
        self.start(self.keep)
        self.start(self.along_z)

    def second(self):
        g = self.grid
        take_all(self.like.at[0, 0, 0], self.local)
        self.taken(0, self.like.at[0 : g.zs - 1, g.x, g.core])
        self.start(self.along_x)

    def third(self):
        g = self.grid
        self.taken(1, self.like.at[:, 0 : g.xs - 1, g.core])
        self.start(self.across)

    def finish(self):
        self.taken(2, self.like.at[:, :, self.grid.core])


class Reduce:
    def __init__(self, grid, part, bufs, out, sems, row, wide):
        self.grid, self.part, self.out, self.wide = grid, part, out, wide
        send, recv = sems
        g = grid
        self.send = send.at[row]
        self.recv = [recv.at[row, i] for i in range(4)]
        self.chip, self.last = bufs[0], bufs[-1]
        self.across = [
            remote(part.at[:, :, 1 - g.core], self.chip, self.send, self.recv[0], g.sibling())
        ]
        self.along_x, self.along_z, self.along_rep = [], [], []
        if wide < 2:
            self.from_x = bufs[1]
            self.line = self.from_x.at[0]
            for d, x in g.x_peers():
                here = self.from_x.at[d - 1]
                device = g.x_device(x)
                self.along_x.append(remote(self.chip.at[:, x], here, self.send, self.recv[1], device))
        if wide:
            for dz, dx, dr in self.steps():
                z, to = lax.rem(g.z + dz, g.zs), lax.rem(g.rep + dr, g.copies)
                x = lax.rem(g.x + dx, g.xs)
                source = self.line.at[z] if wide == 1 else self.chip.at[z, x]
                if dz + dx + dr:
                    here = self.last.at[self.slot(dz, dx, dr)]
                    device = g.at(z, x, g.core, to)
                    self.along_rep.append(remote(source, here, self.send, self.recv[3], device))
            return
        self.from_z = bufs[2]
        self.own = self.from_z.at[0]
        for d, z in g.z_peers():
            self.along_z.append(
                remote(self.line.at[z], self.from_z.at[d - 1], self.send, self.recv[2], g.z_device(z))
            )
        for d, to in g.rep_peers():
            device = g.at(g.z, g.x, g.core, to)
            self.along_rep.append(remote(self.own, self.last.at[d], self.send, self.recv[3], device))

    def steps(self):
        g = self.grid
        zs, xs = (g.zs if self.wide else 1), (g.xs if self.wide == 2 else 1)
        return [(a, b, c) for a in range(zs) for b in range(xs) for c in range(g.copies)]

    def slot(self, dz, dx, dr):
        g = self.grid
        return (dz * (g.xs if self.wide == 2 else 1) + dx) * g.copies + dr

    def start(self, copies):
        for copy in copies:
            copy.start()

    def taken(self, phase, ref):
        take_all(ref, self.recv[phase])
        take_all(ref, self.send)

    def begin(self):
        self.start(self.across)

    def second(self):
        self.taken(0, self.chip)
        mine = self.part[:, :, self.grid.core].astype(F32)
        self.chip[...] = (mine + self.chip[...].astype(F32)).astype(BF)
        if self.wide == 2:
            self.last[0] = self.chip[self.grid.z, self.grid.x]
            self.start(self.along_rep)
        else:
            self.start(self.along_x)

    def third(self):
        g = self.grid
        self.taken(1, self.from_x)
        total = self.chip[:, g.x].astype(F32)
        for d, _ in g.x_peers():
            total = total + self.from_x[d - 1].astype(F32)
        self.line[...] = total.astype(BF)
        if self.wide:
            self.last[0] = self.line[g.z]
            self.start(self.along_rep)
        else:
            self.start(self.along_z)

    def fourth(self):
        g = self.grid
        self.taken(2, self.from_z)
        total = self.line[g.z].astype(F32)
        for d, _ in g.z_peers():
            total = total + self.from_z[d - 1].astype(F32)
        self.own[...] = total.astype(BF)
        self.last[0] = self.own[...]
        self.start(self.along_rep)

    def finish(self):
        g = self.grid
        slots = self.last.shape[0]
        self.taken(3, self.last.at[1:slots])
        total = None
        for z, x, rep in self.steps():
            dz = lax.rem(g.z - z + g.zs, g.zs) if self.wide else 0
            dx = lax.rem(g.x - x + g.xs, g.xs) if self.wide == 2 else 0
            value = self.last[self.slot(dz, dx, lax.rem(g.rep - rep + g.copies, g.copies))]
            total = value.astype(F32) if total is None else total + value.astype(F32)
        held, half, self.leave = self.out
        if half is None:
            held[...] = total[:, 0 : held.shape[1]]
        else:
            for i in range(3):
                held[:, lanes_of(i, half)] = total[:, 128 * i : 128 * i + 128]
        if self.leave is not None:
            self.leave.start()

    def drain(self):
        if self.leave is not None:
            self.leave.wait()


def reduce_bufs(zs, xs, copies, shape, wide):
    dims = [(zs, xs)]
    if wide < 2:
        dims.append((xs - 1, zs))
    if wide == 0:
        dims.append((zs - 1,))
    dims.append((copies * (1, zs, zs * xs)[wide],))
    return [pltpu.VMEM(d + tuple(shape), BF) for d in dims]


SCRATCH = dict(
    x=((3, ROWS, 256), F32),
    after=((2, ROWS, 256), F32),
    n1=((2, ROWS, 256), BF),
    n2=((2, ROWS, 256), BF),
    a=((2, ROWS, 256), BF),
    act=((2, ROWS, 1024), BF),
    slope=((2, ROWS, 1024), BF),
    row=((3, 2, ROWS, 128), BF),
    col=((3, 2, WG, TALL, 128), BF),
    cells=((4, HP, WG, GROUP, 128), F32),
    o_r=((2, HP // STRIPE, 128, WIDE_R), F32),
    o_c=((2, WG, 128, WIDE_C), F32),
    inv_r=((2, HP // STRIPE, 8, WIDE_R), F32),
    inv_c=((2, WG, 8, WIDE_C), F32),
    p_r=((HP // STRIPE, CHUNK, HEADS * WIDE_R), BF),
    p_c=((WG, TALL, HEADS * WIDE_C), BF),
    qs_r=((HEADS * WIDE_R, 256), BF),
    qs_c=((HEADS * WIDE_C, 256), BF),
    dt_r=((128, HEADS * WIDE_R), BF),
    dt_c=((128, HEADS * WIDE_C), BF),
    g_all=((CHUNK, HEADS * WIDE_R), BF),
    g=((ROWS, 256), F32),
    gy=((ROWS, 256), BF),
    g1=((ROWS, 256), BF),
    da_r=((ROWS, 128), BF),
    dqkv_r=((ROWS, 384), BF),
    dqkv_c=((ROWS, 384), BF),
    gv=((128, 256), F32),
    vec=((2, 128, 256), F32),
)


KEPT = ("p_r", "p_c")


class Refs:
    def __init__(self, names, refs):
        self.__dict__.update(zip(names, refs))


QKV, PROJ, FC1, FC2, QKV_R, QKV_C, VEC, SAVE, LOAD_R, LOAD_C = range(10)
MATRICES = (QKV, PROJ, FC1, FC2)
SUMMED = (FC2, FC1, PROJ, QKV_R, QKV_C, VEC)
BEGIN, SECOND, THIRD, FOURTH, FINISH = range(5)
VERBS = ("begin", "second", "third", "fourth", "finish")
P_, H_, V_, F_, G_, BF_, B2_, BS_, BH_, BR_, BV_, BT_, BC_, BM_, BX_, PC_ = range(16)
STRIDE = {P_: 4, F_: 4, BM_: 4, BT_: 4, G_: 4, BV_: 2, V_: 2}


def lanes_of(block, half):
    return slice(256 * block + 128 * half, 256 * block + 128 * half + 128)


class Weights:
    def __init__(self, full):
        self.full = full

    def whole(self, name, l):
        value = self.full[name][l]
        return value.reshape(-1, value.shape[-1])

    def qkv_half(self, l, half):
        parts = []
        for i in range(3):
            value = self.full[QKV][l, :, :, :, :, lanes_of(i, half)]
            parts.append(value.reshape(-1, 128))
        return jnp.concatenate(parts, axis=1)

    def qkv(self, l):
        return self.whole(QKV, l)

    def proj(self, l):
        return self.whole(PROJ, l)

    def fc1(self, l):
        return self.whole(FC1, l)

    def fc2(self, l):
        return self.whole(FC2, l)


GATHER_MOVES = {
    (P_, 0, 3): [(QKV_C, 0, SECOND)],
    (H_, 0, 2): [(PROJ, 0, SECOND), (FC1, 0, SECOND), (QKV_C, 0, THIRD)],
    (H_, 0, 3): [(QKV, 1, BEGIN)],
    (PC_, 0, None): [(QKV_C, 0, FINISH)],
    (V_, 0, 0): [(FC2, 0, SECOND), (PROJ, 1, BEGIN)],
    (V_, 0, 3): [(FC1, 1, BEGIN)],
    (V_, 0, 4): [(PROJ, 0, THIRD), (FC1, 0, THIRD), (QKV, 1, SECOND)],
    (F_, 0, None): [(PROJ, 0, FINISH), (FC1, 0, FINISH), (SAVE, 0, BEGIN)],
    (F_, 0, 1): [(FC2, 0, THIRD), (FC2, 1, BEGIN)],
    (G_, 0, None): [(FC2, 0, FINISH)],
    (G_, 0, 1): [(QKV, 1, THIRD)],
    (P_, 1, None): [(QKV, 1, FINISH), (PROJ, 1, SECOND), (FC1, 1, SECOND)],
    (P_, 1, 3): [(SAVE, 0, FINISH)],
    (H_, 1, 1): [(FC2, 1, SECOND)],
    (V_, 1, 1): [(PROJ, 1, THIRD), (FC1, 1, THIRD)],
    (V_, 1, 4): [(FC2, 1, THIRD)],
    (F_, 1, None): [(PROJ, 1, FINISH), (FC1, 1, FINISH)],
    (G_, 1, None): [(FC2, 1, FINISH)],
}
SUM_MOVES = {
    (B2_, 1, None): [(FC2, 1, BEGIN)],
    (BS_, 1, None): [(FC1, 1, BEGIN), (PROJ, 1, BEGIN)],
    (BH_, 1, 0): [(FC2, 1, SECOND)],
    (BH_, 1, 1): [(FC1, 1, SECOND), (PROJ, 1, SECOND)],
    (BR_, 1, None): [(QKV_R, 1, BEGIN), (LOAD_R, 0, BEGIN)],
    (BV_, 1, 0): [(FC2, 1, THIRD)],
    (BV_, 1, 1): [(QKV_R, 1, SECOND)],
    (BV_, 1, 3): [(FC1, 1, THIRD), (PROJ, 1, THIRD)],
    (BV_, 1, 5): [(QKV_R, 1, THIRD)],
    (BC_, 1, None): [(QKV_C, 1, BEGIN), (LOAD_C, 0, BEGIN)],
    (BM_, 1, 1): [(FC2, 1, FOURTH)],
    (BM_, 1, 3): [(QKV_C, 1, SECOND)],
    (BX_, 1, None): [(VEC, 1, BEGIN)],
    (BF_, 0, 1): [(VEC, 1, SECOND)],
    (BF_, 0, 3): [(QKV_C, 1, THIRD), (FC1, 1, FOURTH), (PROJ, 1, FOURTH), (QKV_R, 1, FOURTH)],
    (B2_, 0, None): [(FC2, 0, BEGIN), (FC2, 1, FINISH)],
    (BS_, 0, None): [(FC1, 0, BEGIN), (PROJ, 0, BEGIN), (LOAD_R, 0, FINISH), (VEC, 1, THIRD)],
    (BH_, 0, 0): [(FC2, 0, SECOND)],
    (BH_, 0, 1): [
        (FC1, 0, SECOND), (PROJ, 0, SECOND), (FC1, 1, FINISH), (PROJ, 1, FINISH),
        (QKV_R, 1, FINISH),
    ],
    (BH_, 0, 3): [(QKV_C, 1, FOURTH), (VEC, 1, FOURTH)],
    (BR_, 0, None): [(QKV_R, 0, BEGIN), (LOAD_C, 0, FINISH)],
    (BV_, 0, 0): [(FC2, 0, THIRD)],
    (BV_, 0, 1): [(QKV_R, 0, SECOND)],
    (BV_, 0, 2): [(QKV_C, 1, FINISH), (VEC, 1, FINISH)],
    (BV_, 0, 3): [(FC1, 0, THIRD), (PROJ, 0, THIRD)],
    (BV_, 0, 5): [(QKV_R, 0, THIRD)],
    (BC_, 0, None): [(QKV_C, 0, BEGIN)],
    (BM_, 0, 1): [(FC2, 0, FOURTH), (QKV_C, 0, SECOND)],
    (BX_, 0, None): [(VEC, 0, BEGIN)],
}
LAST_MOVES = [
    (VEC, 0, SECOND), (QKV_C, 0, THIRD), (QKV_R, 0, FOURTH), (FC1, 0, FOURTH), (PROJ, 0, FOURTH),
    (FC2, 0, FINISH), (QKV_R, 0, FINISH), (FC1, 0, FINISH), (PROJ, 0, FINISH),
    (VEC, 0, FINISH), (QKV_C, 0, FINISH),
]
WIDE = {(QKV_C, 0): 1, (VEC, 0): 2}


class Local:
    def __init__(self, *copies):
        self.copies = copies

    def begin(self):
        for copy in self.copies:
            copy.start()

    def finish(self):
        for copy in self.copies:
            copy.wait()


class Moves:
    def __init__(self, table, parts):
        self.table, self.parts = table, parts

    def take(self, moves):
        for move in moves:
            name, l, verb = move
            getattr(self.parts[name, l], VERBS[verb])()

    def __call__(self, phase, l, step=None):
        if step is None:
            self.take(self.table.get((phase, l, None), []))
            return
        start, turn, stride = step
        for (name, block, when), moves in self.table.items():
            if (name, block) != (phase, l) or when is None or when % stride != turn:
                continue
            if start is None:
                self.take(moves)
            else:
                pl.when(start == when // stride)(functools.partial(self.take, moves))


def sweep(phase, l, count, body, at):
    stride = STRIDE.get(phase, 1)
    if stride == count:
        for s in range(count):
            body(s)
            at(phase, l, (None, s, stride))
        return

    def steps(i, carry):
        for turn in range(stride):
            body(i * stride + turn)
            at(phase, l, (i, turn, stride))
        return carry

    lax.fori_loop(0, count // stride, steps, 0)


class Gradients:
    def __init__(self, parts):
        self.parts = parts

    def put(self, name, l, value):
        ref = self.parts[name, l]
        ref[...] = value.astype(BF).reshape(ref.shape)


def plan(shards, copies, layers, width, hidden, held):
    zs, xs = 4, shards // 8
    place = (zs, xs, 2)
    d, f = width // shards, hidden // shards
    shapes = {k: pltpu.VMEM(*v) for k, v in SCRATCH.items()}
    own = {QKV: (d, 3 * width), PROJ: (d, width), FC1: (d, hidden), FC2: (f, width)}
    for name in MATRICES:
        shapes["full", name] = pltpu.VMEM((layers,) + place + own[name], BF)
    shapes["full", VEC] = pltpu.VMEM(place + (layers, d, held), BF)
    gathers = len(MATRICES) * layers + 2
    shapes["gather send"] = pltpu.SemaphoreType.DMA((gathers,))
    shapes["gather recv"] = pltpu.SemaphoreType.DMA((gathers, 3))
    shapes["gather local"] = pltpu.SemaphoreType.DMA((gathers,))
    half = (d, 3 * width // 2)
    own.update({QKV_R: half, QKV_C: half, VEC: (d, 128)})
    sums = len(SUMMED) * layers
    for l in range(layers):
        for name in SUMMED:
            shapes["part", name, l] = pltpu.VMEM(place + own[name], BF)
            for i, buf in enumerate(reduce_bufs(zs, xs, copies, own[name], WIDE.get((name, l), 0))):
                shapes["buf", name, l, i] = buf
    shapes["sum send"] = pltpu.SemaphoreType.DMA((sums,))
    shapes["sum recv"] = pltpu.SemaphoreType.DMA((sums, 4))
    shapes["out"] = pltpu.SemaphoreType.DMA((8 + 6 * layers,))
    for name in MATRICES:
        shapes["sum", name] = pltpu.VMEM((layers,) + own[name], F32)
    shapes["sum", VEC] = pltpu.VMEM((layers, d, held), F32)
    for name in ("tok", "cot"):
        shapes[name] = pltpu.VMEM((HP * WP, width), BF)
    return shapes


def step_kernel(shards, copies, names, *refs):
    h_ref, w_ref, tok, cot = refs[:4]
    own = dict(zip(MATRICES, refs[4:8]))
    vec_own = refs[8]
    y_ref, gt_ref = refs[9:11]
    outs = dict(zip(MATRICES + (VEC,), refs[11:16]))
    p_r_ref, p_c_ref = refs[16:18]
    s = dict(zip(names, refs[18:]))
    r = Refs(SCRATCH, [s[k] for k in SCRATCH])
    layers = own[QKV].shape[0]
    grid = Grid(shards, copies)
    grid.signal()
    h, w = h_ref[0], w_ref[0]

    sems = [s["gather send"], s["gather recv"], s["gather local"]]
    order = [(name, l) for l in range(layers) for name in MATRICES][1:]
    gathers = {}
    for i, (name, l) in enumerate(order):
        full = s["full", name].at[l]
        gathers[name, l] = Gather(grid, [(own[name].at[l], full)], full, sems, i)
    full = s["full", VEC]
    gathers[VEC, 0] = Gather(grid, [(vec_own, full)], full, sems, len(order))
    full = s["full", QKV].at[0]
    for half, name in enumerate((QKV_R, QKV_C)):
        parts = []
        for i in range(3):
            lanes = lanes_of(i, half)
            parts.append((own[QKV].at[0, :, lanes], full.at[:, :, :, :, lanes]))
        like = full.at[:, :, :, :, 0 : full.shape[-1] // 2]
        gathers[name, 0] = Gather(grid, parts, like, sems, len(order) + 1 + half)
    wt = Weights({name: s["full", name] for name in MATRICES})

    def local(src, dst, i):
        return pltpu.make_async_copy(src, dst, s["out"].at[i])

    tok_copy, cot_copy = local(tok, s["tok"], 6), local(cot, s["cot"], 7)
    tok_copy.start()
    cot_copy.start()
    grid.wait()
    first = [gathers[QKV_R, 0], gathers[VEC, 0]]
    for one in first:
        one.begin()
    for stack in (r.qs_r, r.qs_c):
        stack[...] = jnp.where(iota(stack.shape, 1) == 128, 1.0, 0.0).astype(BF)
    for stack in (r.dt_r, r.dt_c):
        stack[...] = jnp.zeros_like(stack)
    r.gv[...] = jnp.zeros_like(r.gv)
    tok_copy.wait()
    pad_groups(s["tok"], r.x.at[0])
    for i in range(HP // STRIPE):
        rows = slice(i * CHUNK, (i + 1) * CHUNK)
        r.after[0, rows, :] = norm_parts(r.x[0, rows, :])[0]
    cot_copy.wait()
    pad_groups(s["cot"], r.g)
    for one in first:
        one.second()
    gathers[QKV_C, 0].begin()
    for one in first:
        one.third()
    gathers[PROJ, 0].begin()
    gathers[FC1, 0].begin()
    for one in first:
        one.finish()
    gathers[FC2, 0].begin()
    for l in range(layers):
        value = s["full", VEC][:, :, :, l].astype(F32)
        value = value.reshape(-1, value.shape[-1])
        value = jnp.concatenate([value, jnp.zeros((value.shape[0], 128 - value.shape[1]), F32)], axis=1)
        r.vec[l] = value.T

    save = Local(local(r.p_r, p_r_ref, 2), local(r.p_c, p_c_ref, 3))
    at = Moves(GATHER_MOVES, {**gathers, (SAVE, 0): save})
    for l in range(layers):
        forward_layer(l, h, w, wt, r, at)

    sums = {}
    for l in range(layers):
        for i, name in enumerate(SUMMED):
            whole = QKV if name in (QKV_R, QKV_C) else name
            held = s["sum", whole].at[l]
            half = {QKV_R: 0, QKV_C: 1}.get(name)
            leave = None if half == 0 else local(held, outs[whole].at[l], 8 + l * 6 + i)
            out = (held, half, leave)
            wide = WIDE.get((name, l), 0)
            bufs = [s["buf", name, l, j] for j in range(4 - wide)]
            row = l * len(SUMMED) + i
            sums[name, l] = Reduce(
                grid, s["part", name, l], bufs, out, [s["sum send"], s["sum recv"]], row, wide
            )
    gradients = Gradients({(name, l): s["part", name, l] for l in range(layers) for name in SUMMED})

    load_r = Local(local(p_r_ref, r.p_r, 4))
    load_c = Local(local(p_c_ref, r.p_c, 5))
    at = Moves(SUM_MOVES, {**sums, (LOAD_R, 0): load_r, (LOAD_C, 0): load_c})
    for l in reversed(range(layers)):
        backward_layer(l, h, w, wt, r, gradients, at)
    flat = pl.ds(0, HP * WP)
    drop_groups(r.g, r.g)
    g_copy = local(r.g.at[flat], gt_ref, 1)
    g_copy.start()
    at.take(LAST_MOVES[:1])
    drop_groups(r.x.at[layers], r.x.at[layers])
    y_copy = local(r.x.at[layers, flat], y_ref, 0)
    y_copy.start()
    at.take(LAST_MOVES[1:])
    for one in sums.values():
        one.drain()
    y_copy.wait()
    g_copy.wait()


PIECES = 7


def finish_kernel(count, *refs):
    src, dst, held = refs[:count], refs[count : 2 * count], refs[2 * count : 3 * count]
    sems = refs[3 * count]
    moves = []
    for i in range(count):
        pieces = PIECES if i < 2 else 1
        size = src[i].shape[0] // pieces
        for j in range(pieces):
            part, sem = pl.ds(j * size, size), sems.at[len(moves)]
            first = pltpu.make_async_copy(src[i].at[part], held[i].at[part], sem)
            moves.append((first, pltpu.make_async_copy(held[i].at[part], dst[i].at[part], sem)))
    for first, _ in moves:
        first.start()
    for first, last in moves:
        first.wait()
        last.start()
    for _, last in moves:
        last.wait()


def shards_step(shards, copies, tokens, heights, widths, w_qkv, w_proj, w_fc1, w_fc2, vectors, cotangent):
    layers, _, hidden = w_fc1.shape
    count, width = tokens.shape
    vmem = pl.BlockSpec(memory_space=pltpu.VMEM)
    smem = pl.BlockSpec(memory_space=pltpu.SMEM)
    hbm = pl.BlockSpec(memory_space=pl.ANY)
    turned = vectors.transpose(0, 2, 1)
    scratch = plan(shards, copies, layers, width, hidden, turned.shape[2])
    matrices = [w_qkv, w_proj, w_fc1, w_fc2]
    results = [jax.ShapeDtypeStruct((count, width), F32)] * 2
    results += [jax.ShapeDtypeStruct(m.shape, F32) for m in matrices]
    results += [jax.ShapeDtypeStruct(turned.shape, F32)]
    results += [jax.ShapeDtypeStruct(*SCRATCH[k]) for k in KEPT]
    *raw, _, _ = pl.pallas_call(
        functools.partial(step_kernel, shards, copies, list(scratch)),
        out_shape=results,
        in_specs=[smem, smem, hbm, hbm] + [hbm] * 5,
        out_specs=[hbm] * 9,
        scratch_shapes=list(scratch.values()),
        compiler_params=pltpu.CompilerParams(
            collective_id=0,
            has_side_effects=True,
            vmem_limit_bytes=67043328,
        ),
    )(heights, widths, tokens, cotangent, *matrices, turned)
    final = [jax.ShapeDtypeStruct((count, width), F32)] * 2
    final += [jax.ShapeDtypeStruct(m.shape, F32) for m in matrices + [turned]]
    sems = pltpu.SemaphoreType.DMA((2 * PIECES + len(raw) - 2,))
    *arrays, vec = pl.pallas_call(
        functools.partial(finish_kernel, len(raw)),
        out_shape=final,
        in_specs=[hbm] * len(raw),
        out_specs=[hbm] * len(raw),
        scratch_shapes=[pltpu.VMEM(f.shape, F32) for f in final] + [sems],
        compiler_params=pltpu.CompilerParams(vmem_limit_bytes=67043328),
    )(*raw)
    return (*arrays, vec.transpose(0, 2, 1))


def solution(mesh):
    images = P(("fsdp", "rep"), None)
    weights = P(None, "fsdp", None)
    return jax.shard_map(
        functools.partial(shards_step, mesh.shape["fsdp"], mesh.shape["rep"]),
        mesh=mesh,
        in_specs=(images, P(("fsdp", "rep")), P(("fsdp", "rep")), weights, weights, weights, weights, P(None, None, "fsdp"), images),
        out_specs=(images, images, weights, weights, weights, weights, P(None, None, "fsdp")),
        check_vma=False,
    )
```
